16 devices in a mesh: dp: 4 (over z, y), cp: 4 (over x, core).
Axes of the slice: x: 2, y: 2, z: 2, core: 2. Of those that a mesh axis runs over, the one named last changes fastest.
Arguments:
- x: bfloat16 [4, 4096, 2048], P('dp', 'cp')
- grad_out: bfloat16 [4, 4096, 2048], P('dp', 'cp')
- w_q: bfloat16 [2048, 16, 128], replicated
- w_k: bfloat16 [2048, 2, 128], replicated
- w_v: bfloat16 [2048, 2, 128], replicated
- w_o: bfloat16 [2048, 16, 128], replicated
- w_up: bfloat16 [2048, 11008], replicated
- w_down: bfloat16 [11008, 2048], replicated
Outputs:
- output 1: bfloat16 [4, 4096, 2048], P('dp', 'cp')
- output 2: float32 [2048, 16, 128], P(('dp', 'cp'))
- output 3: float32 [2048, 2, 128], P(('dp', 'cp'))
- output 4: float32 [2048, 2, 128], P(('dp', 'cp'))
- output 5: float32 [2048, 16, 128], P(('dp', 'cp'))
- output 6: float32 [2048, 11008], P(('dp', 'cp'))
- output 7: float32 [11008, 2048], P(('dp', 'cp'))
All inputs are finite; a program needn't handle non-finite values.
Results may differ from the reference program's by a relative error of at most 0.0141916.
Values are sent between devices in bfloat16 or wider.
A program may use at most 1 GiB of HBM per device.

```python
import math
import jax
import jax.numpy as jnp
from jax import lax

D_MODEL = 2048
N_HEADS = 16
KV_HEADS = 2
HEAD_DIM = 128
FF_DIM = 11008
CP_SIZE = 4
DP_SIZE = 4
BATCH = 4
SEQ_LEN = 4096
GROUP = N_HEADS // KV_HEADS
HALF = SEQ_LEN // (2 * CP_SIZE)
Q_BLOCK = min(SEQ_LEN, 2 ** max(0, int(math.log2(max(1, 2 ** 22 // (N_HEADS * SEQ_LEN))))))
TOK_BLOCK = min(SEQ_LEN, 2 ** max(0, int(math.log2(max(1, 2 ** 22 // FF_DIM)))))
NEG_BIG = -1e30


def setup_inputs(seed: int = 0) -> dict:
    keys = jax.random.split(jax.random.key(seed), 8)

    def weight(key, shape, fan_in):
        return (jax.random.normal(key, shape, jnp.float32) * fan_in ** -0.5).astype(jnp.bfloat16)

    act_shape = (BATCH, SEQ_LEN, D_MODEL)
    return {
        'x': jax.random.normal(keys[0], act_shape, jnp.float32).astype(jnp.bfloat16),
        'grad_out': jax.random.normal(keys[1], act_shape, jnp.float32).astype(jnp.bfloat16),
        'w_q': weight(keys[2], (D_MODEL, N_HEADS, HEAD_DIM), D_MODEL),
        'w_k': weight(keys[3], (D_MODEL, KV_HEADS, HEAD_DIM), D_MODEL),
        'w_v': weight(keys[4], (D_MODEL, KV_HEADS, HEAD_DIM), D_MODEL),
        'w_o': weight(keys[5], (D_MODEL, N_HEADS, HEAD_DIM), N_HEADS * HEAD_DIM),
        'w_up': weight(keys[6], (D_MODEL, FF_DIM), D_MODEL),
        'w_down': weight(keys[7], (FF_DIM, D_MODEL), FF_DIM),
    }


def to_bf16(values):
    return values.astype(jnp.bfloat16).astype(jnp.float32)


def stored_to_natural(rows):
    blocks = rows.reshape(CP_SIZE, 2, HALF, D_MODEL)
    return jnp.concatenate([blocks[:, 0], blocks[::-1, 1]], axis=0).reshape(SEQ_LEN, D_MODEL)


def natural_to_stored(rows):
    halves = rows.reshape(2, CP_SIZE, HALF, D_MODEL)
    return jnp.stack([halves[0], halves[1][::-1]], axis=1).reshape(SEQ_LEN, D_MODEL)


def layer_row(x_row, w_q, w_k, w_v, w_o, w_up, w_down):
    q_all = to_bf16(jnp.dot(x_row, w_q.reshape(D_MODEL, N_HEADS * HEAD_DIM), preferred_element_type=jnp.float32))
    k_all = to_bf16(jnp.dot(x_row, w_k.reshape(D_MODEL, KV_HEADS * HEAD_DIM), preferred_element_type=jnp.float32)).reshape(SEQ_LEN, KV_HEADS, HEAD_DIM)
    v_all = to_bf16(jnp.dot(x_row, w_v.reshape(D_MODEL, KV_HEADS * HEAD_DIM), preferred_element_type=jnp.float32)).reshape(SEQ_LEN, KV_HEADS, HEAD_DIM)
    q_blocks = q_all.reshape(SEQ_LEN // Q_BLOCK, Q_BLOCK, KV_HEADS, GROUP, HEAD_DIM)
    starts = jnp.arange(SEQ_LEN // Q_BLOCK) * Q_BLOCK
    key_pos = jnp.arange(SEQ_LEN)

    def attn_block(block_in):
        q_blk, start = block_in
        scores = jnp.einsum('qkgd,tkd->kgqt', q_blk, k_all) * HEAD_DIM ** -0.5
        query_pos = start + jnp.arange(Q_BLOCK)
        scores = jnp.where(key_pos[None, :] <= query_pos[:, None], scores, NEG_BIG)
        attn_prob = to_bf16(jax.nn.softmax(scores, axis=-1))
        return to_bf16(jnp.einsum('kgqt,tkd->qkgd', attn_prob, v_all))

    attn_rows = lax.map(jax.checkpoint(attn_block), (q_blocks, starts)).reshape(SEQ_LEN, N_HEADS * HEAD_DIM)
    h_act = to_bf16(x_row + jnp.dot(attn_rows, w_o.reshape(D_MODEL, N_HEADS * HEAD_DIM).T, preferred_element_type=jnp.float32))

    def mlp_block(h_blk):
        hidden = jnp.dot(h_blk, w_up, preferred_element_type=jnp.float32)
        act_out = to_bf16(jax.nn.gelu(hidden, approximate=True))
        return h_blk + jnp.dot(act_out, w_down, preferred_element_type=jnp.float32)

    out_rows = lax.map(jax.checkpoint(mlp_block), h_act.reshape(SEQ_LEN // TOK_BLOCK, TOK_BLOCK, D_MODEL))
    return out_rows.reshape(SEQ_LEN, D_MODEL)


def reference(x, grad_out, w_q, w_k, w_v, w_o, w_up, w_down):
    weights = tuple(weight.astype(jnp.float32) for weight in (w_q, w_k, w_v, w_o, w_up, w_down))

    def row_step(grad_sum, row_pair):
        x_row, cot_row = row_pair
        _, back_fn = jax.vjp(layer_row, stored_to_natural(x_row.astype(jnp.float32)), *weights)
        cotangents = back_fn(stored_to_natural(cot_row.astype(jnp.float32)))
        new_sum = tuple(grad_old + grad_new for grad_old, grad_new in zip(grad_sum, cotangents[1:]))
        return new_sum, natural_to_stored(cotangents[0]).astype(jnp.bfloat16)

    grad_init = tuple(jnp.zeros_like(weight) for weight in weights)
    grad_sums, grad_x = lax.scan(row_step, grad_init, (x, grad_out))
    inv_count = 1.0 / (CP_SIZE * DP_SIZE)
    return (grad_x, grad_sums[0] * inv_count, grad_sums[1] * inv_count, grad_sums[2] * inv_count,
            grad_sums[3] * inv_count, grad_sums[4] * inv_count, grad_sums[5] * inv_count)
```

```python
import functools
import math

import jax
import jax.numpy as jnp
from jax import lax
from jax.experimental import pallas as pl
from jax.experimental.pallas import tpu as pltpu
from jax.experimental.layout import Layout, with_layout_constraint
from jax.sharding import PartitionSpec as P


NEG_BIG = -1e30
LOG2E = math.log2(math.e)
F32 = jnp.float32
FF_TILE = 256
BF16 = jnp.bfloat16


def row_major(values):
    return with_layout_constraint(values, Layout(major_to_minor=(0, 1)))


def dot_nn(lhs, rhs):
    return lax.dot_general(lhs, rhs, (((1,), (0,)), ((), ())), preferred_element_type=F32)


def dot_nt(lhs, rhs):
    return lax.dot_general(lhs, rhs, (((1,), (1,)), ((), ())), preferred_element_type=F32)


def dot_tn(lhs, rhs):
    return lax.dot_general(lhs, rhs, (((0,), (0,)), ((), ())), preferred_element_type=F32)


def dot_tt(lhs, rhs):
    return lax.dot_general(lhs, rhs, (((0,), (1,)), ((), ())), preferred_element_type=F32)


def pair_table(my_idx, cp_size):
    steps = jnp.arange(2 * cp_size + 1)
    late = steps > my_idx
    key_block = jnp.where(late, steps - my_idx - 1, steps)
    key_slot = jnp.where(key_block < cp_size, 2 * key_block, 2 * (2 * cp_size - 1 - key_block) + 1)
    last = (steps == my_idx) | (steps == 2 * cp_size)
    first = (steps == 0) | (steps == my_idx + 1)
    return jnp.stack([late, key_slot, last, first]).astype(jnp.int32)


def causal_keep(half):
    keys = lax.broadcasted_iota(jnp.int32, (half, half), 0)
    queries = lax.broadcasted_iota(jnp.int32, (half, half), 1)
    return keys <= queries


def attn_fwd_kernel(group, scale, tab, q_ref, k_ref, v_ref, of_ref, ob_ref, lse_ref, m_ref, l_ref, acc_ref):
    pair = pl.program_id(1)
    half, dim = k_ref.shape
    factor = scale * LOG2E

    @pl.when(tab[3, pair] == 1)
    def _():
        m_ref[...] = jnp.full(m_ref.shape, NEG_BIG, F32)
        l_ref[...] = jnp.zeros(l_ref.shape, F32)
        acc_ref[...] = jnp.zeros(acc_ref.shape, F32)

    def run(masked):
        keys = k_ref[...]
        vals_t = v_ref[...].T
        for head in range(group):
            rows = slice(head * dim, (head + 1) * dim)
            scores = dot_nn(keys, q_ref[rows, :])
            if masked:
                scores = jnp.where(causal_keep(half), scores, NEG_BIG)
            old_max = m_ref[head:head + 1, :]
            new_max = jnp.maximum(old_max, jnp.max(scores, axis=0, keepdims=True))
            probs = jnp.exp2((scores - new_max) * factor)
            alpha = jnp.exp2((old_max - new_max) * factor)
            m_ref[head:head + 1, :] = new_max
            l_ref[head:head + 1, :] = alpha * l_ref[head:head + 1, :] + jnp.sum(probs, axis=0, keepdims=True)
            acc_ref[rows, :] = alpha * acc_ref[rows, :] + dot_nn(vals_t, probs.astype(BF16))

    @pl.when(tab[2, pair] == 0)
    def _():
        run(False)

    @pl.when(tab[2, pair] == 1)
    def _():
        run(True)
        lse_ref[0] = m_ref[...] * factor + jnp.log2(l_ref[...])
        for head in range(group):
            rows = slice(head * dim, (head + 1) * dim)
            out = acc_ref[rows, :] / l_ref[head:head + 1, :]
            of_ref[rows, :] = out
            ob_ref[rows, :] = out.astype(BF16)


def attn_forward(tab, q_t, kv_all, kv_heads, head_dim):
    width, seq = q_t.shape
    half = seq // 2
    group = width // (kv_heads * head_dim)
    rows = group * head_dim
    n_pairs = tab.shape[1]
    q_spec = pl.BlockSpec((rows, half), lambda k, p, t: (k, t[0, p]))
    return pl.pallas_call(
        functools.partial(attn_fwd_kernel, group, head_dim ** -0.5),
        grid_spec=pltpu.PrefetchScalarGridSpec(
            num_scalar_prefetch=1,
            grid=(kv_heads, n_pairs),
            in_specs=[q_spec,
                      pl.BlockSpec((half, head_dim), lambda k, p, t: (t[1, p], k)),
                      pl.BlockSpec((half, head_dim), lambda k, p, t: (t[1, p], kv_heads + k))],
            out_specs=[q_spec, q_spec,
                       pl.BlockSpec((1, group, half), lambda k, p, t: (k, 0, t[0, p]))],
            scratch_shapes=[pltpu.VMEM((group, half), F32), pltpu.VMEM((group, half), F32),
                            pltpu.VMEM((rows, half), F32)]),
        out_shape=[jax.ShapeDtypeStruct((width, seq), F32), jax.ShapeDtypeStruct((width, seq), BF16),
                   jax.ShapeDtypeStruct((kv_heads, group, seq), F32)],
        compiler_params=pltpu.CompilerParams(vmem_limit_bytes=48 * 2 ** 20),
        cost_estimate=pl.CostEstimate(flops=4 * width * half * half * n_pairs,
                                      bytes_accessed=12 * width * seq, transcendentals=width // head_dim * half * half * n_pairs),
        name='attn_fwd',
    )(tab, q_t, kv_all, kv_all)


def attn_bwd_kernel(group, scale, tab, q_ref, do_ref, of_ref, lse_ref, k_ref, v_ref, dq_ref, dkv_ref, delta_ref, acc_ref):
    pair = pl.program_id(0)
    half, dim = k_ref.shape
    factor = scale * LOG2E
    slot = tab[1, pair]

    @pl.when(pair == 0)
    def _():
        dkv_ref[...] = jnp.zeros(dkv_ref.shape, F32)

    @pl.when(tab[3, pair] == 1)
    def _():
        acc_ref[...] = jnp.zeros(acc_ref.shape, F32)
        for head in range(group):
            rows = slice(head * dim, (head + 1) * dim)
            delta_ref[head:head + 1, :] = jnp.sum(do_ref[rows, :].astype(F32) * of_ref[rows, :], axis=0, keepdims=True)

    def run(masked):
        keys = k_ref[...]
        vals = v_ref[...]
        keys_t = keys.T
        for head in range(group):
            rows = slice(head * dim, (head + 1) * dim)
            q_head = q_ref[rows, :]
            do_head = do_ref[rows, :]
            scores = dot_nn(keys, q_head)
            if masked:
                scores = jnp.where(causal_keep(half), scores, NEG_BIG)
            probs = jnp.exp2(scores * factor - lse_ref[0, head:head + 1, :])
            grad_p = dot_nn(vals, do_head)
            grad_s = (probs * (grad_p - delta_ref[head:head + 1, :])).astype(BF16)
            dkv_ref[slot, 1] += dot_nt(do_head, probs.astype(BF16))
            dkv_ref[slot, 0] += scale * dot_nt(q_head, grad_s)
            acc_ref[rows, :] += dot_nn(keys_t, grad_s)

    @pl.when(tab[2, pair] == 0)
    def _():
        run(False)

    @pl.when(tab[2, pair] == 1)
    def _():
        run(True)
        dq_ref[...] = (scale * acc_ref[...]).astype(BF16)


def attn_backward(tab, q_t, do_t, o_f32, lse, kv_all, kv_heads, head_dim, kv_head):
    width, seq = q_t.shape
    half = seq // 2
    group = width // (kv_heads * head_dim)
    rows = group * head_dim
    n_slots = kv_all.shape[0] // half
    n_pairs = tab.shape[1]
    q_spec = pl.BlockSpec((rows, half), lambda p, t: (kv_head, t[0, p]))
    return pl.pallas_call(
        functools.partial(attn_bwd_kernel, group, head_dim ** -0.5),
        grid_spec=pltpu.PrefetchScalarGridSpec(
            num_scalar_prefetch=1,
            grid=(n_pairs,),
            in_specs=[q_spec, q_spec, q_spec,
                      pl.BlockSpec((1, group, half), lambda p, t: (kv_head, 0, t[0, p])),
                      pl.BlockSpec((half, head_dim), lambda p, t: (t[1, p], kv_head)),
                      pl.BlockSpec((half, head_dim), lambda p, t: (t[1, p], kv_heads + kv_head))],
            out_specs=[pl.BlockSpec((rows, half), lambda p, t: (0, t[0, p])),
                       pl.BlockSpec((n_slots, 2, head_dim, half), lambda p, t: (0, 0, 0, 0))],
            scratch_shapes=[pltpu.VMEM((group, half), F32), pltpu.VMEM((rows, half), F32)]),
        out_shape=[jax.ShapeDtypeStruct((rows, seq), BF16),
                   jax.ShapeDtypeStruct((n_slots, 2, head_dim, half), F32)],
        compiler_params=pltpu.CompilerParams(vmem_limit_bytes=56 * 2 ** 20),
        cost_estimate=pl.CostEstimate(flops=10 * rows * half * half * n_pairs,
                                      bytes_accessed=12 * rows * seq, transcendentals=group * half * half * n_pairs),
        name='attn_bwd',
    )(tab, q_t, do_t, o_f32, lse, kv_all, kv_all)


def gelu_parts(values):
    curve = math.sqrt(2 / math.pi)
    square = values * values
    tanh = jnp.tanh(values * (curve + (curve * 0.044715) * square))
    cdf = 0.5 + 0.5 * tanh
    slope = cdf + (0.5 * values) * (1.0 - tanh * tanh) * (curve + (3 * curve * 0.044715) * square)
    return values * cdf, slope


def ff_kernel(step_rows, h_ref, cot_ref, up_ref, down_ref, *rest):
    act_ref, du_ref, h_out, cot_out = rest[-4:]

    @pl.when(pl.program_id(0) == 0)
    def _():
        h_out[...] = h_ref[...]
        cot_out[...] = cot_ref[...]

    for first in range(0, h_ref.shape[0], step_rows):
        rows = slice(first, first + step_rows)
        hidden = dot_nn(h_ref[rows, :], up_ref[...])
        grad_act = dot_nt(cot_ref[rows, :], down_ref[...]).astype(BF16).astype(F32)
        act, slope = gelu_parts(hidden)
        act_ref[rows, :] = act.astype(BF16)
        du_ref[rows, :] = (grad_act * slope).astype(BF16)


def ff_forward(index, count, h_blk, cot_blk, up, down, carry):
    tokens, d_model = h_blk.shape
    width = up.shape[1]
    tile = FF_TILE
    whole = pl.BlockSpec((tokens, d_model), lambda n: (0, 0))
    shapes = [jax.ShapeDtypeStruct((count * tokens, width), BF16)] * 2 + [jax.ShapeDtypeStruct((count * tokens, d_model), BF16)] * 2
    carry = list(carry)
    return pl.pallas_call(
        functools.partial(ff_kernel, 256),
        grid=(pl.cdiv(width, tile),),
        in_specs=[whole, whole, pl.BlockSpec((d_model, tile), lambda n: (0, n)),
                  pl.BlockSpec((tile, d_model), lambda n: (n, 0))] + [pl.BlockSpec(memory_space=pl.ANY)] * len(carry),
        out_specs=[pl.BlockSpec((tokens, tile), lambda n: (index, n))] * 2 + [pl.BlockSpec((tokens, d_model), lambda n: (index, 0))] * 2,
        out_shape=shapes,
        input_output_aliases={4 + pos: pos for pos in range(len(carry))},
        compiler_params=pltpu.CompilerParams(vmem_limit_bytes=56 * 2 ** 20),
        cost_estimate=pl.CostEstimate(flops=4 * tokens * d_model * width, bytes_accessed=4 * d_model * (width + 2 * tokens),
                                      transcendentals=tokens * width),
        name='ff_forward',
    )(h_blk, cot_blk, up, down, *carry)


def grad_h_kernel(du_ref, up_ref, *rest):
    total = dot_nt(du_ref[...], up_ref[...])
    for extra in rest[:-1]:
        total = total + extra[...]
    rest[-1][...] = total.astype(rest[-1].dtype)


def grad_h_block(index, grad_u, up, extras, dtype):
    d_model, width = up.shape
    tokens = grad_u.shape[0] // 4
    tile = 256
    out_spec = pl.BlockSpec((tokens, tile), lambda n: (0, n))
    return pl.pallas_call(
        grad_h_kernel,
        grid=(d_model // tile,),
        in_specs=[pl.BlockSpec((tokens, width), lambda n: (index, 0)), pl.BlockSpec((tile, width), lambda n: (n, 0))]
        + [out_spec] * len(extras),
        out_specs=out_spec,
        out_shape=jax.ShapeDtypeStruct((tokens, d_model), dtype),
        compiler_params=pltpu.CompilerParams(vmem_limit_bytes=48 * 2 ** 20),
        cost_estimate=pl.CostEstimate(flops=2 * tokens * d_model * width, bytes_accessed=2 * width * (d_model + tokens) + 4 * tokens * d_model,
                                      transcendentals=0),
        name='grad_h',
    )(grad_u, up, *extras)


def spread_kernel(part, scale, idx_ref, got_ref, out_ref):
    count = got_ref.shape[0]
    for blk in range(out_ref.shape[1] // part):
        row, src = blk // count, blk % count
        out_ref[:, blk * part:(blk + 1) * part] = scale * got_ref[idx_ref[0] ^ src, :, row * part:(row + 1) * part]


def spread_columns(my_idx, got, part, scale):
    count, rows, width = got.shape
    return pl.pallas_call(
        functools.partial(spread_kernel, part, scale),
        in_specs=[pl.BlockSpec(memory_space=pltpu.SMEM), pl.BlockSpec(memory_space=pltpu.VMEM)],
        out_specs=pl.BlockSpec(memory_space=pltpu.VMEM),
        out_shape=jax.ShapeDtypeStruct((rows, count * width), F32),
        cost_estimate=pl.CostEstimate(flops=count * rows * width, bytes_accessed=8 * count * rows * width, transcendentals=0),
        name='spread',
    )(my_idx.reshape(1), got)


def solution(mesh):
    cp_size = mesh.shape['cp']
    dp_size = mesh.shape['dp']
    dev_count = cp_size * dp_size

    def swap(values, bits):
        return lax.ppermute(values, 'cp', [(src, src ^ bits) for src in range(cp_size)])

    def dp_reduce(grad):
        return lax.psum_scatter(grad, 'dp', scatter_dimension=0, tiled=True)

    def after(value, *earlier):
        return lax.optimization_barrier((value,) + earlier)[0]

    def per_device(x_loc, cot_loc, w_q, w_k, w_v, w_o, w_up, w_down):
        d_model = x_loc.shape[2]
        kv_heads, head_dim = w_k.shape[1], w_k.shape[2]
        n_heads = w_q.shape[1]
        kv_width = kv_heads * head_dim
        ff_dim = w_up.shape[1]
        ff_part = ff_dim // dev_count
        my_idx = lax.axis_index('cp')
        x = x_loc[0]
        cot = cot_loc[0]
        w_q = w_q.reshape(d_model, n_heads * head_dim)
        w_o = w_o.reshape(d_model, n_heads * head_dim)
        w_kv = jnp.concatenate([w_k.reshape(d_model, kv_width), w_v.reshape(d_model, kv_width)], axis=1)
        tab = pair_table(my_idx, cp_size)

        inv_count = 1.0 / dev_count

        def own_cols(values, bits):
            width = d_model // dev_count
            return jnp.concatenate([lax.dynamic_slice_in_dim(values, (part * cp_size + (my_idx ^ bits)) * width, width, axis=1)
                                    for part in range(dp_size)], axis=1)

        kv_own = dot_nn(x, w_kv).astype(BF16)
        kv_all = lax.all_gather(kv_own, 'cp', axis=0, tiled=True)
        q_t = dot_tt(w_q, x).astype(BF16)

        starts = [(part * cp_size + my_idx) * ff_part for part in range(dp_size)]
        extra = -(dp_size * ff_part) % FF_TILE
        w_up_own = jnp.concatenate([lax.dynamic_slice_in_dim(w_up, start, ff_part, axis=1) for start in starts]
                                   + [jnp.zeros((d_model, extra), BF16)], axis=1)
        w_down_own = jnp.concatenate([lax.dynamic_slice_in_dim(w_down, start, ff_part, axis=0) for start in starts]
                                     + [jnp.zeros((extra, d_model), BF16)], axis=0)

        cot_far = swap(after(cot, kv_all), 2)
        cot_near = swap(cot, 1)
        o_f32, o_t, lse = attn_forward(tab, q_t, kv_all, kv_heads, head_dim)
        o_t = after(o_t, cot_far)

        h_act = (x + dot_tt(o_t, w_o)).astype(BF16)
        h_far = swap(h_act, 2)
        h_near = swap(h_act, 1)
        state = ff_forward(0, cp_size, h_act, cot, w_up_own, w_down_own, ())
        state = ff_forward(1, cp_size, h_near, cot_near, w_up_own, w_down_own, state)
        cot_last = swap(cot_far, 1)
        h_last = swap(after(h_far, state[0]), 1)
        state = ff_forward(2, cp_size, h_far, cot_far, w_up_own, w_down_own, state)
        act_out, grad_u, h_all, cot_all = ff_forward(3, cp_size, h_last, cot_last, w_up_own, w_down_own, state)

        part_up = row_major(inv_count * dot_tn(h_all, grad_u[:, :dp_size * ff_part]))
        up_rows = dp_reduce(part_up)
        grad_u = after(grad_u, part_up)
        part = grad_h_block(3, grad_u, w_up_own, [], F32)
        near = swap(part, 1)
        part = grad_h_block(1, after(grad_u, part), w_up_own, [], F32)
        side = swap(part, 1)
        part = grad_h_block(2, after(grad_u, part), w_up_own, [near], F32)
        far = swap(part, 2)
        part_down = inv_count * dot_tn(after(act_out, part)[:, :dp_size * ff_part], cot_all)
        grad_w_down = dp_reduce(part_down)
        grad_h_bf = grad_h_block(0, after(grad_u, part_down), w_up_own, [cot, side, far], BF16)

        up_got = [lax.dynamic_slice_in_dim(up_rows, (my_idx ^ bits) * (d_model // dev_count), d_model // dev_count, axis=0)
                  for bits in range(cp_size)]
        up_got = jnp.stack([up_got[0]] + [row_major(swap(row_major(up_got[bits]), bits)) for bits in range(1, cp_size)])
        grad_w_up = spread_columns(my_idx, up_got, ff_part, 1.0)

        def block_sum(left, right_t):
            def block(bits):
                return inv_count * dot_tt(own_cols(left, bits), right_t)

            return block

        def first_sends(block):
            parts = block(3), block(1)
            return (swap(parts[0], 1), swap(parts[1], 1)), parts

        def second_send(block, sent):
            part = block(2) + sent[0]
            return swap(part, 2), part

        do_t = dot_tt(w_o, grad_h_bf).astype(BF16)
        o_block = block_sum(grad_h_bf, o_t)
        o_sent, parts = first_sends(o_block)
        do_t = after(do_t, *parts)

        def kv_block(dkv):
            blocks = dkv.reshape((cp_size, 2) + dkv.shape[1:])
            return lambda bits: lax.dynamic_index_in_dim(blocks, my_idx ^ bits, axis=0, keepdims=False)

        dq0_t, dkv0 = attn_backward(tab, q_t, do_t, o_f32, lse, kv_all, kv_heads, head_dim, 0)
        kv0_block, q0_block = kv_block(dkv0), block_sum(x, dq0_t)
        kv0_sent, parts_kv = first_sends(kv0_block)
        q0_sent, parts_q = first_sends(q0_block)
        o_far, part = second_send(o_block, o_sent)
        do_t = after(do_t, part, *parts_kv, *parts_q)
        dq1_t, dkv1 = attn_backward(tab, q_t, do_t, o_f32, lse, kv_all, kv_heads, head_dim, 1)
        kv1_block, q1_block = kv_block(dkv1), block_sum(x, dq1_t)
        kv1_sent, _ = first_sends(kv1_block)
        kv0_far, _ = second_send(kv0_block, kv0_sent)
        q0_far, _ = second_send(q0_block, q0_sent)
        q1_sent, _ = first_sends(q1_block)
        kv1_far, _ = second_send(kv1_block, kv1_sent)
        q1_far, part = second_send(q1_block, q1_sent)
        grad_w_o = dp_reduce(o_block(0) + o_sent[1] + o_far)
        grad_x = grad_h_bf + dot_tt(after(jnp.concatenate([dq0_t, dq1_t], axis=0), part), w_q)
        dkv_parts = [(kv0_block(0) + kv0_sent[1] + kv0_far).astype(BF16), (kv1_block(0) + kv1_sent[1] + kv1_far).astype(BF16)]
        dkv_t = jnp.concatenate([jnp.concatenate([part[0, which], part[1, which]], axis=1)
                                 for which in range(2) for part in dkv_parts], axis=0)
        w_block = block_sum(x, dkv_t)
        w_sent, _ = first_sends(w_block)
        grad_q0 = dp_reduce(q0_block(0) + q0_sent[1] + q0_far)
        w_far, _ = second_send(w_block, w_sent)
        grad_x = grad_x + dot_tt(dkv_t, w_kv)
        grad_q1 = dp_reduce(q1_block(0) + q1_sent[1] + q1_far)
        grad_kv = dp_reduce(w_block(0) + w_sent[1] + w_far)

        own_rows = d_model // dev_count
        grad_w_q = jnp.concatenate([grad_q0, grad_q1], axis=1).reshape(own_rows, n_heads, head_dim)
        grad_w_k = grad_kv[:, :kv_width].reshape(own_rows, kv_heads, head_dim)
        grad_w_v = grad_kv[:, kv_width:].reshape(own_rows, kv_heads, head_dim)
        grad_w_o = grad_w_o.reshape(own_rows, n_heads, head_dim)
        return grad_x.astype(BF16)[None], grad_w_q, grad_w_k, grad_w_v, grad_w_o, grad_w_up, grad_w_down

    act_spec = P('dp', 'cp', None)
    rep_three = P(None, None, None)
    rep_two = P(None, None)
    grad_three = P(('dp', 'cp'), None, None)
    grad_two = P(('dp', 'cp'), None)
    return jax.shard_map(per_device, mesh=mesh,
                         in_specs=(act_spec, act_spec, rep_three, rep_three, rep_three, rep_three, rep_two, rep_two),
                         out_specs=(act_spec, grad_three, grad_three, grad_three, grad_three, grad_two, grad_two),
                         check_vma=False)
```

```python
import functools
import math

import jax
import jax.numpy as jnp
from jax import lax
from jax.experimental import pallas as pl
from jax.experimental.pallas import tpu as pltpu
from jax.experimental.layout import Layout, with_layout_constraint
from jax.sharding import PartitionSpec as P


NEG_BIG = -1e30
LOG2E = math.log2(math.e)
F32 = jnp.float32
FF_TILE = 256
BF16 = jnp.bfloat16


def row_major(values):
    return with_layout_constraint(values, Layout(major_to_minor=(0, 1)))


def dot_nn(lhs, rhs):
    return lax.dot_general(lhs, rhs, (((1,), (0,)), ((), ())), preferred_element_type=F32)


def dot_nt(lhs, rhs):
    return lax.dot_general(lhs, rhs, (((1,), (1,)), ((), ())), preferred_element_type=F32)


def dot_tn(lhs, rhs):
    return lax.dot_general(lhs, rhs, (((0,), (0,)), ((), ())), preferred_element_type=F32)


def dot_tt(lhs, rhs):
    return lax.dot_general(lhs, rhs, (((0,), (1,)), ((), ())), preferred_element_type=F32)


def pair_table(my_idx, cp_size):
    steps = jnp.arange(2 * cp_size + 1)
    late = steps > my_idx
    key_block = jnp.where(late, steps - my_idx - 1, steps)
    key_slot = jnp.where(key_block < cp_size, 2 * key_block, 2 * (2 * cp_size - 1 - key_block) + 1)
    last = (steps == my_idx) | (steps == 2 * cp_size)
    first = (steps == 0) | (steps == my_idx + 1)
    return jnp.stack([late, key_slot, last, first]).astype(jnp.int32)


def causal_keep(half):
    keys = lax.broadcasted_iota(jnp.int32, (half, half), 0)
    queries = lax.broadcasted_iota(jnp.int32, (half, half), 1)
    return keys <= queries


def attn_fwd_kernel(group, scale, tab, q_ref, k_ref, v_ref, of_ref, ob_ref, lse_ref, m_ref, l_ref):
    dim = k_ref.shape[1]
    half = q_ref.shape[1] // 2
    factor = scale * LOG2E

    def pair_step(pair, carry):
        cols = pl.ds(pl.multiple_of(tab[0, pair] * half, half), half)
        slot = pl.ds(pl.multiple_of(tab[1, pair] * half, half), half)

        @pl.when(tab[3, pair] == 1)
        def _():
            m_ref[...] = jnp.full(m_ref.shape, NEG_BIG, F32)
            l_ref[...] = jnp.zeros(l_ref.shape, F32)
            of_ref[:, cols] = jnp.zeros((of_ref.shape[0], half), F32)

        def run(masked):
            keys = k_ref[slot, :]
            vals_t = v_ref[slot, :].T
            for head in range(group):
                rows = slice(head * dim, (head + 1) * dim)
                scores = dot_nn(keys, q_ref[rows, cols])
                if masked:
                    scores = jnp.where(causal_keep(half), scores, NEG_BIG)
                old_max = m_ref[head:head + 1, :]
                new_max = jnp.maximum(old_max, jnp.max(scores, axis=0, keepdims=True))
                probs = jnp.exp2((scores - new_max) * factor)
                alpha = jnp.exp2((old_max - new_max) * factor)
                m_ref[head:head + 1, :] = new_max
                l_ref[head:head + 1, :] = alpha * l_ref[head:head + 1, :] + jnp.sum(probs, axis=0, keepdims=True)
                of_ref[rows, cols] = alpha * of_ref[rows, cols] + dot_nn(vals_t, probs.astype(BF16))

        @pl.when(tab[2, pair] == 0)
        def _():
            run(False)

        @pl.when(tab[2, pair] == 1)
        def _():
            run(True)
            lse_ref[0, :, cols] = m_ref[...] * factor + jnp.log2(l_ref[...])
            for head in range(group):
                rows = slice(head * dim, (head + 1) * dim)
                out = of_ref[rows, cols] / l_ref[head:head + 1, :]
                of_ref[rows, cols] = out
                ob_ref[rows, cols] = out.astype(BF16)

        return carry

    lax.fori_loop(0, tab.shape[1], pair_step, 0)


def attn_forward(tab, q_t, kv_all, kv_heads, head_dim):
    width, seq = q_t.shape
    half = seq // 2
    group = width // (kv_heads * head_dim)
    rows = group * head_dim
    n_pairs = tab.shape[1]
    q_spec = pl.BlockSpec((rows, seq), lambda k, t: (k, 0))
    return pl.pallas_call(
        functools.partial(attn_fwd_kernel, group, head_dim ** -0.5),
        grid_spec=pltpu.PrefetchScalarGridSpec(
            num_scalar_prefetch=1,
            grid=(kv_heads,),
            in_specs=[q_spec,
                      pl.BlockSpec((kv_all.shape[0], head_dim), lambda k, t: (0, k)),
                      pl.BlockSpec((kv_all.shape[0], head_dim), lambda k, t: (0, kv_heads + k))],
            out_specs=[q_spec, q_spec,
                       pl.BlockSpec((1, group, seq), lambda k, t: (k, 0, 0))],
            scratch_shapes=[pltpu.VMEM((group, half), F32), pltpu.VMEM((group, half), F32)]),
        out_shape=[jax.ShapeDtypeStruct((width, seq), F32), jax.ShapeDtypeStruct((width, seq), BF16),
                   jax.ShapeDtypeStruct((kv_heads, group, seq), F32)],
        compiler_params=pltpu.CompilerParams(vmem_limit_bytes=56 * 2 ** 20),
        cost_estimate=pl.CostEstimate(flops=4 * width * half * half * n_pairs,
                                      bytes_accessed=12 * width * seq, transcendentals=width // head_dim * half * half * n_pairs),
        name='attn_fwd',
    )(tab, q_t, kv_all, kv_all)


def attn_bwd_kernel(group, scale, tab, q_ref, do_ref, of_ref, lse_ref, k_ref, v_ref, dq_ref, dkv_ref, delta_ref, acc_ref):
    dim = k_ref.shape[1]
    half = q_ref.shape[1] // 2
    factor = scale * LOG2E
    dkv_ref[...] = jnp.zeros(dkv_ref.shape, F32)

    def pair_step(pair, carry):
        cols = pl.ds(pl.multiple_of(tab[0, pair] * half, half), half)
        slot = tab[1, pair]
        slot_rows = pl.ds(pl.multiple_of(slot * half, half), half)

        @pl.when(tab[3, pair] == 1)
        def _():
            acc_ref[...] = jnp.zeros(acc_ref.shape, F32)
            for head in range(group):
                rows = slice(head * dim, (head + 1) * dim)
                delta_ref[head:head + 1, :] = jnp.sum(do_ref[rows, cols].astype(F32) * of_ref[rows, cols], axis=0, keepdims=True)

        def run(masked):
            keys = k_ref[slot_rows, :]
            vals = v_ref[slot_rows, :]
            keys_t = keys.T
            for head in range(group):
                rows = slice(head * dim, (head + 1) * dim)
                q_head = q_ref[rows, cols]
                do_head = do_ref[rows, cols]
                scores = dot_nn(keys, q_head)
                if masked:
                    scores = jnp.where(causal_keep(half), scores, NEG_BIG)
                probs = jnp.exp2(scores * factor - lse_ref[0, head:head + 1, cols])
                grad_p = dot_nn(vals, do_head)
                grad_s = (probs * (grad_p - delta_ref[head:head + 1, :])).astype(BF16)
                dkv_ref[slot, 1] += dot_nt(do_head, probs.astype(BF16))
                dkv_ref[slot, 0] += scale * dot_nt(q_head, grad_s)
                acc_ref[rows, :] += dot_nn(keys_t, grad_s)

        @pl.when(tab[2, pair] == 0)
        def _():
            run(False)

        @pl.when(tab[2, pair] == 1)
        def _():
            run(True)
            dq_ref[:, cols] = (scale * acc_ref[...]).astype(BF16)

        return carry

    lax.fori_loop(0, tab.shape[1], pair_step, 0)


def attn_backward(tab, q_t, do_t, o_f32, lse, kv_all, kv_heads, head_dim, kv_head):
    width, seq = q_t.shape
    half = seq // 2
    group = width // (kv_heads * head_dim)
    rows = group * head_dim
    n_slots = kv_all.shape[0] // half
    n_pairs = tab.shape[1]
    q_spec = pl.BlockSpec((rows, seq), lambda p, t: (kv_head, 0))
    return pl.pallas_call(
        functools.partial(attn_bwd_kernel, group, head_dim ** -0.5),
        grid_spec=pltpu.PrefetchScalarGridSpec(
            num_scalar_prefetch=1,
            grid=(1,),
            in_specs=[q_spec, q_spec, q_spec,
                      pl.BlockSpec((1, group, seq), lambda p, t: (kv_head, 0, 0)),
                      pl.BlockSpec((kv_all.shape[0], head_dim), lambda p, t: (0, kv_head)),
                      pl.BlockSpec((kv_all.shape[0], head_dim), lambda p, t: (0, kv_heads + kv_head))],
            out_specs=[pl.BlockSpec((rows, seq), lambda p, t: (0, 0)),
                       pl.BlockSpec((n_slots, 2, head_dim, half), lambda p, t: (0, 0, 0, 0))],
            scratch_shapes=[pltpu.VMEM((group, half), F32), pltpu.VMEM((rows, half), F32)]),
        out_shape=[jax.ShapeDtypeStruct((rows, seq), BF16),
                   jax.ShapeDtypeStruct((n_slots, 2, head_dim, half), F32)],
        compiler_params=pltpu.CompilerParams(vmem_limit_bytes=56 * 2 ** 20),
        cost_estimate=pl.CostEstimate(flops=10 * rows * half * half * n_pairs,
                                      bytes_accessed=12 * rows * seq, transcendentals=group * half * half * n_pairs),
        name='attn_bwd',
    )(tab, q_t, do_t, o_f32, lse, kv_all, kv_all)


def gelu_parts(values):
    curve = math.sqrt(2 / math.pi)
    square = values * values
    tanh = jnp.tanh(values * (curve + (curve * 0.044715) * square))
    cdf = 0.5 + 0.5 * tanh
    slope = cdf + (0.5 * values) * (1.0 - tanh * tanh) * (curve + (3 * curve * 0.044715) * square)
    return values * cdf, slope


def prep_kernel(segs, parts, idx_ref, *refs):
    n_blocks = sum(seg['tiles'] + 1 for seg in segs)
    blocks, down_ref = refs[:n_blocks], refs[n_blocks]
    n_parts = len(parts)
    up_refs, down_refs = refs[n_blocks + 1:n_blocks + 1 + n_parts], refs[n_blocks + 1 + n_parts:n_blocks + 1 + 2 * n_parts]
    buf_ref, zero_ref, in_sem, out_sem = refs[n_blocks + 1 + 2 * n_parts:]
    step = pl.program_id(0)
    n_own, own_rows = buf_ref.shape[0], buf_ref.shape[1]
    ins = [pltpu.make_async_copy(down_ref.at[pl.ds(pl.multiple_of(idx_ref[0, own], 16), own_rows)], buf_ref.at[own], in_sem.at[own])
           for own in range(n_own)]
    outs = []
    for part, down_out in zip(parts, down_refs):
        for own in range(n_own):
            outs.append(pltpu.make_async_copy(buf_ref.at[own, pl.ds(part['first'], part['rows'])],
                                              down_out.at[pl.ds(own * part['rows'], part['rows'])], out_sem.at[len(outs)]))
        if part['pad']:
            outs.append(pltpu.make_async_copy(zero_ref.at[pl.ds(0, part['pad'])],
                                              down_out.at[pl.ds(n_own * part['rows'], part['pad'])], out_sem.at[len(outs)]))

    @pl.when(step == 0)
    def _():
        zero_ref[...] = jnp.zeros(zero_ref.shape, BF16)
        for copy in ins:
            copy.start()

    @pl.when(step == 1)
    def _():
        for copy in ins:
            copy.wait()
        for copy in outs:
            copy.start()

    rows = blocks[0].shape[0]
    lanes = lax.broadcasted_iota(jnp.int32, (rows, 128), 1)
    cover = [{} for _ in parts]
    pos = 0
    for number, seg in enumerate(segs):
        shift = idx_ref[1, number]
        turned = [pltpu.roll(blocks[pos + tile][...].astype(F32), (128 - shift) % 128, 1) for tile in range(seg['tiles'] + 1)]
        pos += seg['tiles'] + 1
        for tile in range(seg['tiles']):
            cover[seg['part']].setdefault(seg['tile'] + tile, []).append(
                (seg['start'], jnp.where(lanes < 128 - shift, turned[tile], turned[tile + 1])))
    for part, tiles, up_ref in zip(parts, cover, up_refs):
        used = n_own * part['rows']
        for tile in range(up_ref.shape[1] // 128):
            value = jnp.zeros((rows, 128), F32)
            for start, piece in tiles.get(tile, []):
                value = piece if start <= tile * 128 else jnp.where(lanes >= start - tile * 128, piece, value)
            if used < (tile + 1) * 128:
                value = jnp.where(lanes < used - tile * 128, value, 0.0)
            up_ref[:, tile * 128:(tile + 1) * 128] = value.astype(BF16)

    @pl.when(step == pl.num_programs(0) - 1)
    def _():
        for copy in outs:
            copy.wait()


def prepare(starts, splits, w_up, w_down):
    d_model, own_rows = w_up.shape[0], splits[-1][0] + splits[-1][1]
    n_own = starts.shape[0]
    parts = [{'first': first, 'rows': count, 'pad': -(n_own * count) % FF_TILE} for first, count in splits]
    segs, shifts, bases = [], [], []
    for number, part in enumerate(parts):
        for own in range(n_own):
            dest = own * part['rows']
            segs.append({'part': number, 'start': dest, 'tile': dest // 128, 'tiles': -(-(dest % 128 + part['rows']) // 128)})
            source = starts[own] + part['first'] - dest % 128
            shifts.append(source % 128)
            bases.append(source // 128)
    table = jnp.stack([jnp.pad(starts, (0, len(segs) - n_own)), jnp.stack(shifts), jnp.stack(bases)]).astype(jnp.int32)
    rows = 512
    last = w_up.shape[1] // 128 - 1
    in_specs = []
    for number, seg in enumerate(segs):
        for tile in range(seg['tiles'] + 1):
            in_specs.append(pl.BlockSpec((rows, 128), lambda i, t, number=number, tile=tile:
                                         (i, jnp.clip(t[2, number] + tile, 0, last))))
    widths = [n_own * part['rows'] + part['pad'] for part in parts]
    outs = pl.pallas_call(
        functools.partial(prep_kernel, segs, parts),
        grid_spec=pltpu.PrefetchScalarGridSpec(
            num_scalar_prefetch=1,
            grid=(d_model // rows,),
            in_specs=in_specs + [pl.BlockSpec(memory_space=pl.ANY)],
            out_specs=[pl.BlockSpec((rows, width), lambda i, t: (i, 0)) for width in widths]
            + [pl.BlockSpec(memory_space=pl.ANY) for _ in widths],
            scratch_shapes=[pltpu.VMEM((n_own, own_rows, d_model), BF16), pltpu.VMEM((64, d_model), BF16),
                            pltpu.SemaphoreType.DMA((n_own,)), pltpu.SemaphoreType.DMA((n_own * len(parts) + len(parts),))]),
        out_shape=[jax.ShapeDtypeStruct((d_model, width), BF16) for width in widths]
        + [jax.ShapeDtypeStruct((width, d_model), BF16) for width in widths],
        compiler_params=pltpu.CompilerParams(vmem_limit_bytes=56 * 2 ** 20),
        cost_estimate=pl.CostEstimate(flops=8 * d_model * sum(widths), bytes_accessed=9 * d_model * sum(widths), transcendentals=0),
        name='prepare',
    )(table, *([w_up] * len(in_specs)), w_down)
    return outs[:len(parts)], outs[len(parts):]


def ff_kernel(step_rows, copies, index, h_ref, cot_ref, up_ref, down_ref, *rest):
    if copies:
        act_ref, du_ref, h_out, cot_out, sem = rest[-5:]
        rows = pl.ds(index * h_ref.shape[0], h_ref.shape[0])
        moves = [pltpu.make_async_copy(h_ref, h_out.at[rows], sem.at[0]), pltpu.make_async_copy(cot_ref, cot_out.at[rows], sem.at[1])]

        @pl.when(pl.program_id(0) == 0)
        def _():
            for move in moves:
                move.start()
    else:
        act_ref, du_ref = rest[-2:]

    for first in range(0, h_ref.shape[0], step_rows):
        rows = slice(first, first + step_rows)
        hidden = dot_nn(h_ref[rows, :], up_ref[...])
        grad_act = dot_nt(cot_ref[rows, :], down_ref[...]).astype(BF16).astype(F32)
        act, slope = gelu_parts(hidden)
        act_ref[rows, :] = act.astype(BF16)
        du_ref[rows, :] = (grad_act * slope).astype(BF16)

    if copies:
        @pl.when(pl.program_id(0) == pl.num_programs(0) - 1)
        def _():
            for move in moves:
                move.wait()


def ff_forward(index, count, h_blk, cot_blk, up, down, copies, carry):
    tokens, d_model = h_blk.shape
    width = up.shape[1]
    tile = FF_TILE
    whole = pl.BlockSpec((tokens, d_model), lambda n: (0, 0))
    shapes = [jax.ShapeDtypeStruct((count * tokens, width), BF16)] * 2
    specs = [pl.BlockSpec((tokens, tile), lambda n: (index, n))] * 2
    if copies:
        shapes = shapes + [jax.ShapeDtypeStruct((count * tokens, d_model), BF16)] * 2
        specs = specs + [pl.BlockSpec(memory_space=pl.ANY)] * 2
    carry = list(carry)
    return pl.pallas_call(
        functools.partial(ff_kernel, 256, copies, index),
        grid=(width // tile,),
        in_specs=[whole, whole, pl.BlockSpec((d_model, tile), lambda n: (0, n)),
                  pl.BlockSpec((tile, d_model), lambda n: (n, 0))] + [pl.BlockSpec(memory_space=pl.ANY)] * len(carry),
        out_specs=specs,
        out_shape=shapes,
        input_output_aliases={4 + pos: pos for pos in range(len(carry))},
        scratch_shapes=[pltpu.SemaphoreType.DMA((2,))] if copies else [],
        compiler_params=pltpu.CompilerParams(vmem_limit_bytes=56 * 2 ** 20),
        cost_estimate=pl.CostEstimate(flops=4 * tokens * d_model * width, bytes_accessed=4 * d_model * (width + 2 * tokens),
                                      transcendentals=tokens * width),
        name='ff_forward',
    )(h_blk, cot_blk, up, down, *carry)


def grad_h_kernel(n_parts, *refs):
    total = sum(dot_nt(refs[2 * part][...], refs[2 * part + 1][...]) for part in range(n_parts))
    for extra in refs[2 * n_parts:-1]:
        total = total + extra[...]
    refs[-1][...] = total.astype(refs[-1].dtype)


def grad_h_block(index, grad_u, up, extras, dtype):
    d_model = up[0].shape[0]
    tokens = grad_u[0].shape[0] // 4
    width = sum(part.shape[1] for part in up)
    tile = 256
    out_spec = pl.BlockSpec((tokens, tile), lambda n: (0, n))
    in_specs, args = [], []
    for left, right in zip(grad_u, up):
        in_specs += [pl.BlockSpec((tokens, left.shape[1]), lambda n: (index, 0)), pl.BlockSpec((tile, right.shape[1]), lambda n: (n, 0))]
        args += [left, right]
    return pl.pallas_call(
        functools.partial(grad_h_kernel, len(up)),
        grid=(d_model // tile,),
        in_specs=in_specs + [out_spec] * len(extras),
        out_specs=out_spec,
        out_shape=jax.ShapeDtypeStruct((tokens, d_model), dtype),
        compiler_params=pltpu.CompilerParams(vmem_limit_bytes=48 * 2 ** 20),
        cost_estimate=pl.CostEstimate(flops=2 * tokens * d_model * width, bytes_accessed=2 * width * (d_model + tokens) + 4 * tokens * d_model,
                                      transcendentals=0),
        name='grad_h',
    )(*args, *extras)


def spread_kernel(splits, idx_ref, *refs):
    got_refs, out_ref = refs[:-1], refs[-1]
    count = got_refs[0].shape[0]
    block = splits[-1][0] + splits[-1][1]
    for dest in range(out_ref.shape[1] // block):
        row, src = dest // count, dest % count
        for (first, cols), got_ref in zip(splits, got_refs):
            out_ref[:, dest * block + first:dest * block + first + cols] = got_ref[idx_ref[0] ^ src, :, row * cols:(row + 1) * cols]


def spread_columns(my_idx, got, splits):
    count, rows = got[0].shape[:2]
    width = count * sum(part.shape[2] for part in got)
    return pl.pallas_call(
        functools.partial(spread_kernel, splits),
        in_specs=[pl.BlockSpec(memory_space=pltpu.SMEM)] + [pl.BlockSpec(memory_space=pltpu.VMEM)] * len(got),
        out_specs=pl.BlockSpec(memory_space=pltpu.VMEM),
        out_shape=jax.ShapeDtypeStruct((rows, width), F32),
        cost_estimate=pl.CostEstimate(flops=rows * width, bytes_accessed=8 * rows * width, transcendentals=0),
        name='spread',
    )(my_idx.reshape(1), *got)


def solution(mesh):
    cp_size = mesh.shape['cp']
    dp_size = mesh.shape['dp']
    dev_count = cp_size * dp_size

    def swap(values, bits):
        return lax.ppermute(values, 'cp', [(src, src ^ bits) for src in range(cp_size)])

    def dp_reduce(grad):
        return lax.psum_scatter(grad, 'dp', scatter_dimension=0, tiled=True)

    def after(value, *earlier):
        return lax.optimization_barrier((value,) + earlier)[0]

    def per_device(x_loc, cot_loc, w_q, w_k, w_v, w_o, w_up, w_down):
        d_model = x_loc.shape[2]
        kv_heads, head_dim = w_k.shape[1], w_k.shape[2]
        n_heads = w_q.shape[1]
        kv_width = kv_heads * head_dim
        ff_dim = w_up.shape[1]
        ff_part = ff_dim // dev_count
        my_idx = lax.axis_index('cp')
        x = x_loc[0]
        cot = cot_loc[0]
        w_q = w_q.reshape(d_model, n_heads * head_dim)
        w_o = w_o.reshape(d_model, n_heads * head_dim)
        w_kv = jnp.concatenate([w_k.reshape(d_model, kv_width), w_v.reshape(d_model, kv_width)], axis=1)
        tab = pair_table(my_idx, cp_size)

        inv_count = 1.0 / dev_count

        def own_cols(values, bits):
            width = d_model // dev_count
            return jnp.concatenate([lax.dynamic_slice_in_dim(values, (part * cp_size + (my_idx ^ bits)) * width, width, axis=1)
                                    for part in range(dp_size)], axis=1)

        kv_own = dot_nn(x, w_kv).astype(BF16)
        kv_all = lax.all_gather(kv_own, 'cp', axis=0, tiled=True)
        cot_near = swap(cot, 1)
        q_t = dot_tt(w_q, x).astype(BF16)

        first_part = FF_TILE * (dp_size * ff_part // (2 * FF_TILE)) // dp_size
        splits = ((0, first_part), (first_part, ff_part - first_part))
        used = [dp_size * count for _, count in splits]
        starts = (jnp.arange(dp_size) * cp_size + my_idx) * ff_part
        w_up_own, w_down_own = prepare(starts, splits, w_up, w_down)

        kv_all = after(kv_all, q_t, w_up_own[0])
        cot_far = swap(after(cot, kv_all), 2)
        o_f32, o_t, lse = attn_forward(tab, q_t, kv_all, kv_heads, head_dim)
        o_t = after(o_t, cot_far)

        h_act = (x + dot_tt(o_t, w_o)).astype(BF16)
        h_far = swap(h_act, 2)
        h_near = swap(h_act, 1)
        cot_last = swap(cot_far, 1)
        state = ff_forward(0, cp_size, h_act, cot, w_up_own[0], w_down_own[0], True, ())
        state = ff_forward(1, cp_size, h_near, cot_near, w_up_own[0], w_down_own[0], True, state)
        more = ff_forward(0, cp_size, after(h_act, state[0]), cot, w_up_own[1], w_down_own[1], False, ())
        more = ff_forward(1, cp_size, h_near, cot_near, w_up_own[1], w_down_own[1], False, more)
        h_far = after(h_far, more[0])
        h_last = swap(h_far, 1)
        state = ff_forward(2, cp_size, h_far, cot_far, w_up_own[0], w_down_own[0], True, state)
        act0, grad_u0, h_all, cot_all = ff_forward(3, cp_size, h_last, cot_last, w_up_own[0], w_down_own[0], True, state)
        part = row_major(inv_count * dot_tn(h_all, grad_u0))
        up_rows = [dp_reduce(part)]
        later = after(h_far, part)
        more = ff_forward(2, cp_size, later, cot_far, w_up_own[1], w_down_own[1], False, more)
        act1, grad_u1 = ff_forward(3, cp_size, h_last, cot_last, w_up_own[1], w_down_own[1], False, more)

        part = grad_h_block(3, (grad_u0, grad_u1), w_up_own, [], F32)
        near = swap(part, 1)
        later = after(grad_u1, part)
        part = row_major(inv_count * dot_tn(h_all, later[:, :used[1]]))
        up_rows.append(dp_reduce(part))
        later = after(grad_u1, part)
        part = grad_h_block(2, (grad_u0, later), w_up_own, [near], F32)
        far = swap(part, 2)
        later = after(act0, part)
        part = row_major(inv_count * dot_tn(later, cot_all))
        down_rows = [dp_reduce(part)]
        later = after(act1, part)
        part = row_major(inv_count * dot_tn(later[:, :used[1]], cot_all))
        down_rows.append(dp_reduce(part))
        later = after(grad_u1, part)
        part = grad_h_block(1, (grad_u0, later), w_up_own, [], F32)
        side = swap(part, 1)
        far = after(far, part)

        own_rows = d_model // dev_count
        up_got = []
        for rows_of in up_rows:
            blocks = [lax.dynamic_slice_in_dim(rows_of, (my_idx ^ bits) * own_rows, own_rows, axis=0) for bits in range(cp_size)]
            up_got.append(jnp.stack([blocks[0]] + [row_major(swap(row_major(blocks[bits]), bits))
                                                   for bits in range(1, cp_size)]))
        later = after(grad_u1, part)
        grad_h_bf = grad_h_block(0, (grad_u0, later), w_up_own, [cot, side, far], BF16)
        grad_w_up = spread_columns(my_idx, up_got, splits)

        def block_sum(left, right_t):
            def block(bits):
                return inv_count * dot_tt(own_cols(left, bits), right_t)

            return block

        def first_sends(block):
            parts = block(3), block(1)
            return (swap(parts[0], 1), swap(parts[1], 1)), parts

        def second_send(block, sent):
            part = block(2) + sent[0]
            return swap(part, 2), part

        o_block = block_sum(grad_h_bf, o_t)
        o_sent, parts = first_sends(o_block)
        later = after(grad_h_bf, *parts)
        do_t = dot_tt(w_o, later).astype(BF16)
        o_sent = (after(o_sent[0], do_t), o_sent[1])
        o_far, part = second_send(o_block, o_sent)
        do_t = after(do_t, part)

        def kv_block(dkv):
            blocks = dkv.reshape((cp_size, 2) + dkv.shape[1:])
            return lambda bits: lax.dynamic_index_in_dim(blocks, my_idx ^ bits, axis=0, keepdims=False)

        dq0_t, dkv0 = attn_backward(tab, q_t, do_t, o_f32, lse, kv_all, kv_heads, head_dim, 0)
        kv0_block, q0_block = kv_block(dkv0), block_sum(x, dq0_t)
        kv0_sent, _ = first_sends(kv0_block)
        q0_sent, parts_q = first_sends(q0_block)
        kv0_far, part_kv = second_send(kv0_block, (after(kv0_sent[0], *parts_q), kv0_sent[1]))
        q0_far, part_q = second_send(q0_block, q0_sent)
        do_t = after(do_t, part_kv, part_q)
        dq1_t, dkv1 = attn_backward(tab, q_t, do_t, o_f32, lse, kv_all, kv_heads, head_dim, 1)
        kv1_block, q1_block = kv_block(dkv1), block_sum(x, dq1_t)
        kv1_sent, _ = first_sends(kv1_block)
        q1_sent, parts_q = first_sends(q1_block)
        grad_w_o = dp_reduce(after(o_block(0), *parts_q) + o_sent[1] + o_far)
        kv1_far, part_kv = second_send(kv1_block, kv1_sent)
        q1_far, part_q = second_send(q1_block, q1_sent)
        grad_q0 = dp_reduce(q0_block(0) + q0_sent[1] + q0_far)
        later = after(jnp.concatenate([dq0_t, dq1_t], axis=0), part_q, part_kv)
        grad_x = dot_tt(later, w_q)
        grad_x = grad_h_bf + grad_x
        dkv_parts = [(kv0_block(0) + kv0_sent[1] + kv0_far).astype(BF16), (kv1_block(0) + kv1_sent[1] + kv1_far).astype(BF16)]
        dkv_t = jnp.concatenate([jnp.concatenate([part[0, which], part[1, which]], axis=1)
                                 for which in range(2) for part in dkv_parts], axis=0)
        w_block = block_sum(x, dkv_t)
        w_sent, _ = first_sends(w_block)
        w_far, _ = second_send(w_block, w_sent)
        grad_q1 = dp_reduce(q1_block(0) + q1_sent[1] + q1_far)
        grad_x = grad_x + dot_tt(dkv_t, w_kv)
        grad_kv = dp_reduce(w_block(0) + w_sent[1] + w_far)
        grad_w_down = jnp.concatenate(down_rows, axis=0)

        grad_w_q = jnp.concatenate([grad_q0, grad_q1], axis=1).reshape(own_rows, n_heads, head_dim)
        grad_w_k = grad_kv[:, :kv_width].reshape(own_rows, kv_heads, head_dim)
        grad_w_v = grad_kv[:, kv_width:].reshape(own_rows, kv_heads, head_dim)
        grad_w_o = grad_w_o.reshape(own_rows, n_heads, head_dim)
        return grad_x.astype(BF16)[None], grad_w_q, grad_w_k, grad_w_v, grad_w_o, grad_w_up, grad_w_down

    act_spec = P('dp', 'cp', None)
    rep_three = P(None, None, None)
    rep_two = P(None, None)
    grad_three = P(('dp', 'cp'), None, None)
    grad_two = P(('dp', 'cp'), None)
    return jax.shard_map(per_device, mesh=mesh,
                         in_specs=(act_spec, act_spec, rep_three, rep_three, rep_three, rep_three, rep_two, rep_two),
                         out_specs=(act_spec, grad_three, grad_three, grad_three, grad_three, grad_two, grad_two),
                         check_vma=False)
```

```python
import functools
import math

import jax
import jax.numpy as jnp
from jax import lax
from jax.experimental import pallas as pl
from jax.experimental.pallas import tpu as pltpu
from jax.experimental.layout import Layout, with_layout_constraint
from jax.sharding import PartitionSpec as P


NEG_BIG = -1e30
LOG2E = math.log2(math.e)
F32 = jnp.float32
FF_TILE = 256
BF16 = jnp.bfloat16


def row_major(values):
    return with_layout_constraint(values, Layout(major_to_minor=(0, 1)))


def dot_nn(lhs, rhs):
    return lax.dot_general(lhs, rhs, (((1,), (0,)), ((), ())), preferred_element_type=F32)


def dot_nt(lhs, rhs):
    return lax.dot_general(lhs, rhs, (((1,), (1,)), ((), ())), preferred_element_type=F32)


def dot_tn(lhs, rhs):
    return lax.dot_general(lhs, rhs, (((0,), (0,)), ((), ())), preferred_element_type=F32)


def dot_tt(lhs, rhs):
    return lax.dot_general(lhs, rhs, (((0,), (1,)), ((), ())), preferred_element_type=F32)


def pair_table(my_idx, cp_size):
    steps = jnp.arange(2 * cp_size + 1)
    late = steps > my_idx
    key_block = jnp.where(late, steps - my_idx - 1, steps)
    key_slot = jnp.where(key_block < cp_size, 2 * key_block, 2 * (2 * cp_size - 1 - key_block) + 1)
    last = (steps == my_idx) | (steps == 2 * cp_size)
    first = (steps == 0) | (steps == my_idx + 1)
    return jnp.stack([late, key_slot, last, first]).astype(jnp.int32)


def causal_keep(half):
    keys = lax.broadcasted_iota(jnp.int32, (half, half), 0)
    queries = lax.broadcasted_iota(jnp.int32, (half, half), 1)
    return keys <= queries


def attn_fwd_kernel(group, scale, tab, q_ref, k_ref, v_ref, of_ref, ob_ref, lse_ref, m_ref, l_ref):
    dim = k_ref.shape[1]
    half = q_ref.shape[1] // 2
    factor = scale * LOG2E

    def pair_step(pair, carry):
        cols = pl.ds(pl.multiple_of(tab[0, pair] * half, half), half)
        slot = pl.ds(pl.multiple_of(tab[1, pair] * half, half), half)

        @pl.when(tab[3, pair] == 1)
        def _():
            m_ref[...] = jnp.full(m_ref.shape, NEG_BIG, F32)
            l_ref[...] = jnp.zeros(l_ref.shape, F32)
            of_ref[:, cols] = jnp.zeros((of_ref.shape[0], half), F32)

        def run(masked):
            keys = k_ref[slot, :]
            vals_t = v_ref[slot, :].T
            for head in range(group):
                rows = slice(head * dim, (head + 1) * dim)
                scores = dot_nn(keys, q_ref[rows, cols])
                if masked:
                    scores = jnp.where(causal_keep(half), scores, NEG_BIG)
                old_max = m_ref[head:head + 1, :]
                new_max = jnp.maximum(old_max, jnp.max(scores, axis=0, keepdims=True))
                probs = jnp.exp2((scores - new_max) * factor)
                alpha = jnp.exp2((old_max - new_max) * factor)
                m_ref[head:head + 1, :] = new_max
                l_ref[head:head + 1, :] = alpha * l_ref[head:head + 1, :] + jnp.sum(probs, axis=0, keepdims=True)
                of_ref[rows, cols] = alpha * of_ref[rows, cols] + dot_nn(vals_t, probs.astype(BF16))

        @pl.when(tab[2, pair] == 0)
        def _():
            run(False)

        @pl.when(tab[2, pair] == 1)
        def _():
            run(True)
            lse_ref[0, :, cols] = m_ref[...] * factor + jnp.log2(l_ref[...])
            for head in range(group):
                rows = slice(head * dim, (head + 1) * dim)
                out = of_ref[rows, cols] / l_ref[head:head + 1, :]
                of_ref[rows, cols] = out
                ob_ref[rows, cols] = out.astype(BF16)

        return carry

    lax.fori_loop(0, tab.shape[1], pair_step, 0)


def attn_forward(tab, q_t, kv_all, kv_heads, head_dim):
    width, seq = q_t.shape
    half = seq // 2
    group = width // (kv_heads * head_dim)
    rows = group * head_dim
    n_pairs = tab.shape[1]
    q_spec = pl.BlockSpec((rows, seq), lambda k, t: (k, 0))
    return pl.pallas_call(
        functools.partial(attn_fwd_kernel, group, head_dim ** -0.5),
        grid_spec=pltpu.PrefetchScalarGridSpec(
            num_scalar_prefetch=1,
            grid=(kv_heads,),
            in_specs=[q_spec,
                      pl.BlockSpec((kv_all.shape[0], head_dim), lambda k, t: (0, k)),
                      pl.BlockSpec((kv_all.shape[0], head_dim), lambda k, t: (0, kv_heads + k))],
            out_specs=[q_spec, q_spec,
                       pl.BlockSpec((1, group, seq), lambda k, t: (k, 0, 0))],
            scratch_shapes=[pltpu.VMEM((group, half), F32), pltpu.VMEM((group, half), F32)]),
        out_shape=[jax.ShapeDtypeStruct((width, seq), F32), jax.ShapeDtypeStruct((width, seq), BF16),
                   jax.ShapeDtypeStruct((kv_heads, group, seq), F32)],
        compiler_params=pltpu.CompilerParams(vmem_limit_bytes=56 * 2 ** 20),
        cost_estimate=pl.CostEstimate(flops=4 * width * half * half * n_pairs,
                                      bytes_accessed=12 * width * seq, transcendentals=width // head_dim * half * half * n_pairs),
        name='attn_fwd',
    )(tab, q_t, kv_all, kv_all)


def attn_bwd_kernel(group, scale, tab, q_ref, do_ref, of_ref, lse_ref, k_ref, v_ref, dq_ref, dkv_ref, delta_ref, acc_ref):
    dim = k_ref.shape[1]
    half = q_ref.shape[1] // 2
    factor = scale * LOG2E
    dkv_ref[...] = jnp.zeros(dkv_ref.shape, F32)

    def pair_step(pair, carry):
        cols = pl.ds(pl.multiple_of(tab[0, pair] * half, half), half)
        slot = tab[1, pair]
        slot_rows = pl.ds(pl.multiple_of(slot * half, half), half)

        @pl.when(tab[3, pair] == 1)
        def _():
            acc_ref[...] = jnp.zeros(acc_ref.shape, F32)
            for head in range(group):
                rows = slice(head * dim, (head + 1) * dim)
                delta_ref[head:head + 1, :] = jnp.sum(do_ref[rows, cols].astype(F32) * of_ref[rows, cols], axis=0, keepdims=True)

        def run(masked):
            keys = k_ref[slot_rows, :]
            vals = v_ref[slot_rows, :]
            keys_t = keys.T
            for head in range(group):
                rows = slice(head * dim, (head + 1) * dim)
                q_head = q_ref[rows, cols]
                do_head = do_ref[rows, cols]
                scores = dot_nn(keys, q_head)
                if masked:
                    scores = jnp.where(causal_keep(half), scores, NEG_BIG)
                probs = jnp.exp2(scores * factor - lse_ref[0, head:head + 1, cols])
                grad_p = dot_nn(vals, do_head)
                grad_s = (probs * (grad_p - delta_ref[head:head + 1, :])).astype(BF16)
                dkv_ref[slot, 1] += dot_nt(do_head, probs.astype(BF16))
                dkv_ref[slot, 0] += scale * dot_nt(q_head, grad_s)
                acc_ref[rows, :] += dot_nn(keys_t, grad_s)

        @pl.when(tab[2, pair] == 0)
        def _():
            run(False)

        @pl.when(tab[2, pair] == 1)
        def _():
            run(True)
            dq_ref[:, cols] = (scale * acc_ref[...]).astype(BF16)

        return carry

    lax.fori_loop(0, tab.shape[1], pair_step, 0)


def attn_backward(tab, q_t, do_t, o_f32, lse, kv_all, kv_heads, head_dim, kv_head):
    width, seq = q_t.shape
    half = seq // 2
    group = width // (kv_heads * head_dim)
    rows = group * head_dim
    n_slots = kv_all.shape[0] // half
    n_pairs = tab.shape[1]
    q_spec = pl.BlockSpec((rows, seq), lambda p, t: (kv_head, 0))
    return pl.pallas_call(
        functools.partial(attn_bwd_kernel, group, head_dim ** -0.5),
        grid_spec=pltpu.PrefetchScalarGridSpec(
            num_scalar_prefetch=1,
            grid=(1,),
            in_specs=[q_spec, q_spec, q_spec,
                      pl.BlockSpec((1, group, seq), lambda p, t: (kv_head, 0, 0)),
                      pl.BlockSpec((kv_all.shape[0], head_dim), lambda p, t: (0, kv_head)),
                      pl.BlockSpec((kv_all.shape[0], head_dim), lambda p, t: (0, kv_heads + kv_head))],
            out_specs=[pl.BlockSpec((rows, seq), lambda p, t: (0, 0)),
                       pl.BlockSpec((n_slots, 2, head_dim, half), lambda p, t: (0, 0, 0, 0))],
            scratch_shapes=[pltpu.VMEM((group, half), F32), pltpu.VMEM((rows, half), F32)]),
        out_shape=[jax.ShapeDtypeStruct((rows, seq), BF16),
                   jax.ShapeDtypeStruct((n_slots, 2, head_dim, half), F32)],
        compiler_params=pltpu.CompilerParams(vmem_limit_bytes=56 * 2 ** 20),
        cost_estimate=pl.CostEstimate(flops=10 * rows * half * half * n_pairs,
                                      bytes_accessed=12 * rows * seq, transcendentals=group * half * half * n_pairs),
        name='attn_bwd',
    )(tab, q_t, do_t, o_f32, lse, kv_all, kv_all)


def gelu_parts(values):
    curve = math.sqrt(2 / math.pi)
    square = values * values
    tanh = jnp.tanh(values * (curve + (curve * 0.044715) * square))
    cdf = 0.5 + 0.5 * tanh
    slope = cdf + (0.5 * values) * (1.0 - tanh * tanh) * (curve + (3 * curve * 0.044715) * square)
    return values * cdf, slope


def prep_kernel(segs, parts, idx_ref, *refs):
    n_blocks = sum(seg['tiles'] + 1 for seg in segs)
    blocks, down_ref = refs[:n_blocks], refs[n_blocks]
    n_parts = len(parts)
    up_refs, down_refs = refs[n_blocks + 1:n_blocks + 1 + n_parts], refs[n_blocks + 1 + n_parts:n_blocks + 1 + 2 * n_parts]
    buf_ref, zero_ref, in_sem, out_sem = refs[n_blocks + 1 + 2 * n_parts:]
    step = pl.program_id(0)
    n_own, own_rows = buf_ref.shape[0], buf_ref.shape[1]
    ins = [pltpu.make_async_copy(down_ref.at[pl.ds(pl.multiple_of(idx_ref[0, own], 16), own_rows)], buf_ref.at[own], in_sem.at[own])
           for own in range(n_own)]
    outs = []
    for part, down_out in zip(parts, down_refs):
        for own in range(n_own):
            outs.append(pltpu.make_async_copy(buf_ref.at[own, pl.ds(part['first'], part['rows'])],
                                              down_out.at[pl.ds(own * part['rows'], part['rows'])], out_sem.at[len(outs)]))
        if part['pad']:
            outs.append(pltpu.make_async_copy(zero_ref.at[pl.ds(0, part['pad'])],
                                              down_out.at[pl.ds(n_own * part['rows'], part['pad'])], out_sem.at[len(outs)]))

    @pl.when(step == 0)
    def _():
        zero_ref[...] = jnp.zeros(zero_ref.shape, BF16)
        for copy in ins:
            copy.start()

    @pl.when(step == 1)
    def _():
        for copy in ins:
            copy.wait()
        for copy in outs:
            copy.start()

    rows = blocks[0].shape[0]
    lanes = lax.broadcasted_iota(jnp.int32, (rows, 128), 1)
    cover = [{} for _ in parts]
    pos = 0
    for number, seg in enumerate(segs):
        shift = idx_ref[1, number]
        turned = [pltpu.roll(blocks[pos + tile][...].astype(F32), (128 - shift) % 128, 1) for tile in range(seg['tiles'] + 1)]
        pos += seg['tiles'] + 1
        for tile in range(seg['tiles']):
            cover[seg['part']].setdefault(seg['tile'] + tile, []).append(
                (seg['start'], jnp.where(lanes < 128 - shift, turned[tile], turned[tile + 1])))
    for part, tiles, up_ref in zip(parts, cover, up_refs):
        used = n_own * part['rows']
        for tile in range(up_ref.shape[1] // 128):
            value = jnp.zeros((rows, 128), F32)
            for start, piece in tiles.get(tile, []):
                value = piece if start <= tile * 128 else jnp.where(lanes >= start - tile * 128, piece, value)
            if used < (tile + 1) * 128:
                value = jnp.where(lanes < used - tile * 128, value, 0.0)
            up_ref[:, tile * 128:(tile + 1) * 128] = value.astype(BF16)

    @pl.when(step == pl.num_programs(0) - 1)
    def _():
        for copy in outs:
            copy.wait()


def prepare(starts, splits, w_up, w_down):
    d_model, own_rows = w_up.shape[0], splits[-1][0] + splits[-1][1]
    n_own = starts.shape[0]
    parts = [{'first': first, 'rows': count, 'pad': -(n_own * count) % FF_TILE} for first, count in splits]
    segs, shifts, bases = [], [], []
    for number, part in enumerate(parts):
        for own in range(n_own):
            dest = own * part['rows']
            segs.append({'part': number, 'start': dest, 'tile': dest // 128, 'tiles': -(-(dest % 128 + part['rows']) // 128)})
            source = starts[own] + part['first'] - dest % 128
            shifts.append(source % 128)
            bases.append(source // 128)
    table = jnp.stack([jnp.pad(starts, (0, len(segs) - n_own)), jnp.stack(shifts), jnp.stack(bases)]).astype(jnp.int32)
    rows = 512
    last = w_up.shape[1] // 128 - 1
    in_specs = []
    for number, seg in enumerate(segs):
        for tile in range(seg['tiles'] + 1):
            in_specs.append(pl.BlockSpec((rows, 128), lambda i, t, number=number, tile=tile:
                                         (i, jnp.clip(t[2, number] + tile, 0, last))))
    widths = [n_own * part['rows'] + part['pad'] for part in parts]
    outs = pl.pallas_call(
        functools.partial(prep_kernel, segs, parts),
        grid_spec=pltpu.PrefetchScalarGridSpec(
            num_scalar_prefetch=1,
            grid=(d_model // rows,),
            in_specs=in_specs + [pl.BlockSpec(memory_space=pl.ANY)],
            out_specs=[pl.BlockSpec((rows, width), lambda i, t: (i, 0)) for width in widths]
            + [pl.BlockSpec(memory_space=pl.ANY) for _ in widths],
            scratch_shapes=[pltpu.VMEM((n_own, own_rows, d_model), BF16), pltpu.VMEM((64, d_model), BF16),
                            pltpu.SemaphoreType.DMA((n_own,)), pltpu.SemaphoreType.DMA((n_own * len(parts) + len(parts),))]),
        out_shape=[jax.ShapeDtypeStruct((d_model, width), BF16) for width in widths]
        + [jax.ShapeDtypeStruct((width, d_model), BF16) for width in widths],
        compiler_params=pltpu.CompilerParams(vmem_limit_bytes=56 * 2 ** 20),
        cost_estimate=pl.CostEstimate(flops=8 * d_model * sum(widths), bytes_accessed=9 * d_model * sum(widths), transcendentals=0),
        name='prepare',
    )(table, *([w_up] * len(in_specs)), w_down)
    return outs[:len(parts)], outs[len(parts):]


def ff_kernel(step_rows, copies, first_row, n_pieces, *refs):
    pieces = [(refs[2 * piece], refs[2 * piece + 1]) for piece in range(n_pieces)]
    up_ref, down_ref = refs[2 * n_pieces:2 * n_pieces + 2]
    if copies:
        act_ref, du_ref, h_out, cot_out, sem = refs[-5:]
        moves, row = [], first_row
        for h_ref, cot_ref in pieces:
            rows = pl.ds(row, h_ref.shape[0])
            moves.append(pltpu.make_async_copy(h_ref, h_out.at[rows], sem.at[len(moves)]))
            moves.append(pltpu.make_async_copy(cot_ref, cot_out.at[rows], sem.at[len(moves)]))
            row += h_ref.shape[0]

        @pl.when(pl.program_id(0) == 0)
        def _():
            for move in moves:
                move.start()
    else:
        act_ref, du_ref = refs[-2:]

    base = 0
    for h_ref, cot_ref in pieces:
        for first in range(0, h_ref.shape[0], step_rows):
            rows = slice(first, first + step_rows)
            out_rows = slice(base + first, base + first + step_rows)
            hidden = dot_nn(h_ref[rows, :], up_ref[...])
            grad_act = dot_nt(cot_ref[rows, :], down_ref[...]).astype(BF16).astype(F32)
            act, slope = gelu_parts(hidden)
            act_ref[out_rows, :] = act.astype(BF16)
            du_ref[out_rows, :] = (grad_act * slope).astype(BF16)
        base += h_ref.shape[0]

    if copies:
        @pl.when(pl.program_id(0) == pl.num_programs(0) - 1)
        def _():
            for move in moves:
                move.wait()


def ff_forward(index, count, pieces, up, down, copies, carry):
    tokens = sum(piece[0].shape[0] for piece in pieces)
    d_model, width = up.shape
    tile = FF_TILE
    shapes = [jax.ShapeDtypeStruct((count * tokens, width), BF16)] * 2
    specs = [pl.BlockSpec((tokens, tile), lambda n: (index, n))] * 2
    if copies:
        shapes = shapes + [jax.ShapeDtypeStruct((count * tokens, d_model), BF16)] * 2
        specs = specs + [pl.BlockSpec(memory_space=pl.ANY)] * 2
    in_specs, args = [], []
    for h_blk, cot_blk, row_blk in pieces:
        in_specs += [pl.BlockSpec(h_blk.shape, lambda n: (0, 0)),
                     pl.BlockSpec(h_blk.shape, lambda n, row_blk=row_blk: (row_blk, 0))]
        args += [h_blk, cot_blk]
    carry = list(carry)
    return pl.pallas_call(
        functools.partial(ff_kernel, 512, copies, index * tokens, len(pieces)),
        grid=(width // tile,),
        in_specs=in_specs + [pl.BlockSpec((d_model, tile), lambda n: (0, n)), pl.BlockSpec((tile, d_model), lambda n: (n, 0))]
        + [pl.BlockSpec(memory_space=pl.ANY)] * len(carry),
        out_specs=specs,
        out_shape=shapes,
        input_output_aliases={len(args) + 2 + pos: pos for pos in range(len(carry))},
        scratch_shapes=[pltpu.SemaphoreType.DMA((2 * len(pieces),))] if copies else [],
        compiler_params=pltpu.CompilerParams(vmem_limit_bytes=56 * 2 ** 20),
        cost_estimate=pl.CostEstimate(flops=4 * tokens * d_model * width, bytes_accessed=4 * d_model * (width + 2 * tokens),
                                      transcendentals=tokens * width),
        name='ff_forward',
    )(*args, up, down, *carry)


def grad_h_kernel(n_parts, *refs):
    total = sum(dot_nt(refs[2 * part][...], refs[2 * part + 1][...]) for part in range(n_parts))
    halves = []
    for extra in refs[2 * n_parts:-1]:
        if extra.shape == total.shape:
            total = total + extra[...]
        else:
            halves.append(extra[...])
    if halves:
        total = total + jnp.concatenate(halves, axis=0)
    refs[-1][...] = total.astype(refs[-1].dtype)


def grad_h_block(index, tokens, grad_u, up, extras, dtype):
    d_model = up[0].shape[0]
    width = sum(part.shape[1] for part in up)
    tile = 256
    in_specs, args = [], []
    for left, right in zip(grad_u, up):
        in_specs += [pl.BlockSpec((tokens, left.shape[1]), lambda n: (index, 0)), pl.BlockSpec((tile, right.shape[1]), lambda n: (n, 0))]
        args += [left, right]
    return pl.pallas_call(
        functools.partial(grad_h_kernel, len(up)),
        grid=(d_model // tile,),
        in_specs=in_specs + [pl.BlockSpec((extra.shape[0], tile), lambda n: (0, n)) for extra in extras],
        out_specs=pl.BlockSpec((tokens, tile), lambda n: (0, n)),
        out_shape=jax.ShapeDtypeStruct((tokens, d_model), dtype),
        compiler_params=pltpu.CompilerParams(vmem_limit_bytes=48 * 2 ** 20),
        cost_estimate=pl.CostEstimate(flops=2 * tokens * d_model * width, bytes_accessed=2 * width * (d_model + tokens) + 4 * tokens * d_model,
                                      transcendentals=0),
        name='grad_h',
    )(*args, *extras)


def spread_kernel(splits, idx_ref, *refs):
    got_refs, out_ref = refs[:-1], refs[-1]
    count = got_refs[0].shape[0]
    block = splits[-1][0] + splits[-1][1]
    for dest in range(out_ref.shape[1] // block):
        row, src = dest // count, dest % count
        for (first, cols), got_ref in zip(splits, got_refs):
            out_ref[:, dest * block + first:dest * block + first + cols] = got_ref[idx_ref[0] ^ src, :, row * cols:(row + 1) * cols]


def spread_columns(my_idx, got, splits):
    count, rows = got[0].shape[:2]
    width = count * sum(part.shape[2] for part in got)
    return pl.pallas_call(
        functools.partial(spread_kernel, splits),
        in_specs=[pl.BlockSpec(memory_space=pltpu.SMEM)] + [pl.BlockSpec(memory_space=pltpu.VMEM)] * len(got),
        out_specs=pl.BlockSpec(memory_space=pltpu.VMEM),
        out_shape=jax.ShapeDtypeStruct((rows, width), F32),
        cost_estimate=pl.CostEstimate(flops=rows * width, bytes_accessed=8 * rows * width, transcendentals=0),
        name='spread',
    )(my_idx.reshape(1), *got)


def solution(mesh):
    cp_size = mesh.shape['cp']
    dp_size = mesh.shape['dp']
    dev_count = cp_size * dp_size

    def swap(values, bits):
        return lax.ppermute(values, 'cp', [(src, src ^ bits) for src in range(cp_size)])

    def dp_reduce(grad):
        return lax.psum_scatter(grad, 'dp', scatter_dimension=0, tiled=True)

    def after(value, *earlier):
        return lax.optimization_barrier((value,) + earlier)[0]

    def per_device(x_loc, cot_loc, w_q, w_k, w_v, w_o, w_up, w_down):
        d_model = x_loc.shape[2]
        seq_len = x_loc.shape[1]
        kv_heads, head_dim = w_k.shape[1], w_k.shape[2]
        n_heads = w_q.shape[1]
        group = n_heads // kv_heads
        half = seq_len // 2
        kv_width = kv_heads * head_dim
        rows = group * head_dim
        ff_dim = w_up.shape[1]
        ff_part = ff_dim // dev_count
        my_idx = lax.axis_index('cp')
        x = x_loc[0]
        cot = cot_loc[0]
        w_q = w_q.reshape(d_model, n_heads * head_dim)
        w_o = w_o.reshape(d_model, n_heads * head_dim)
        w_kv = jnp.concatenate([w_k.reshape(d_model, kv_width), w_v.reshape(d_model, kv_width)], axis=1)
        tab = pair_table(my_idx, cp_size)

        inv_count = 1.0 / dev_count

        def own_cols(values, bits):
            width = d_model // dev_count
            return jnp.concatenate([lax.dynamic_slice_in_dim(values, (part * cp_size + (my_idx ^ bits)) * width, width, axis=1)
                                    for part in range(dp_size)], axis=1)

        kv_own = dot_nn(x, w_kv).astype(BF16)
        kv_all = lax.all_gather(kv_own, 'cp', axis=0, tiled=True)
        cot_near = swap(cot, 1)
        q_t = dot_tt(w_q, x).astype(BF16)

        first_part = FF_TILE * (dp_size * ff_part // (2 * FF_TILE)) // dp_size
        splits = ((0, first_part), (first_part, ff_part - first_part))
        used = [dp_size * count for _, count in splits]
        starts = (jnp.arange(dp_size) * cp_size + my_idx) * ff_part
        w_up_own, w_down_own = prepare(starts, splits, w_up, w_down)

        kv_all = after(kv_all, q_t, w_up_own[0])
        cot_far = swap(after(cot, kv_all), 2)
        o_f32, o_t, lse = attn_forward(tab, q_t, kv_all, kv_heads, head_dim)
        o_t = after(o_t, cot_far)

        h_act = (x + dot_tt(o_t, w_o)).astype(BF16)
        h_far = [swap(h_act[:half], 2), swap(h_act[half:], 2)]
        h_near = swap(h_act, 1)
        cot_last = swap(cot_far, 1)

        def ff_call(index, part, pieces, carry, *earlier):
            first = after(pieces[0][0], *earlier) if earlier else pieces[0][0]
            pieces = [(first,) + pieces[0][1:]] + pieces[1:]
            return ff_forward(index, cp_size, pieces, w_up_own[part], w_down_own[part], part == 0, carry)

        own, near = [(h_act, cot, 0)], [(h_near, cot_near, 0)]
        state = ff_call(0, 0, own, ())
        state = ff_call(1, 0, near, state)
        more = ff_call(0, 1, own, (), state[0])

        def remote(piece, *earlier):
            far_piece = after(h_far[piece], *earlier)
            return [(far_piece, cot_far, piece), (swap(far_piece, 1), cot_last, piece)]

        remote0 = remote(0, more[0])
        state = ff_call(2, 0, remote0, state)
        more = ff_call(2, 1, remote0, more, state[0])
        remote1 = remote(1, more[0])

        def grad_h(index, tokens, grads, earlier, extras, dtype):
            later = after(grads[1], earlier)
            return grad_h_block(index, tokens, (grads[0], later), w_up_own, extras, dtype)

        gh_last0 = grad_h(5, half, (state[1], more[1]), more[0], [], F32)
        near0 = swap(gh_last0, 1)
        act0, grad_u0, h_all, cot_all = ff_call(3, 0, remote1, state, gh_last0)
        part = grad_h(4, half, (grad_u0, more[1]), act0, [near0], F32)
        far0 = swap(part, 2)
        later = after(grad_u0, part)
        part = row_major(inv_count * dot_tn(h_all, later))
        up_rows = [dp_reduce(part)]
        more = ff_call(3, 1, remote1, more, part)
        gh_last1 = grad_h(7, half, (grad_u0, more[1]), more[0], [], F32)
        near1 = swap(gh_last1, 1)
        act1, grad_u1 = ff_call(1, 1, near, more, gh_last1)
        part = grad_h(6, half, (grad_u0, grad_u1), act1, [near1], F32)
        far1 = swap(part, 2)
        later = after(grad_u1, part)
        part = row_major(inv_count * dot_tn(h_all, later[:, :used[1]]))
        up_rows.append(dp_reduce(part))
        later = after(act0, part)
        part = row_major(inv_count * dot_tn(later, cot_all))
        down_rows = [dp_reduce(part)]
        part = grad_h(1, seq_len, (grad_u0, grad_u1), part, [], F32)
        side = swap(part, 1)
        later = after(act1, part)
        part = row_major(inv_count * dot_tn(later[:, :used[1]], cot_all))
        down_rows.append(dp_reduce(part))
        far0 = after(far0, part)

        own_rows = d_model // dev_count
        up_got = []
        for rows_of in up_rows:
            blocks = [lax.dynamic_slice_in_dim(rows_of, (my_idx ^ bits) * own_rows, own_rows, axis=0) for bits in range(cp_size)]
            up_got.append(jnp.stack([blocks[0]] + [row_major(swap(row_major(blocks[bits]), bits))
                                                   for bits in range(1, cp_size)]))
        grad_h_bf = grad_h(0, seq_len, (grad_u0, grad_u1), part, [cot, side, far0, far1], BF16)
        grad_w_up = spread_columns(my_idx, up_got, splits)

        def block_sum(left, right_t):
            def block(bits):
                return inv_count * dot_tt(own_cols(left, bits), right_t)

            return block

        def first_sends(block):
            parts = block(3), block(1)
            return (swap(parts[0], 1), swap(parts[1], 1)), parts

        def second_send(block, sent):
            part = block(2) + sent[0]
            return swap(part, 2), part

        o_block = block_sum(grad_h_bf, o_t)
        o_sent, parts = first_sends(o_block)
        later = after(grad_h_bf, *parts)
        do_t = dot_tt(w_o, later).astype(BF16)
        o_sent = (after(o_sent[0], do_t), o_sent[1])
        o_far, part = second_send(o_block, o_sent)
        do_t = after(do_t, part)

        def kv_block(dkv):
            blocks = dkv.reshape((cp_size, 2) + dkv.shape[1:])
            return lambda bits: lax.dynamic_index_in_dim(blocks, my_idx ^ bits, axis=0, keepdims=False)

        dq0_t, dkv0 = attn_backward(tab, q_t, do_t, o_f32, lse, kv_all, kv_heads, head_dim, 0)
        kv0_block, q0_block = kv_block(dkv0), block_sum(x, dq0_t)
        kv0_sent, _ = first_sends(kv0_block)
        q0_sent, parts_q = first_sends(q0_block)
        kv0_far, part_kv = second_send(kv0_block, (after(kv0_sent[0], *parts_q), kv0_sent[1]))
        q0_far, part_q = second_send(q0_block, q0_sent)
        do_t = after(do_t, part_kv, part_q)
        dq1_t, dkv1 = attn_backward(tab, q_t, do_t, o_f32, lse, kv_all, kv_heads, head_dim, 1)
        kv1_block, q1_block = kv_block(dkv1), block_sum(x, dq1_t)
        kv1_sent, _ = first_sends(kv1_block)
        q1_sent, parts_q = first_sends(q1_block)
        sum_o = after(o_block(0), *parts_q) + o_sent[1] + o_far
        kv1_far, part_kv = second_send(kv1_block, kv1_sent)
        q1_far, part_q = second_send(q1_block, q1_sent)
        grad_oq = dp_reduce(jnp.concatenate([sum_o, q0_block(0) + q0_sent[1] + q0_far], axis=1))
        later = after(jnp.concatenate([dq0_t, dq1_t], axis=0), part_q, part_kv)
        grad_x = dot_tt(later, w_q)
        grad_x = grad_h_bf + grad_x
        dkv_parts = [(kv0_block(0) + kv0_sent[1] + kv0_far).astype(BF16), (kv1_block(0) + kv1_sent[1] + kv1_far).astype(BF16)]
        dkv_t = jnp.concatenate([jnp.concatenate([part[0, which], part[1, which]], axis=1)
                                 for which in range(2) for part in dkv_parts], axis=0)
        w_block = block_sum(x, dkv_t)
        w_sent, _ = first_sends(w_block)
        w_far, _ = second_send(w_block, w_sent)
        sum_q1 = q1_block(0) + q1_sent[1] + q1_far
        grad_x = grad_x + dot_tt(dkv_t, w_kv)
        grad_qk = dp_reduce(jnp.concatenate([sum_q1, w_block(0) + w_sent[1] + w_far], axis=1))
        o_width = n_heads * head_dim
        grad_w_down = jnp.concatenate(down_rows, axis=0)

        grad_w_q = jnp.concatenate([grad_oq[:, o_width:], grad_qk[:, :rows]], axis=1).reshape(own_rows, n_heads, head_dim)
        grad_w_k = grad_qk[:, rows:rows + kv_width].reshape(own_rows, kv_heads, head_dim)
        grad_w_v = grad_qk[:, rows + kv_width:].reshape(own_rows, kv_heads, head_dim)
        grad_w_o = grad_oq[:, :o_width].reshape(own_rows, n_heads, head_dim)
        return grad_x.astype(BF16)[None], grad_w_q, grad_w_k, grad_w_v, grad_w_o, grad_w_up, grad_w_down

    act_spec = P('dp', 'cp', None)
    rep_three = P(None, None, None)
    rep_two = P(None, None)
    grad_three = P(('dp', 'cp'), None, None)
    grad_two = P(('dp', 'cp'), None)
    return jax.shard_map(per_device, mesh=mesh,
                         in_specs=(act_spec, act_spec, rep_three, rep_three, rep_three, rep_three, rep_two, rep_two),
                         out_specs=(act_spec, grad_three, grad_three, grad_three, grad_three, grad_two, grad_two),
                         check_vma=False)
```

```python
import functools
import math

import jax
import jax.numpy as jnp
from jax import lax
from jax.experimental import pallas as pl
from jax.experimental.pallas import tpu as pltpu
from jax.experimental.layout import Layout, with_layout_constraint
from jax.sharding import PartitionSpec as P


NEG_BIG = -1e30
LOG2E = math.log2(math.e)
F32 = jnp.float32
FF_TILE = 256
BF16 = jnp.bfloat16


def row_major(values):
    return with_layout_constraint(values, Layout(major_to_minor=(0, 1)))


def dot_nn(lhs, rhs):
    return lax.dot_general(lhs, rhs, (((1,), (0,)), ((), ())), preferred_element_type=F32)


def dot_nt(lhs, rhs):
    return lax.dot_general(lhs, rhs, (((1,), (1,)), ((), ())), preferred_element_type=F32)


def dot_tn(lhs, rhs):
    return lax.dot_general(lhs, rhs, (((0,), (0,)), ((), ())), preferred_element_type=F32)


def dot_tt(lhs, rhs):
    return lax.dot_general(lhs, rhs, (((0,), (1,)), ((), ())), preferred_element_type=F32)


def pair_table(my_idx, cp_size):
    steps = jnp.arange(2 * cp_size + 1)
    late = steps > my_idx
    key_block = jnp.where(late, steps - my_idx - 1, steps)
    key_slot = jnp.where(key_block < cp_size, 2 * key_block, 2 * (2 * cp_size - 1 - key_block) + 1)
    last = (steps == my_idx) | (steps == 2 * cp_size)
    first = (steps == 0) | (steps == my_idx + 1)
    return jnp.stack([late, key_slot, last, first]).astype(jnp.int32)


def causal_keep(half):
    keys = lax.broadcasted_iota(jnp.int32, (half, half), 0)
    queries = lax.broadcasted_iota(jnp.int32, (half, half), 1)
    return keys <= queries


def attn_fwd_kernel(group, scale, tab, q_ref, k_ref, v_ref, of_ref, ob_ref, lse_ref, m_ref, l_ref):
    dim = k_ref.shape[1]
    half = q_ref.shape[1] // 2
    factor = scale * LOG2E

    def pair_step(pair, carry):
        cols = pl.ds(pl.multiple_of(tab[0, pair] * half, half), half)
        slot = pl.ds(pl.multiple_of(tab[1, pair] * half, half), half)

        @pl.when(tab[3, pair] == 1)
        def _():
            m_ref[...] = jnp.full(m_ref.shape, NEG_BIG, F32)
            l_ref[...] = jnp.zeros(l_ref.shape, F32)
            of_ref[:, cols] = jnp.zeros((of_ref.shape[0], half), F32)

        def run(masked):
            keys = k_ref[slot, :]
            vals_t = v_ref[slot, :].T
            for head in range(group):
                rows = slice(head * dim, (head + 1) * dim)
                scores = dot_nn(keys, q_ref[rows, cols])
                if masked:
                    scores = jnp.where(causal_keep(half), scores, NEG_BIG)
                old_max = m_ref[head:head + 1, :]
                new_max = jnp.maximum(old_max, jnp.max(scores, axis=0, keepdims=True))
                probs = jnp.exp2((scores - new_max) * factor)
                alpha = jnp.exp2((old_max - new_max) * factor)
                m_ref[head:head + 1, :] = new_max
                l_ref[head:head + 1, :] = alpha * l_ref[head:head + 1, :] + jnp.sum(probs, axis=0, keepdims=True)
                of_ref[rows, cols] = alpha * of_ref[rows, cols] + dot_nn(vals_t, probs.astype(BF16))

        @pl.when(tab[2, pair] == 0)
        def _():
            run(False)

        @pl.when(tab[2, pair] == 1)
        def _():
            run(True)
            lse_ref[0, :, cols] = m_ref[...] * factor + jnp.log2(l_ref[...])
            for head in range(group):
                rows = slice(head * dim, (head + 1) * dim)
                out = of_ref[rows, cols] / l_ref[head:head + 1, :]
                of_ref[rows, cols] = out
                ob_ref[rows, cols] = out.astype(BF16)

        return carry

    lax.fori_loop(0, tab.shape[1], pair_step, 0)


def attn_forward(tab, q_t, kv_all, kv_heads, head_dim):
    width, seq = q_t.shape
    half = seq // 2
    group = width // (kv_heads * head_dim)
    rows = group * head_dim
    n_pairs = tab.shape[1]
    q_spec = pl.BlockSpec((rows, seq), lambda k, t: (k, 0))
    return pl.pallas_call(
        functools.partial(attn_fwd_kernel, group, head_dim ** -0.5),
        grid_spec=pltpu.PrefetchScalarGridSpec(
            num_scalar_prefetch=1,
            grid=(kv_heads,),
            in_specs=[q_spec,
                      pl.BlockSpec((kv_all.shape[0], head_dim), lambda k, t: (0, k)),
                      pl.BlockSpec((kv_all.shape[0], head_dim), lambda k, t: (0, kv_heads + k))],
            out_specs=[q_spec, q_spec,
                       pl.BlockSpec((1, group, seq), lambda k, t: (k, 0, 0))],
            scratch_shapes=[pltpu.VMEM((group, half), F32), pltpu.VMEM((group, half), F32)]),
        out_shape=[jax.ShapeDtypeStruct((width, seq), F32), jax.ShapeDtypeStruct((width, seq), BF16),
                   jax.ShapeDtypeStruct((kv_heads, group, seq), F32)],
        compiler_params=pltpu.CompilerParams(vmem_limit_bytes=56 * 2 ** 20),
        cost_estimate=pl.CostEstimate(flops=4 * width * half * half * n_pairs,
                                      bytes_accessed=12 * width * seq, transcendentals=width // head_dim * half * half * n_pairs),
    )(tab, q_t, kv_all, kv_all)


def attn_bwd_kernel(group, scale, tab, q_ref, do_ref, of_ref, lse_ref, k_ref, v_ref, dq_ref, dkv_ref, delta_ref, acc_ref):
    dim = k_ref.shape[1]
    half = q_ref.shape[1] // 2
    factor = scale * LOG2E
    dkv_ref[...] = jnp.zeros(dkv_ref.shape, F32)

    def pair_step(pair, carry):
        cols = pl.ds(pl.multiple_of(tab[0, pair] * half, half), half)
        slot = tab[1, pair]
        slot_rows = pl.ds(pl.multiple_of(slot * half, half), half)

        @pl.when(tab[3, pair] == 1)
        def _():
            acc_ref[...] = jnp.zeros(acc_ref.shape, F32)
            for head in range(group):
                rows = slice(head * dim, (head + 1) * dim)
                delta_ref[head:head + 1, :] = jnp.sum(do_ref[rows, cols].astype(F32) * of_ref[rows, cols], axis=0, keepdims=True)

        def run(masked):
            keys = k_ref[slot_rows, :]
            vals = v_ref[slot_rows, :]
            keys_t = keys.T
            for head in range(group):
                rows = slice(head * dim, (head + 1) * dim)
                q_head = q_ref[rows, cols]
                do_head = do_ref[rows, cols]
                scores = dot_nn(keys, q_head)
                if masked:
                    scores = jnp.where(causal_keep(half), scores, NEG_BIG)
                probs = jnp.exp2(scores * factor - lse_ref[0, head:head + 1, cols])
                grad_p = dot_nn(vals, do_head)
                grad_s = (probs * (grad_p - delta_ref[head:head + 1, :])).astype(BF16)
                dkv_ref[slot, 1] += dot_nt(do_head, probs.astype(BF16))
                dkv_ref[slot, 0] += scale * dot_nt(q_head, grad_s)
                acc_ref[rows, :] += dot_nn(keys_t, grad_s)

        @pl.when(tab[2, pair] == 0)
        def _():
            run(False)

        @pl.when(tab[2, pair] == 1)
        def _():
            run(True)
            dq_ref[:, cols] = (scale * acc_ref[...]).astype(BF16)

        return carry

    lax.fori_loop(0, tab.shape[1], pair_step, 0)


def attn_backward(tab, q_t, do_t, o_f32, lse, kv_all, kv_heads, head_dim, kv_head):
    width, seq = q_t.shape
    half = seq // 2
    group = width // (kv_heads * head_dim)
    rows = group * head_dim
    n_slots = kv_all.shape[0] // half
    n_pairs = tab.shape[1]
    q_spec = pl.BlockSpec((rows, seq), lambda p, t: (kv_head, 0))
    return pl.pallas_call(
        functools.partial(attn_bwd_kernel, group, head_dim ** -0.5),
        grid_spec=pltpu.PrefetchScalarGridSpec(
            num_scalar_prefetch=1,
            grid=(1,),
            in_specs=[q_spec, q_spec, q_spec,
                      pl.BlockSpec((1, group, seq), lambda p, t: (kv_head, 0, 0)),
                      pl.BlockSpec((kv_all.shape[0], head_dim), lambda p, t: (0, kv_head)),
                      pl.BlockSpec((kv_all.shape[0], head_dim), lambda p, t: (0, kv_heads + kv_head))],
            out_specs=[pl.BlockSpec((rows, seq), lambda p, t: (0, 0)),
                       pl.BlockSpec((n_slots, 2, head_dim, half), lambda p, t: (0, 0, 0, 0))],
            scratch_shapes=[pltpu.VMEM((group, half), F32), pltpu.VMEM((rows, half), F32)]),
        out_shape=[jax.ShapeDtypeStruct((rows, seq), BF16),
                   jax.ShapeDtypeStruct((n_slots, 2, head_dim, half), F32)],
        compiler_params=pltpu.CompilerParams(vmem_limit_bytes=56 * 2 ** 20),
        cost_estimate=pl.CostEstimate(flops=10 * rows * half * half * n_pairs,
                                      bytes_accessed=12 * rows * seq, transcendentals=group * half * half * n_pairs),
    )(tab, q_t, do_t, o_f32, lse, kv_all, kv_all)


def gelu_parts(values):
    curve = math.sqrt(2 / math.pi)
    square = values * values
    tanh = jnp.tanh(values * (curve + (curve * 0.044715) * square))
    cdf = 0.5 + 0.5 * tanh
    slope = cdf + (0.5 * values) * (1.0 - tanh * tanh) * (curve + (3 * curve * 0.044715) * square)
    return values * cdf, slope


def prep_kernel(segs, parts, idx_ref, *refs):
    n_blocks = sum(seg[3] + 1 for seg in segs)
    blocks, down_ref = refs[:n_blocks], refs[n_blocks]
    n_parts = len(parts)
    up_refs, down_refs = refs[n_blocks + 1:n_blocks + 1 + n_parts], refs[n_blocks + 1 + n_parts:n_blocks + 1 + 2 * n_parts]
    buf_ref, zero_ref, in_sem, out_sem = refs[n_blocks + 1 + 2 * n_parts:]
    step = pl.program_id(0)
    n_own, own_rows = buf_ref.shape[0], buf_ref.shape[1]
    ins = [pltpu.make_async_copy(down_ref.at[pl.ds(pl.multiple_of(idx_ref[0, own], 16), own_rows)], buf_ref.at[own], in_sem.at[own])
           for own in range(n_own)]
    outs = []
    for part, down_out in zip(parts, down_refs):
        for own in range(n_own):
            outs.append(pltpu.make_async_copy(buf_ref.at[own, pl.ds(part[0], part[1])],
                                              down_out.at[pl.ds(own * part[1], part[1])], out_sem.at[len(outs)]))
        if part[2]:
            outs.append(pltpu.make_async_copy(zero_ref.at[pl.ds(0, part[2])],
                                              down_out.at[pl.ds(n_own * part[1], part[2])], out_sem.at[len(outs)]))

    @pl.when(step == 0)
    def _():
        zero_ref[...] = jnp.zeros(zero_ref.shape, BF16)
        for copy in ins:
            copy.start()

    @pl.when(step == 1)
    def _():
        for copy in ins:
            copy.wait()
        for copy in outs:
            copy.start()

    rows = blocks[0].shape[0]
    lanes = lax.broadcasted_iota(jnp.int32, (rows, 128), 1)
    cover = [{} for _ in parts]
    pos = 0
    for number, seg in enumerate(segs):
        shift = idx_ref[1, number]
        turned = [pltpu.roll(blocks[pos + tile][...].astype(F32), (128 - shift) % 128, 1) for tile in range(seg[3] + 1)]
        pos += seg[3] + 1
        for tile in range(seg[3]):
            cover[seg[0]].setdefault(seg[2] + tile, []).append(
                (seg[1], jnp.where(lanes < 128 - shift, turned[tile], turned[tile + 1])))
    for part, tiles, up_ref in zip(parts, cover, up_refs):
        used = n_own * part[1]
        for tile in range(up_ref.shape[1] // 128):
            value = jnp.zeros((rows, 128), F32)
            for start, piece in tiles.get(tile, []):
                value = piece if start <= tile * 128 else jnp.where(lanes >= start - tile * 128, piece, value)
            if used < (tile + 1) * 128:
                value = jnp.where(lanes < used - tile * 128, value, 0.0)
            up_ref[:, tile * 128:(tile + 1) * 128] = value.astype(BF16)

    @pl.when(step == pl.num_programs(0) - 1)
    def _():
        for copy in outs:
            copy.wait()


def prepare(starts, splits, w_up, w_down):
    d_model, own_rows = w_up.shape[0], splits[-1][0] + splits[-1][1]
    n_own = starts.shape[0]
    parts = [(first, count, -(n_own * count) % FF_TILE) for first, count in splits]
    segs, shifts, bases = [], [], []
    for number, part in enumerate(parts):
        for own in range(n_own):
            dest = own * part[1]
            segs.append((number, dest, dest // 128, -(-(dest % 128 + part[1]) // 128)))
            source = starts[own] + part[0] - dest % 128
            shifts.append(source % 128)
            bases.append(source // 128)
    table = jnp.stack([jnp.pad(starts, (0, len(segs) - n_own)), jnp.stack(shifts), jnp.stack(bases)]).astype(jnp.int32)
    rows = 512
    last = w_up.shape[1] // 128 - 1
    in_specs = []
    for number, seg in enumerate(segs):
        for tile in range(seg[3] + 1):
            in_specs.append(pl.BlockSpec((rows, 128), lambda i, t, number=number, tile=tile:
                                         (i, jnp.clip(t[2, number] + tile, 0, last))))
    widths = [n_own * part[1] + part[2] for part in parts]
    outs = pl.pallas_call(
        functools.partial(prep_kernel, segs, parts),
        grid_spec=pltpu.PrefetchScalarGridSpec(
            num_scalar_prefetch=1,
            grid=(d_model // rows,),
            in_specs=in_specs + [pl.BlockSpec(memory_space=pl.ANY)],
            out_specs=[pl.BlockSpec((rows, width), lambda i, t: (i, 0)) for width in widths]
            + [pl.BlockSpec(memory_space=pl.ANY) for _ in widths],
            scratch_shapes=[pltpu.VMEM((n_own, own_rows, d_model), BF16), pltpu.VMEM((64, d_model), BF16),
                            pltpu.SemaphoreType.DMA((n_own,)), pltpu.SemaphoreType.DMA((n_own * len(parts) + len(parts),))]),
        out_shape=[jax.ShapeDtypeStruct((d_model, width), BF16) for width in widths]
        + [jax.ShapeDtypeStruct((width, d_model), BF16) for width in widths],
        compiler_params=pltpu.CompilerParams(vmem_limit_bytes=56 * 2 ** 20),
        cost_estimate=pl.CostEstimate(flops=8 * d_model * sum(widths), bytes_accessed=9 * d_model * sum(widths), transcendentals=0),
    )(table, *([w_up] * len(in_specs)), w_down)
    return outs[:len(parts)], outs[len(parts):]


def ff_kernel(chunk, copies, first_row, cot_rows, tiles, *refs):
    n_pieces = len(cot_rows)
    weights = refs[2 * n_pieces:2 * n_pieces + 2 * len(tiles)]
    h_buf, cot_buf, in_sem, out_sem = refs[-4:]
    n_copied = 2 if copies else 0
    outs = refs[-4 - n_copied - 2 * len(tiles):-4]
    step = pl.program_id(0)
    loads = []
    for piece, cot_row in enumerate(cot_rows):
        for first in range(0, refs[2 * piece].shape[0], chunk):
            number = len(loads)
            rows = pl.ds(number * chunk, chunk)
            loads.append((pltpu.make_async_copy(refs[2 * piece].at[pl.ds(first, chunk)], h_buf.at[rows], in_sem.at[2 * number]),
                          pltpu.make_async_copy(refs[2 * piece + 1].at[pl.ds(cot_row + first, chunk)], cot_buf.at[rows],
                                                in_sem.at[2 * number + 1])))
    moves = []
    if copies:
        rows = pl.ds(first_row, h_buf.shape[0])
        moves = [pltpu.make_async_copy(h_buf, outs[-2].at[rows], out_sem.at[0]),
                 pltpu.make_async_copy(cot_buf, outs[-1].at[rows], out_sem.at[1])]

    @pl.when(step == 0)
    def _():
        for pair in loads:
            for load in pair:
                load.start()

    first_tile = 0
    for part, count in enumerate(tiles):
        up_ref, down_ref = weights[2 * part:2 * part + 2]
        act_ref, du_ref = outs[2 * part:2 * part + 2]

        @pl.when((step >= first_tile) & (step < first_tile + count))
        def _(up_ref=up_ref, down_ref=down_ref, act_ref=act_ref, du_ref=du_ref, part=part):
            for number, pair in enumerate(loads):
                if part == 0:
                    @pl.when(step == 0)
                    def _(pair=pair):
                        for load in pair:
                            load.wait()

                rows = slice(number * chunk, (number + 1) * chunk)
                hidden = dot_nn(h_buf[rows, :], up_ref[...])
                grad_act = dot_nt(cot_buf[rows, :], down_ref[...]).astype(BF16).astype(F32)
                act, slope = gelu_parts(hidden)
                act_ref[rows, :] = act.astype(BF16)
                du_ref[rows, :] = (grad_act * slope).astype(BF16)

        first_tile += count

    if copies:
        @pl.when(step == 1)
        def _():
            for move in moves:
                move.start()

        @pl.when(step == pl.num_programs(0) - 1)
        def _():
            for move in moves:
                move.wait()


def ff_forward(index, count, pieces, ups, downs, copies, carry):
    tokens = sum(piece[0].shape[0] for piece in pieces)
    d_model = ups[0].shape[0]
    tile = FF_TILE
    tiles = [up.shape[1] // tile for up in ups]
    width = sum(up.shape[1] for up in ups)
    chunk = 512
    hbm = pl.BlockSpec(memory_space=pl.ANY)
    shapes, specs, args, in_specs = [], [], [], []
    for h_blk, cot_blk, _ in pieces:
        args += [h_blk, cot_blk]
        in_specs += [hbm, hbm]
    first_tile = 0
    for up, down, n_tiles in zip(ups, downs, tiles):
        def place(n, first_tile=first_tile, n_tiles=n_tiles):
            return jnp.clip(n - first_tile, 0, n_tiles - 1)

        shapes += [jax.ShapeDtypeStruct((count * tokens, up.shape[1]), BF16)] * 2
        specs += [pl.BlockSpec((tokens, tile), lambda n, place=place: (index, place(n)))] * 2
        args += [up, down]
        in_specs += [pl.BlockSpec((d_model, tile), lambda n, place=place: (0, place(n))),
                     pl.BlockSpec((tile, d_model), lambda n, place=place: (place(n), 0))]
        first_tile += n_tiles
    if copies:
        shapes += [jax.ShapeDtypeStruct((count * tokens, d_model), BF16)] * 2
        specs += [hbm, hbm]
    carry = list(carry)
    return pl.pallas_call(
        functools.partial(ff_kernel, chunk, copies, index * tokens, [piece[2] for piece in pieces], tiles),
        grid=(sum(tiles),),
        in_specs=in_specs + [hbm] * len(carry),
        out_specs=specs,
        out_shape=shapes,
        input_output_aliases={len(args) + pos: pos for pos in range(len(carry))},
        scratch_shapes=[pltpu.VMEM((tokens, d_model), BF16)] * 2
        + [pltpu.SemaphoreType.DMA((2 * tokens // chunk,)), pltpu.SemaphoreType.DMA((2,))],
        compiler_params=pltpu.CompilerParams(vmem_limit_bytes=56 * 2 ** 20),
        cost_estimate=pl.CostEstimate(flops=4 * tokens * d_model * width, bytes_accessed=4 * d_model * (width + 2 * tokens),
                                      transcendentals=tokens * width),
    )(*args, *carry)


def grad_h_kernel(n_parts, *refs):
    total = sum(dot_nt(refs[2 * part][...], refs[2 * part + 1][...]) for part in range(n_parts))
    halves = []
    for extra in refs[2 * n_parts:-1]:
        if extra.shape == total.shape:
            total = total + extra[...]
        else:
            halves.append(extra[...])
    if halves:
        total = total + jnp.concatenate(halves, axis=0)
    refs[-1][...] = total.astype(refs[-1].dtype)


def grad_h_block(index, tokens, grad_u, up, extras, dtype):
    d_model = up[0].shape[0]
    width = sum(part.shape[1] for part in up)
    tile = 256
    in_specs, args = [], []
    for left, right in zip(grad_u, up):
        in_specs += [pl.BlockSpec((tokens, left.shape[1]), lambda n: (index, 0)), pl.BlockSpec((tile, right.shape[1]), lambda n: (n, 0))]
        args += [left, right]
    return pl.pallas_call(
        functools.partial(grad_h_kernel, len(up)),
        grid=(d_model // tile,),
        in_specs=in_specs + [pl.BlockSpec((extra.shape[0], tile), lambda n: (0, n)) for extra in extras],
        out_specs=pl.BlockSpec((tokens, tile), lambda n: (0, n)),
        out_shape=jax.ShapeDtypeStruct((tokens, d_model), dtype),
        compiler_params=pltpu.CompilerParams(vmem_limit_bytes=48 * 2 ** 20),
        cost_estimate=pl.CostEstimate(flops=2 * tokens * d_model * width, bytes_accessed=2 * width * (d_model + tokens) + 4 * tokens * d_model,
                                      transcendentals=0),
    )(*args, *extras)


def spread_kernel(splits, idx_ref, *refs):
    got_refs, out_ref = refs[:-1], refs[-1]
    count = got_refs[0].shape[0]
    block = splits[-1][0] + splits[-1][1]
    for dest in range(out_ref.shape[1] // block):
        row, src = dest // count, dest % count
        for (first, cols), got_ref in zip(splits, got_refs):
            out_ref[:, dest * block + first:dest * block + first + cols] = got_ref[idx_ref[0] ^ src, :, row * cols:(row + 1) * cols]


def spread_columns(my_idx, got, splits):
    count, rows = got[0].shape[:2]
    width = count * sum(part.shape[2] for part in got)
    return pl.pallas_call(
        functools.partial(spread_kernel, splits),
        in_specs=[pl.BlockSpec(memory_space=pltpu.SMEM)] + [pl.BlockSpec(memory_space=pltpu.VMEM)] * len(got),
        out_specs=pl.BlockSpec(memory_space=pltpu.VMEM),
        out_shape=jax.ShapeDtypeStruct((rows, width), F32),
        cost_estimate=pl.CostEstimate(flops=rows * width, bytes_accessed=8 * rows * width, transcendentals=0),
    )(my_idx.reshape(1), *got)


def solution(mesh):
    cp_size = mesh.shape['cp']
    dp_size = mesh.shape['dp']
    dev_count = cp_size * dp_size

    def swap(values, bits):
        return lax.ppermute(values, 'cp', [(src, src ^ bits) for src in range(cp_size)])

    def dp_reduce(grad):
        return lax.psum_scatter(grad, 'dp', scatter_dimension=0, tiled=True)

    def after(value, *earlier):
        return lax.optimization_barrier((value,) + earlier)[0]

    def per_device(x_loc, cot_loc, w_q, w_k, w_v, w_o, w_up, w_down):
        d_model = x_loc.shape[2]
        seq_len = x_loc.shape[1]
        kv_heads, head_dim = w_k.shape[1], w_k.shape[2]
        n_heads = w_q.shape[1]
        group = n_heads // kv_heads
        half = seq_len // 2
        kv_width = kv_heads * head_dim
        rows = group * head_dim
        ff_dim = w_up.shape[1]
        ff_part = ff_dim // dev_count
        my_idx = lax.axis_index('cp')
        x = x_loc[0]
        cot = cot_loc[0]
        w_q = w_q.reshape(d_model, n_heads * head_dim)
        w_o = w_o.reshape(d_model, n_heads * head_dim)
        w_kv = jnp.concatenate([w_k.reshape(d_model, kv_width), w_v.reshape(d_model, kv_width)], axis=1)
        tab = pair_table(my_idx, cp_size)

        inv_count = 1.0 / dev_count

        def own_cols(values, bits):
            width = d_model // dev_count
            return jnp.concatenate([lax.dynamic_slice_in_dim(values, (part * cp_size + (my_idx ^ bits)) * width, width, axis=1)
                                    for part in range(dp_size)], axis=1)

        kv_own = dot_nn(x, w_kv).astype(BF16)
        kv_all = lax.all_gather(kv_own, 'cp', axis=0, tiled=True)
        cot_near = swap(cot, 1)
        q_t = dot_tt(w_q, x).astype(BF16)

        first_part = FF_TILE * (dp_size * ff_part // (2 * FF_TILE)) // dp_size
        splits = ((0, first_part), (first_part, ff_part - first_part))
        used = [dp_size * count for _, count in splits]
        starts = (jnp.arange(dp_size) * cp_size + my_idx) * ff_part
        w_up_own, w_down_own = prepare(starts, splits, w_up, w_down)

        kv_all = after(kv_all, q_t, w_up_own[0])
        cot_far = swap(after(cot, kv_all), 2)
        o_f32, o_t, lse = attn_forward(tab, q_t, kv_all, kv_heads, head_dim)

        h_act = (x + dot_tt(o_t, w_o)).astype(BF16)
        h_far = [swap(h_act[:half], 2), swap(h_act[half:], 2)]
        h_near = swap(h_act, 1)
        cot_last = swap(cot_far, 1)

        def ff_call(index, parts, pieces, carry, *earlier):
            first = after(pieces[0][0], *earlier) if earlier else pieces[0][0]
            pieces = [(first,) + pieces[0][1:]] + pieces[1:]
            return ff_forward(index, cp_size, pieces, [w_up_own[part] for part in parts], [w_down_own[part] for part in parts],
                              0 in parts, carry)

        def remote(piece, *earlier):
            far_piece = after(h_far[piece], *earlier)
            return [(far_piece, cot_far, piece * half), (swap(far_piece, 1), cot_last, piece * half)]

        act0, grad_u0, act1, grad_u1, h_all, cot_all = ff_call(0, (0, 1), [(h_act, cot, 0)], ())
        near = [(h_near, cot_near, 0)]
        act0, grad_u0, h_all, cot_all = ff_call(1, (0,), near, (act0, grad_u0, h_all, cot_all), act1)
        block = remote(0, act0)
        act0, grad_u0, act1, grad_u1, h_all, cot_all = ff_call(2, (0, 1), block, (act0, grad_u0, act1, grad_u1, h_all, cot_all))
        block = remote(1, act1)
        act0, grad_u0, h_all, cot_all = ff_call(3, (0,), block, (act0, grad_u0, h_all, cot_all))
        part = row_major(inv_count * dot_tn(h_all, grad_u0))
        up_rows = [dp_reduce(part)]

        def grad_h(index, tokens, earlier, extras, dtype):
            later = after(grad_u1, earlier)
            return grad_h_block(index, tokens, (grad_u0, later), w_up_own, extras, dtype)

        part = grad_h(5, half, part, [], F32)
        near0 = swap(part, 1)
        act1, grad_u1 = ff_call(3, (1,), block, (act1, grad_u1), part)
        part = grad_h(4, half, act1, [near0], F32)
        far0 = swap(part, 2)
        part = grad_h(7, half, part, [], F32)
        near1 = swap(part, 1)
        act1, grad_u1 = ff_call(1, (1,), near, (act1, grad_u1), part)
        later = after(grad_u1, act1)
        part = row_major(inv_count * dot_tn(h_all, later[:, :used[1]]))
        up_rows.append(dp_reduce(part))
        part = grad_h(6, half, part, [near1], F32)
        far1 = swap(part, 2)
        later = after(act0, part)
        part = row_major(inv_count * dot_tn(later, cot_all))
        down_rows = [dp_reduce(part)]
        part = grad_h(1, seq_len, part, [], F32)
        side = swap(part, 1)
        later = after(act1, part)
        part = row_major(inv_count * dot_tn(later[:, :used[1]], cot_all))
        down_rows.append(dp_reduce(part))
        far0 = after(far0, part)

        own_rows = d_model // dev_count
        up_got = []
        for rows_of in up_rows:
            blocks = [lax.dynamic_slice_in_dim(rows_of, (my_idx ^ bits) * own_rows, own_rows, axis=0) for bits in range(cp_size)]
            up_got.append(jnp.stack([blocks[0]] + [row_major(swap(row_major(blocks[bits]), bits))
                                                   for bits in range(1, cp_size)]))
        grad_h_bf = grad_h(0, seq_len, part, [cot, side, far0, far1], BF16)
        grad_w_up = spread_columns(my_idx, up_got, splits)

        def block_sum(left, right_t):
            def block(bits):
                return inv_count * dot_tt(own_cols(left, bits), right_t)

            return block

        def first_sends(block):
            parts = block(3), block(1)
            return (swap(parts[0], 1), swap(parts[1], 1)), parts

        def second_send(block, sent):
            part = block(2) + sent[0]
            return swap(part, 2), part

        o_block = block_sum(grad_h_bf, o_t)
        o_sent, parts = first_sends(o_block)
        later = after(grad_h_bf, *parts)
        do_t = dot_tt(w_o, later).astype(BF16)
        o_sent = (after(o_sent[0], do_t), o_sent[1])
        o_far, part = second_send(o_block, o_sent)
        do_t = after(do_t, part)

        def kv_block(dkv):
            blocks = dkv.reshape((cp_size, 2) + dkv.shape[1:])
            return lambda bits: lax.dynamic_index_in_dim(blocks, my_idx ^ bits, axis=0, keepdims=False)

        dq0_t, dkv0 = attn_backward(tab, q_t, do_t, o_f32, lse, kv_all, kv_heads, head_dim, 0)
        kv0_block, q0_block = kv_block(dkv0), block_sum(x, dq0_t)
        kv0_sent, parts_kv = first_sends(kv0_block)
        q0_sent, parts_q = first_sends(q0_block)
        kv0_far, part_kv = second_send(kv0_block, (after(kv0_sent[0], *parts_q), kv0_sent[1]))
        q0_far, part_q = second_send(q0_block, q0_sent)
        do_t = after(do_t, part_kv, part_q)
        dq1_t, dkv1 = attn_backward(tab, q_t, do_t, o_f32, lse, kv_all, kv_heads, head_dim, 1)
        kv1_block, q1_block = kv_block(dkv1), block_sum(x, dq1_t)
        kv1_sent, parts_kv = first_sends(kv1_block)
        q1_sent, parts_q = first_sends(q1_block)
        kv1_far, part_kv = second_send(kv1_block, (after(kv1_sent[0], *parts_q), kv1_sent[1]))
        q1_far, part_q = second_send(q1_block, (after(q1_sent[0], part_kv), q1_sent[1]))
        o_far = after(o_far, part_q)
        base_o, base_q = o_block(0), q0_block(0)
        sum_o = base_o + o_sent[1] + o_far
        grad_oq = dp_reduce(jnp.concatenate([sum_o, base_q + q0_sent[1] + q0_far], axis=1))
        kv0_own = (kv0_block(0) + kv0_sent[1] + after(kv0_far, part_q)).astype(BF16)
        kv1_own = (kv1_block(0) + kv1_sent[1] + after(kv1_far, kv0_own)).astype(BF16)
        dkv_t = jnp.concatenate([jnp.concatenate([part[0, which], part[1, which]], axis=1)
                                 for which in range(2) for part in (kv0_own, kv1_own)], axis=0)
        w_block = block_sum(x, dkv_t)
        w_sent, parts = first_sends(w_block)
        w_far, part_w = second_send(w_block, w_sent)
        later = after(jnp.concatenate([dq0_t, dq1_t], axis=0), part_w)
        grad_x = dot_tt(later, w_q)
        grad_x = grad_h_bf + grad_x + dot_tt(after(dkv_t, part_w), w_kv)
        sum_q1 = q1_block(0) + q1_sent[1] + q1_far
        grad_qk = dp_reduce(jnp.concatenate([sum_q1, w_block(0) + w_sent[1] + w_far], axis=1))
        o_width = n_heads * head_dim
        grad_w_down = jnp.concatenate(down_rows, axis=0)

        grad_w_q = jnp.concatenate([grad_oq[:, o_width:], grad_qk[:, :rows]], axis=1).reshape(own_rows, n_heads, head_dim)
        grad_w_k = grad_qk[:, rows:rows + kv_width].reshape(own_rows, kv_heads, head_dim)
        grad_w_v = grad_qk[:, rows + kv_width:].reshape(own_rows, kv_heads, head_dim)
        grad_w_o = grad_oq[:, :o_width].reshape(own_rows, n_heads, head_dim)
        return grad_x.astype(BF16)[None], grad_w_q, grad_w_k, grad_w_v, grad_w_o, grad_w_up, grad_w_down

    act_spec = P('dp', 'cp', None)
    rep_three = P(None, None, None)
    rep_two = P(None, None)
    grad_three = P(('dp', 'cp'), None, None)
    grad_two = P(('dp', 'cp'), None)
    return jax.shard_map(per_device, mesh=mesh,
                         in_specs=(act_spec, act_spec, rep_three, rep_three, rep_three, rep_three, rep_two, rep_two),
                         out_specs=(act_spec, grad_three, grad_three, grad_three, grad_three, grad_two, grad_two),
                         check_vma=False)
```

```python
import functools
import math

import jax
import jax.numpy as jnp
from jax import lax
from jax.experimental import pallas as pl
from jax.experimental.pallas import tpu as pltpu
from jax.experimental.layout import Layout, with_layout_constraint
from jax.sharding import PartitionSpec as P


NEG_BIG = -1e30
LOG2E = math.log2(math.e)
F32 = jnp.float32
FF_TILE = 256
FF_ROWS = 512
BF16 = jnp.bfloat16


def row_major(values):
    return with_layout_constraint(values, Layout(major_to_minor=(0, 1)))


def dot_nn(lhs, rhs):
    return lax.dot_general(lhs, rhs, (((1,), (0,)), ((), ())), preferred_element_type=F32)


def dot_nt(lhs, rhs):
    return lax.dot_general(lhs, rhs, (((1,), (1,)), ((), ())), preferred_element_type=F32)


def dot_tn(lhs, rhs):
    return lax.dot_general(lhs, rhs, (((0,), (0,)), ((), ())), preferred_element_type=F32)


def dot_tt(lhs, rhs):
    return lax.dot_general(lhs, rhs, (((0,), (1,)), ((), ())), preferred_element_type=F32)


def pair_table(my_idx, cp_size):
    steps = jnp.arange(2 * cp_size + 1)
    late = steps > my_idx
    key_block = jnp.where(late, steps - my_idx - 1, steps)
    key_slot = jnp.where(key_block < cp_size, 2 * key_block, 2 * (2 * cp_size - 1 - key_block) + 1)
    last = (steps == my_idx) | (steps == 2 * cp_size)
    first = (steps == 0) | (steps == my_idx + 1)
    return jnp.stack([late, key_slot, last, first]).astype(jnp.int32)


def causal_keep(half):
    keys = lax.broadcasted_iota(jnp.int32, (half, half), 0)
    queries = lax.broadcasted_iota(jnp.int32, (half, half), 1)
    return keys <= queries


def attn_fwd_kernel(group, scale, tab, q_ref, k_ref, v_ref, of_ref, ob_ref, lse_ref, m_ref, l_ref, acc_ref):
    dim = k_ref.shape[1]
    half = q_ref.shape[1] // 2
    factor = scale * LOG2E

    def pair_step(pair, carry):
        cols = pl.ds(pl.multiple_of(tab[0, pair] * half, half), half)
        slot = pl.ds(pl.multiple_of(tab[1, pair] * half, half), half)

        @pl.when(tab[3, pair] == 1)
        def _():
            m_ref[...] = jnp.full(m_ref.shape, NEG_BIG, F32)
            l_ref[...] = jnp.zeros(l_ref.shape, F32)
            acc_ref[...] = jnp.zeros(acc_ref.shape, F32)

        def run(masked):
            keys = k_ref[slot, :]
            vals_t = v_ref[slot, :].T

            def scores_of(head):
                scores = dot_nn(keys, q_ref[head * dim:(head + 1) * dim, cols])
                return jnp.where(causal_keep(half), scores, NEG_BIG) if masked else scores

            following = scores_of(0)
            for head in range(group):
                scores = following
                if head + 1 < group:
                    following = scores_of(head + 1)
                rows = slice(head * dim, (head + 1) * dim)
                old_max = m_ref[head:head + 1, :]
                new_max = jnp.maximum(old_max, jnp.max(scores, axis=0, keepdims=True))
                probs = jnp.exp2(scores * factor - new_max * factor)
                alpha = jnp.exp2((old_max - new_max) * factor)
                m_ref[head:head + 1, :] = new_max
                l_ref[head:head + 1, :] = alpha * l_ref[head:head + 1, :] + jnp.sum(probs, axis=0, keepdims=True)
                acc_ref[rows, :] = alpha * acc_ref[rows, :] + dot_nn(vals_t, probs.astype(BF16))

        @pl.when(tab[2, pair] == 0)
        def _():
            run(False)

        @pl.when(tab[2, pair] == 1)
        def _():
            run(True)
            lse_ref[0, :, cols] = m_ref[...] * factor + jnp.log2(l_ref[...])
            for head in range(group):
                rows = slice(head * dim, (head + 1) * dim)
                out = acc_ref[rows, :] / l_ref[head:head + 1, :]
                of_ref[rows, cols] = out
                ob_ref[rows, cols] = out.astype(BF16)

        return carry

    lax.fori_loop(0, tab.shape[1], pair_step, 0)


def attn_forward(tab, q_t, kv_all, kv_heads, head_dim):
    width, seq = q_t.shape
    half = seq // 2
    group = width // (kv_heads * head_dim)
    rows = group * head_dim
    n_pairs = tab.shape[1]
    q_spec = pl.BlockSpec((rows, seq), lambda k, t: (k, 0))
    return pl.pallas_call(
        functools.partial(attn_fwd_kernel, group, head_dim ** -0.5),
        grid_spec=pltpu.PrefetchScalarGridSpec(
            num_scalar_prefetch=1,
            grid=(kv_heads,),
            in_specs=[q_spec,
                      pl.BlockSpec((kv_all.shape[0], head_dim), lambda k, t: (0, k)),
                      pl.BlockSpec((kv_all.shape[0], head_dim), lambda k, t: (0, kv_heads + k))],
            out_specs=[q_spec, q_spec,
                       pl.BlockSpec((1, group, seq), lambda k, t: (k, 0, 0))],
            scratch_shapes=[pltpu.VMEM((group, half), F32), pltpu.VMEM((group, half), F32), pltpu.VMEM((rows, half), F32)]),
        out_shape=[jax.ShapeDtypeStruct((width, seq), F32), jax.ShapeDtypeStruct((width, seq), BF16),
                   jax.ShapeDtypeStruct((kv_heads, group, seq), F32)],
        compiler_params=pltpu.CompilerParams(vmem_limit_bytes=56 * 2 ** 20),
        cost_estimate=pl.CostEstimate(flops=4 * width * half * half * n_pairs,
                                      bytes_accessed=12 * width * seq, transcendentals=width // head_dim * half * half * n_pairs),
    )(tab, q_t, kv_all, kv_all)


def attn_bwd_kernel(group, scale, tab, q_ref, do_ref, of_ref, lse_ref, k_ref, v_ref, dq_ref, dkv_ref, delta_ref, acc_ref):
    dim = k_ref.shape[1]
    half = q_ref.shape[1] // 2
    factor = scale * LOG2E
    dkv_ref[...] = jnp.zeros(dkv_ref.shape, F32)

    def pair_step(pair, carry):
        cols = pl.ds(pl.multiple_of(tab[0, pair] * half, half), half)
        slot = tab[1, pair]
        slot_rows = pl.ds(pl.multiple_of(slot * half, half), half)

        @pl.when(tab[3, pair] == 1)
        def _():
            acc_ref[...] = jnp.zeros(acc_ref.shape, F32)
            for head in range(group):
                rows = slice(head * dim, (head + 1) * dim)
                delta_ref[head:head + 1, :] = jnp.sum(do_ref[rows, cols].astype(F32) * of_ref[rows, cols], axis=0, keepdims=True)

        def run(masked):
            keys = k_ref[slot_rows, :]
            vals = v_ref[slot_rows, :]
            keys_t = keys.T

            def products(head):
                rows = slice(head * dim, (head + 1) * dim)
                scores = dot_nn(keys, q_ref[rows, cols])
                if masked:
                    scores = jnp.where(causal_keep(half), scores, NEG_BIG)
                return scores, dot_nn(vals, do_ref[rows, cols])

            following = products(0)
            grad_v = grad_k = jnp.zeros((dim, half), F32)
            for head in range(group):
                scores, grad_p = following
                if head + 1 < group:
                    following = products(head + 1)
                rows = slice(head * dim, (head + 1) * dim)
                probs = jnp.exp2(scores * factor - lse_ref[0, head:head + 1, cols])
                grad_s = (probs * (grad_p - delta_ref[head:head + 1, :])).astype(BF16)
                grad_v = grad_v + dot_nt(do_ref[rows, cols], probs.astype(BF16))
                grad_k = grad_k + dot_nt(q_ref[rows, cols], grad_s)
                acc_ref[rows, :] += dot_nn(keys_t, grad_s)
            dkv_ref[slot, 1] += grad_v
            dkv_ref[slot, 0] += scale * grad_k

        @pl.when(tab[2, pair] == 0)
        def _():
            run(False)

        @pl.when(tab[2, pair] == 1)
        def _():
            run(True)
            dq_ref[:, cols] = (scale * acc_ref[...]).astype(BF16)

        return carry

    lax.fori_loop(0, tab.shape[1], pair_step, 0)


def attn_backward(tab, q_t, do_t, o_f32, lse, kv_all, kv_heads, head_dim, kv_head):
    width, seq = q_t.shape
    half = seq // 2
    group = width // (kv_heads * head_dim)
    rows = group * head_dim
    n_slots = kv_all.shape[0] // half
    n_pairs = tab.shape[1]
    q_spec = pl.BlockSpec((rows, seq), lambda p, t: (kv_head, 0))
    return pl.pallas_call(
        functools.partial(attn_bwd_kernel, group, head_dim ** -0.5),
        grid_spec=pltpu.PrefetchScalarGridSpec(
            num_scalar_prefetch=1,
            grid=(1,),
            in_specs=[q_spec, q_spec, q_spec,
                      pl.BlockSpec((1, group, seq), lambda p, t: (kv_head, 0, 0)),
                      pl.BlockSpec((kv_all.shape[0], head_dim), lambda p, t: (0, kv_head)),
                      pl.BlockSpec((kv_all.shape[0], head_dim), lambda p, t: (0, kv_heads + kv_head))],
            out_specs=[pl.BlockSpec((rows, seq), lambda p, t: (0, 0)),
                       pl.BlockSpec((n_slots, 2, head_dim, half), lambda p, t: (0, 0, 0, 0))],
            scratch_shapes=[pltpu.VMEM((group, half), F32), pltpu.VMEM((rows, half), F32)]),
        out_shape=[jax.ShapeDtypeStruct((rows, seq), BF16),
                   jax.ShapeDtypeStruct((n_slots, 2, head_dim, half), F32)],
        compiler_params=pltpu.CompilerParams(vmem_limit_bytes=56 * 2 ** 20),
        cost_estimate=pl.CostEstimate(flops=10 * rows * half * half * n_pairs,
                                      bytes_accessed=12 * rows * seq, transcendentals=group * half * half * n_pairs),
    )(tab, q_t, do_t, o_f32, lse, kv_all, kv_all)


def gelu_parts(values):
    curve = math.sqrt(2 / math.pi)
    square = values * values
    tanh = jnp.tanh(values * (curve + (curve * 0.044715) * square))
    cdf = 0.5 + 0.5 * tanh
    slope = cdf + (0.5 * values) * (1.0 - tanh * tanh) * (curve + (3 * curve * 0.044715) * square)
    return values * cdf, slope


def prep_kernel(segs, parts, idx_ref, *refs):
    n_blocks = sum(seg[3] + 1 for seg in segs)
    blocks, down_ref = refs[:n_blocks], refs[n_blocks]
    n_parts = len(parts)
    up_refs, down_refs = refs[n_blocks + 1:n_blocks + 1 + n_parts], refs[n_blocks + 1 + n_parts:n_blocks + 1 + 2 * n_parts]
    buf_ref, zero_ref, in_sem, out_sem = refs[n_blocks + 1 + 2 * n_parts:]
    step = pl.program_id(0)
    n_own, own_rows = buf_ref.shape[0], buf_ref.shape[1]
    ins = [pltpu.make_async_copy(down_ref.at[pl.ds(pl.multiple_of(idx_ref[0, own], 16), own_rows)], buf_ref.at[own], in_sem.at[own])
           for own in range(n_own)]
    outs = []
    for part, down_out in zip(parts, down_refs):
        for own in range(n_own):
            outs.append(pltpu.make_async_copy(buf_ref.at[own, pl.ds(part[0], part[1])],
                                              down_out.at[pl.ds(own * part[1], part[1])], out_sem.at[len(outs)]))
        if part[2]:
            outs.append(pltpu.make_async_copy(zero_ref.at[pl.ds(0, part[2])],
                                              down_out.at[pl.ds(n_own * part[1], part[2])], out_sem.at[len(outs)]))

    @pl.when(step == 0)
    def _():
        zero_ref[...] = jnp.zeros(zero_ref.shape, BF16)
        for copy in ins:
            copy.start()

    @pl.when(step == 1)
    def _():
        for copy in ins:
            copy.wait()
        for copy in outs:
            copy.start()

    rows = blocks[0].shape[0]
    lanes = lax.broadcasted_iota(jnp.int32, (rows, 128), 1)
    cover = [{} for _ in parts]
    pos = 0
    for number, seg in enumerate(segs):
        shift = idx_ref[1, number]
        turned = [pltpu.roll(blocks[pos + tile][...].astype(F32), (128 - shift) % 128, 1) for tile in range(seg[3] + 1)]
        pos += seg[3] + 1
        for tile in range(seg[3]):
            cover[seg[0]].setdefault(seg[2] + tile, []).append(
                (seg[1], jnp.where(lanes < 128 - shift, turned[tile], turned[tile + 1])))
    for part, tiles, up_ref in zip(parts, cover, up_refs):
        used = n_own * part[1]
        for tile in range(up_ref.shape[1] // 128):
            value = jnp.zeros((rows, 128), F32)
            for start, piece in tiles.get(tile, []):
                value = piece if start <= tile * 128 else jnp.where(lanes >= start - tile * 128, piece, value)
            if used < (tile + 1) * 128:
                value = jnp.where(lanes < used - tile * 128, value, 0.0)
            up_ref[:, tile * 128:(tile + 1) * 128] = value.astype(BF16)

    @pl.when(step == pl.num_programs(0) - 1)
    def _():
        for copy in outs:
            copy.wait()


def prepare(starts, splits, w_up, w_down):
    d_model, own_rows = w_up.shape[0], splits[-1][0] + splits[-1][1]
    n_own = starts.shape[0]
    parts = [(first, count, -(n_own * count) % FF_TILE) for first, count in splits]
    segs, shifts, bases = [], [], []
    for number, part in enumerate(parts):
        for own in range(n_own):
            dest = own * part[1]
            segs.append((number, dest, dest // 128, -(-(dest % 128 + part[1]) // 128)))
            source = starts[own] + part[0] - dest % 128
            shifts.append(source % 128)
            bases.append(source // 128)
    table = jnp.stack([jnp.pad(starts, (0, len(segs) - n_own)), jnp.stack(shifts), jnp.stack(bases)]).astype(jnp.int32)
    rows = 512
    last = w_up.shape[1] // 128 - 1
    in_specs = []
    for number, seg in enumerate(segs):
        for tile in range(seg[3] + 1):
            in_specs.append(pl.BlockSpec((rows, 128), lambda i, t, number=number, tile=tile:
                                         (i, jnp.clip(t[2, number] + tile, 0, last))))
    widths = [n_own * part[1] + part[2] for part in parts]
    outs = pl.pallas_call(
        functools.partial(prep_kernel, segs, parts),
        grid_spec=pltpu.PrefetchScalarGridSpec(
            num_scalar_prefetch=1,
            grid=(d_model // rows,),
            in_specs=in_specs + [pl.BlockSpec(memory_space=pl.ANY)],
            out_specs=[pl.BlockSpec((rows, width), lambda i, t: (i, 0)) for width in widths]
            + [pl.BlockSpec(memory_space=pl.ANY) for _ in widths],
            scratch_shapes=[pltpu.VMEM((n_own, own_rows, d_model), BF16), pltpu.VMEM((64, d_model), BF16),
                            pltpu.SemaphoreType.DMA((n_own,)), pltpu.SemaphoreType.DMA((n_own * len(parts) + len(parts),))]),
        out_shape=[jax.ShapeDtypeStruct((d_model, width), BF16) for width in widths]
        + [jax.ShapeDtypeStruct((width, d_model), BF16) for width in widths],
        compiler_params=pltpu.CompilerParams(vmem_limit_bytes=56 * 2 ** 20),
        cost_estimate=pl.CostEstimate(flops=8 * d_model * sum(widths), bytes_accessed=9 * d_model * sum(widths), transcendentals=0),
    )(table, *([w_up] * len(in_specs)), w_down)
    return outs[:len(parts)], outs[len(parts):]


def ff_kernel(step_rows, copies, first_row, n_pieces, *refs):
    pieces = [(refs[2 * piece], refs[2 * piece + 1]) for piece in range(n_pieces)]
    up_ref, down_ref = refs[2 * n_pieces:2 * n_pieces + 2]
    if copies:
        act_ref, du_ref, h_out, cot_out, sem = refs[-5:]
        moves, row = [], first_row
        for h_ref, cot_ref in pieces:
            rows = pl.ds(row, h_ref.shape[0])
            moves.append(pltpu.make_async_copy(h_ref, h_out.at[rows], sem.at[len(moves)]))
            moves.append(pltpu.make_async_copy(cot_ref, cot_out.at[rows], sem.at[len(moves)]))
            row += h_ref.shape[0]

        @pl.when(pl.program_id(0) == 0)
        def _():
            for move in moves:
                move.start()
    else:
        act_ref, du_ref = refs[-2:]

    places, base = [], 0
    for h_ref, cot_ref in pieces:
        places += [(h_ref, cot_ref, first, base + first) for first in range(0, h_ref.shape[0], step_rows)]
        base += h_ref.shape[0]

    def products(h_ref, cot_ref, first, _):
        rows = slice(first, first + step_rows)
        return dot_nn(h_ref[rows, :], up_ref[...]), dot_nt(cot_ref[rows, :], down_ref[...])

    following = products(*places[0])
    for number, place in enumerate(places):
        hidden, grad_act = following
        if number + 1 < len(places):
            following = products(*places[number + 1])
        out_rows = slice(place[3], place[3] + step_rows)
        act, slope = gelu_parts(hidden)
        act_ref[out_rows, :] = act.astype(BF16)
        du_ref[out_rows, :] = (grad_act.astype(BF16).astype(F32) * slope).astype(BF16)

    if copies:
        @pl.when(pl.program_id(0) == pl.num_programs(0) - 1)
        def _():
            for move in moves:
                move.wait()


def ff_forward(index, count, pieces, up, down, copies, carry):
    tokens = sum(piece[0].shape[0] for piece in pieces)
    d_model, width = up.shape
    tile = FF_TILE
    shapes = [jax.ShapeDtypeStruct((count * tokens, width), BF16)] * 2
    specs = [pl.BlockSpec((tokens, tile), lambda n: (index, n))] * 2
    if copies:
        shapes = shapes + [jax.ShapeDtypeStruct((count * tokens, d_model), BF16)] * 2
        specs = specs + [pl.BlockSpec(memory_space=pl.ANY)] * 2
    in_specs, args = [], []
    for h_blk, cot_blk, row_blk in pieces:
        in_specs += [pl.BlockSpec(h_blk.shape, lambda n: (0, 0)),
                     pl.BlockSpec(h_blk.shape, lambda n, row_blk=row_blk: (row_blk, 0))]
        args += [h_blk, cot_blk]
    carry = list(carry)
    return pl.pallas_call(
        functools.partial(ff_kernel, FF_ROWS, copies, index * tokens, len(pieces)),
        grid=(width // tile,),
        in_specs=in_specs + [pl.BlockSpec((d_model, tile), lambda n: (0, n)), pl.BlockSpec((tile, d_model), lambda n: (n, 0))]
        + [pl.BlockSpec(memory_space=pl.ANY)] * len(carry),
        out_specs=specs,
        out_shape=shapes,
        input_output_aliases={len(args) + 2 + pos: pos for pos in range(len(carry))},
        scratch_shapes=[pltpu.SemaphoreType.DMA((2 * len(pieces),))] if copies else [],
        compiler_params=pltpu.CompilerParams(vmem_limit_bytes=56 * 2 ** 20),
        cost_estimate=pl.CostEstimate(flops=4 * tokens * d_model * width, bytes_accessed=4 * d_model * (width + 2 * tokens),
                                      transcendentals=tokens * width),
    )(*args, up, down, *carry)


def grad_h_kernel(n_parts, *refs):
    total = sum(dot_nt(refs[2 * part][...], refs[2 * part + 1][...]) for part in range(n_parts))
    halves = []
    for extra in refs[2 * n_parts:-1]:
        if extra.shape == total.shape:
            total = total + extra[...]
        else:
            halves.append(extra[...])
    if halves:
        total = total + jnp.concatenate(halves, axis=0)
    refs[-1][...] = total.astype(refs[-1].dtype)


def grad_h_block(index, tokens, grad_u, up, extras, dtype):
    d_model = up[0].shape[0]
    width = sum(part.shape[1] for part in up)
    tile = 256
    in_specs, args = [], []
    for left, right in zip(grad_u, up):
        in_specs += [pl.BlockSpec((tokens, left.shape[1]), lambda n: (index, 0)), pl.BlockSpec((tile, right.shape[1]), lambda n: (n, 0))]
        args += [left, right]
    return pl.pallas_call(
        functools.partial(grad_h_kernel, len(up)),
        grid=(d_model // tile,),
        in_specs=in_specs + [pl.BlockSpec((extra.shape[0], tile), lambda n: (0, n)) for extra in extras],
        out_specs=pl.BlockSpec((tokens, tile), lambda n: (0, n)),
        out_shape=jax.ShapeDtypeStruct((tokens, d_model), dtype),
        compiler_params=pltpu.CompilerParams(vmem_limit_bytes=48 * 2 ** 20),
        cost_estimate=pl.CostEstimate(flops=2 * tokens * d_model * width, bytes_accessed=2 * width * (d_model + tokens) + 4 * tokens * d_model,
                                      transcendentals=0),
    )(*args, *extras)


def spread_kernel(splits, idx_ref, *refs):
    got_refs, out_ref = refs[:-1], refs[-1]
    count = got_refs[0].shape[0]
    block = splits[-1][0] + splits[-1][1]
    for dest in range(out_ref.shape[1] // block):
        row, src = dest // count, dest % count
        for (first, cols), got_ref in zip(splits, got_refs):
            out_ref[:, dest * block + first:dest * block + first + cols] = got_ref[idx_ref[0] ^ src, :, row * cols:(row + 1) * cols]


def spread_columns(my_idx, got, splits):
    count, rows = got[0].shape[:2]
    width = count * sum(part.shape[2] for part in got)
    return pl.pallas_call(
        functools.partial(spread_kernel, splits),
        in_specs=[pl.BlockSpec(memory_space=pltpu.SMEM)] + [pl.BlockSpec(memory_space=pltpu.VMEM)] * len(got),
        out_specs=pl.BlockSpec(memory_space=pltpu.VMEM),
        out_shape=jax.ShapeDtypeStruct((rows, width), F32),
        cost_estimate=pl.CostEstimate(flops=rows * width, bytes_accessed=8 * rows * width, transcendentals=0),
    )(my_idx.reshape(1), *got)


def solution(mesh):
    cp_size = mesh.shape['cp']
    dp_size = mesh.shape['dp']
    dev_count = cp_size * dp_size

    def swap(values, bits):
        return lax.ppermute(values, 'cp', [(src, src ^ bits) for src in range(cp_size)])

    def dp_reduce(grad):
        return lax.psum_scatter(grad, 'dp', scatter_dimension=0, tiled=True)

    def after(value, *earlier):
        return lax.optimization_barrier((value,) + earlier)[0]

    def per_device(x_loc, cot_loc, w_q, w_k, w_v, w_o, w_up, w_down):
        d_model = x_loc.shape[2]
        seq_len = x_loc.shape[1]
        kv_heads, head_dim = w_k.shape[1], w_k.shape[2]
        n_heads = w_q.shape[1]
        group = n_heads // kv_heads
        half = seq_len // 2
        kv_width = kv_heads * head_dim
        rows = group * head_dim
        ff_dim = w_up.shape[1]
        ff_part = ff_dim // dev_count
        my_idx = lax.axis_index('cp')
        x = x_loc[0]
        cot = cot_loc[0]
        w_q = w_q.reshape(d_model, n_heads * head_dim)
        w_o = w_o.reshape(d_model, n_heads * head_dim)
        w_kv = jnp.concatenate([w_k.reshape(d_model, kv_width), w_v.reshape(d_model, kv_width)], axis=1)
        tab = pair_table(my_idx, cp_size)

        inv_count = 1.0 / dev_count

        def own_cols(values, bits):
            width = d_model // dev_count
            return jnp.concatenate([lax.dynamic_slice_in_dim(values, (part * cp_size + (my_idx ^ bits)) * width, width, axis=1)
                                    for part in range(dp_size)], axis=1)

        kv_own = dot_nn(x, w_kv).astype(BF16)
        kv_all = lax.all_gather(kv_own, 'cp', axis=0, tiled=True)
        cot_near = swap(cot, 1)
        q_t = dot_tt(w_q, x).astype(BF16)

        first_part = FF_TILE * (dp_size * ff_part // (2 * FF_TILE)) // dp_size
        splits = ((0, first_part), (first_part, ff_part - first_part))
        used = [dp_size * count for _, count in splits]
        starts = (jnp.arange(dp_size) * cp_size + my_idx) * ff_part
        cot_far = swap(after(cot, tab), 2)
        w_up_own, w_down_own = prepare(starts, splits, w_up, w_down)

        kv_all = after(kv_all, q_t, w_up_own[0])
        o_f32, o_t, lse = attn_forward(tab, q_t, kv_all, kv_heads, head_dim)

        h_act = (x + dot_tt(o_t, w_o)).astype(BF16)
        h_far0 = swap(h_act[:half], 2)
        h_near = swap(h_act, 1)

        def ff_call(index, part, pieces, carry, *earlier):
            first = after(pieces[0][0], *earlier) if earlier else pieces[0][0]
            pieces = [(first,) + pieces[0][1:]] + pieces[1:]
            return ff_forward(index, cp_size, pieces, w_up_own[part], w_down_own[part], part == 0, carry)

        def remote(piece, far_piece):
            return [(far_piece, cot_far, piece), (swap(far_piece, 1), cot_last, piece)]

        own, near = [(h_act, cot, 0)], [(h_near, cot_near, 0)]
        state = ff_call(0, 0, own, ())
        h_far1 = swap(after(h_act, state[0])[half:], 2)
        cot_last = swap(after(cot_far, state[0]), 1)
        state = ff_call(1, 0, near, state)
        more = ff_call(0, 1, own, (), state[0])
        block = remote(0, after(h_far0, more[0]))
        state = ff_call(2, 0, block, state)
        act1, grad_u1 = ff_call(2, 1, block, more, state[0])

        def grad_h(index, tokens, earlier, extras, dtype):
            later = after(grad_u1, earlier)
            return grad_h_block(index, tokens, (state[1], later), w_up_own, extras, dtype)

        part = grad_h(5, half, act1, [], F32)
        near0 = swap(part, 1)
        block = remote(1, after(h_far1, act1))
        state = ff_call(3, 0, block, state, part)
        part = grad_h(4, half, state[0], [near0], F32)
        far0 = swap(part, 2)
        act0, grad_u0, h_all, cot_all = state
        later = after(grad_u0, part)
        part = row_major(inv_count * dot_tn(h_all, later))
        up_rows = [dp_reduce(part)]
        act1, grad_u1 = ff_call(3, 1, block, (act1, grad_u1), part)
        part = grad_h(7, half, act1, [], F32)
        near1 = swap(part, 1)
        act1, grad_u1 = ff_call(1, 1, near, (act1, grad_u1), part)
        part = grad_h(6, half, act1, [near1], F32)
        far1 = swap(part, 2)
        later = after(grad_u1, part)
        part = row_major(inv_count * dot_tn(h_all, later[:, :used[1]]))
        up_rows.append(dp_reduce(part))
        later = after(act0, part)
        part = row_major(inv_count * dot_tn(later, cot_all))
        down_rows = [dp_reduce(part)]
        part = grad_h(1, seq_len, part, [], F32)
        side = swap(part, 1)
        later = after(act1, part)
        part = row_major(inv_count * dot_tn(later[:, :used[1]], cot_all))
        down_rows.append(dp_reduce(part))
        far0 = after(far0, part)

        own_rows = d_model // dev_count
        up_got = []
        for rows_of in up_rows:
            blocks = [lax.dynamic_slice_in_dim(rows_of, (my_idx ^ bits) * own_rows, own_rows, axis=0) for bits in range(cp_size)]
            up_got.append(jnp.stack([blocks[0]] + [row_major(swap(row_major(blocks[bits]), bits))
                                                   for bits in range(1, cp_size)]))
        grad_h_bf = grad_h(0, seq_len, part, [cot, side, far0, far1], BF16)
        grad_w_up = spread_columns(my_idx, up_got, splits)

        def block_sum(left, right_t):
            def block(bits):
                return inv_count * dot_tt(own_cols(left, bits), right_t)

            return block

        def first_sends(block):
            parts = block(3), block(1)
            return (swap(parts[0], 1), swap(parts[1], 1)), parts

        def second_send(block, sent):
            part = block(2) + sent[0]
            return swap(part, 2), part

        o_block = block_sum(grad_h_bf, o_t)
        o_sent, parts = first_sends(o_block)
        later = after(grad_h_bf, *parts)
        do_t = dot_tt(w_o, later).astype(BF16)
        o_sent = (after(o_sent[0], do_t), o_sent[1])
        o_far, part = second_send(o_block, o_sent)
        do_t = after(do_t, part)

        def kv_block(dkv):
            blocks = dkv.reshape((cp_size, 2) + dkv.shape[1:])
            return lambda bits: lax.dynamic_index_in_dim(blocks, my_idx ^ bits, axis=0, keepdims=False)

        dq0_t, dkv0 = attn_backward(tab, q_t, do_t, o_f32, lse, kv_all, kv_heads, head_dim, 0)
        kv0_block, q0_block = kv_block(dkv0), block_sum(x, dq0_t)
        kv0_sent, parts_kv = first_sends(kv0_block)
        q0_sent, parts_q = first_sends(q0_block)
        kv0_far, part_kv = second_send(kv0_block, (after(kv0_sent[0], *parts_q), kv0_sent[1]))
        q0_far, part_q = second_send(q0_block, q0_sent)
        do_t = after(do_t, part_kv, part_q)
        dq1_t, dkv1 = attn_backward(tab, q_t, do_t, o_f32, lse, kv_all, kv_heads, head_dim, 1)
        kv1_block, q1_block = kv_block(dkv1), block_sum(x, dq1_t)
        kv1_sent, parts_kv = first_sends(kv1_block)
        q1_sent, parts_q = first_sends(q1_block)
        kv1_far, part_kv = second_send(kv1_block, (after(kv1_sent[0], *parts_q), kv1_sent[1]))
        q1_far, part_q = second_send(q1_block, (after(q1_sent[0], part_kv), q1_sent[1]))
        o_far = after(o_far, part_q)
        base_o, base_q = o_block(0), q0_block(0)
        sum_o = base_o + o_sent[1] + o_far
        grad_oq = dp_reduce(jnp.concatenate([sum_o, base_q + q0_sent[1] + q0_far], axis=1))
        kv0_own = (kv0_block(0) + kv0_sent[1] + after(kv0_far, part_q)).astype(BF16)
        kv1_own = (kv1_block(0) + kv1_sent[1] + after(kv1_far, kv0_own)).astype(BF16)
        dkv_t = jnp.concatenate([jnp.concatenate([part[0, which], part[1, which]], axis=1)
                                 for which in range(2) for part in (kv0_own, kv1_own)], axis=0)
        w_block = block_sum(x, dkv_t)
        w_sent, parts = first_sends(w_block)
        w_far, part_w = second_send(w_block, w_sent)
        later = after(jnp.concatenate([dq0_t, dq1_t], axis=0), part_w)
        grad_x = dot_tt(later, w_q)
        grad_x = grad_h_bf + grad_x + dot_tt(after(dkv_t, part_w), w_kv)
        sum_q1 = q1_block(0) + q1_sent[1] + q1_far
        grad_qk = dp_reduce(jnp.concatenate([sum_q1, w_block(0) + w_sent[1] + w_far], axis=1))
        o_width = n_heads * head_dim
        grad_w_down = jnp.concatenate(down_rows, axis=0)

        grad_w_q = jnp.concatenate([grad_oq[:, o_width:], grad_qk[:, :rows]], axis=1).reshape(own_rows, n_heads, head_dim)
        grad_w_k = grad_qk[:, rows:rows + kv_width].reshape(own_rows, kv_heads, head_dim)
        grad_w_v = grad_qk[:, rows + kv_width:].reshape(own_rows, kv_heads, head_dim)
        grad_w_o = grad_oq[:, :o_width].reshape(own_rows, n_heads, head_dim)
        return grad_x.astype(BF16)[None], grad_w_q, grad_w_k, grad_w_v, grad_w_o, grad_w_up, grad_w_down

    act_spec = P('dp', 'cp', None)
    rep_three = P(None, None, None)
    rep_two = P(None, None)
    grad_three = P(('dp', 'cp'), None, None)
    grad_two = P(('dp', 'cp'), None)
    return jax.shard_map(per_device, mesh=mesh,
                         in_specs=(act_spec, act_spec, rep_three, rep_three, rep_three, rep_three, rep_two, rep_two),
                         out_specs=(act_spec, grad_three, grad_three, grad_three, grad_three, grad_two, grad_two),
                         check_vma=False)
```

```python
import functools
import math

import jax
import jax.numpy as jnp
from jax import lax
from jax.experimental import pallas as pl
from jax.experimental.pallas import tpu as pltpu
from jax.experimental.layout import Layout, with_layout_constraint
from jax.sharding import PartitionSpec as P


NEG_BIG = -1e30
LOG2E = math.log2(math.e)
F32 = jnp.float32
FF_TILE = 256
FF_ROWS = 512
BF16 = jnp.bfloat16


def row_major(values):
    return with_layout_constraint(values, Layout(major_to_minor=(0, 1)))


def dot_nn(lhs, rhs):
    return lax.dot_general(lhs, rhs, (((1,), (0,)), ((), ())), preferred_element_type=F32)


def dot_nt(lhs, rhs):
    return lax.dot_general(lhs, rhs, (((1,), (1,)), ((), ())), preferred_element_type=F32)


def dot_tn(lhs, rhs):
    return lax.dot_general(lhs, rhs, (((0,), (0,)), ((), ())), preferred_element_type=F32)


def dot_tt(lhs, rhs):
    return lax.dot_general(lhs, rhs, (((0,), (1,)), ((), ())), preferred_element_type=F32)


def pair_table(my_idx, cp_size):
    steps = jnp.arange(2 * cp_size + 1)
    late = steps > my_idx
    key_block = jnp.where(late, steps - my_idx - 1, steps)
    key_slot = jnp.where(key_block < cp_size, 2 * key_block, 2 * (2 * cp_size - 1 - key_block) + 1)
    last = (steps == my_idx) | (steps == 2 * cp_size)
    first = (steps == 0) | (steps == my_idx + 1)
    return jnp.stack([late, key_slot, last, first]).astype(jnp.int32)


def causal_keep(half):
    keys = lax.broadcasted_iota(jnp.int32, (half, half), 0)
    queries = lax.broadcasted_iota(jnp.int32, (half, half), 1)
    return keys <= queries


def attn_fwd_kernel(group, scale, tab, q_ref, k_ref, v_ref, of_ref, ob_ref, lse_ref, m_ref, l_ref, acc_ref):
    dim = k_ref.shape[1]
    half = q_ref.shape[1] // 2
    factor = scale * LOG2E

    def pair_step(pair, carry):
        cols = pl.ds(pl.multiple_of(tab[0, pair] * half, half), half)
        slot = pl.ds(pl.multiple_of(tab[1, pair] * half, half), half)

        @pl.when(tab[3, pair] == 1)
        def _():
            m_ref[...] = jnp.full(m_ref.shape, NEG_BIG, F32)
            l_ref[...] = jnp.zeros(l_ref.shape, F32)
            acc_ref[...] = jnp.zeros(acc_ref.shape, F32)

        def run(masked):
            keys = k_ref[slot, :]
            vals_t = v_ref[slot, :].T

            def scores_of(head):
                scores = dot_nn(keys, q_ref[head * dim:(head + 1) * dim, cols])
                return jnp.where(causal_keep(half), scores, NEG_BIG) if masked else scores

            following = scores_of(0)
            for head in range(group):
                scores = following
                if head + 1 < group:
                    following = scores_of(head + 1)
                rows = slice(head * dim, (head + 1) * dim)
                old_max = m_ref[head:head + 1, :]
                new_max = jnp.maximum(old_max, jnp.max(scores, axis=0, keepdims=True))
                probs = jnp.exp2(scores * factor - new_max * factor)
                alpha = jnp.exp2((old_max - new_max) * factor)
                m_ref[head:head + 1, :] = new_max
                l_ref[head:head + 1, :] = alpha * l_ref[head:head + 1, :] + jnp.sum(probs, axis=0, keepdims=True)
                acc_ref[rows, :] = alpha * acc_ref[rows, :] + dot_nn(vals_t, probs.astype(BF16))

        @pl.when(tab[2, pair] == 0)
        def _():
            run(False)

        @pl.when(tab[2, pair] == 1)
        def _():
            run(True)
            lse_ref[0, :, cols] = m_ref[...] * factor + jnp.log2(l_ref[...])
            for head in range(group):
                rows = slice(head * dim, (head + 1) * dim)
                out = acc_ref[rows, :] / l_ref[head:head + 1, :]
                of_ref[rows, cols] = out
                ob_ref[rows, cols] = out.astype(BF16)

        return carry

    lax.fori_loop(0, tab.shape[1], pair_step, 0)


def attn_forward(tab, q_t, kv_all, kv_heads, head_dim):
    width, seq = q_t.shape
    half = seq // 2
    group = width // (kv_heads * head_dim)
    rows = group * head_dim
    n_pairs = tab.shape[1]
    q_spec = pl.BlockSpec((rows, seq), lambda k, t: (k, 0))
    return pl.pallas_call(
        functools.partial(attn_fwd_kernel, group, head_dim ** -0.5),
        grid_spec=pltpu.PrefetchScalarGridSpec(
            num_scalar_prefetch=1,
            grid=(kv_heads,),
            in_specs=[q_spec,
                      pl.BlockSpec((kv_all.shape[0], head_dim), lambda k, t: (0, k)),
                      pl.BlockSpec((kv_all.shape[0], head_dim), lambda k, t: (0, kv_heads + k))],
            out_specs=[q_spec, q_spec,
                       pl.BlockSpec((1, group, seq), lambda k, t: (k, 0, 0))],
            scratch_shapes=[pltpu.VMEM((group, half), F32), pltpu.VMEM((group, half), F32), pltpu.VMEM((rows, half), F32)]),
        out_shape=[jax.ShapeDtypeStruct((width, seq), F32), jax.ShapeDtypeStruct((width, seq), BF16),
                   jax.ShapeDtypeStruct((kv_heads, group, seq), F32)],
        compiler_params=pltpu.CompilerParams(vmem_limit_bytes=56 * 2 ** 20),
        cost_estimate=pl.CostEstimate(flops=4 * width * half * half * n_pairs,
                                      bytes_accessed=12 * width * seq, transcendentals=width // head_dim * half * half * n_pairs),
    )(tab, q_t, kv_all, kv_all)


def attn_bwd_kernel(group, first_head, scale, tab, q_ref, do_ref, of_ref, lse_ref, k_ref, v_ref, *refs):
    dim = k_ref.shape[1]
    half = q_ref.shape[1] // 2
    factor = scale * LOG2E
    dq_ref, dkv_ref, delta_ref, acc_ref = refs[-4:]
    dkv_ref[...] = refs[0][...] if len(refs) > 4 else jnp.zeros(dkv_ref.shape, F32)

    def pair_step(pair, carry):
        cols = pl.ds(pl.multiple_of(tab[0, pair] * half, half), half)
        slot = tab[1, pair]
        slot_rows = pl.ds(pl.multiple_of(slot * half, half), half)

        @pl.when(tab[3, pair] == 1)
        def _():
            acc_ref[...] = jnp.zeros(acc_ref.shape, F32)
            for head in range(group):
                rows = slice(head * dim, (head + 1) * dim)
                delta_ref[head:head + 1, :] = jnp.sum(do_ref[rows, cols].astype(F32) * of_ref[rows, cols], axis=0, keepdims=True)

        def run(masked):
            keys = k_ref[slot_rows, :]
            vals = v_ref[slot_rows, :]
            keys_t = keys.T

            def products(head):
                rows = slice(head * dim, (head + 1) * dim)
                scores = dot_nn(keys, q_ref[rows, cols])
                if masked:
                    scores = jnp.where(causal_keep(half), scores, NEG_BIG)
                return scores, dot_nn(vals, do_ref[rows, cols])

            following = products(0)
            grad_v = grad_k = jnp.zeros((dim, half), F32)
            for head in range(group):
                scores, grad_p = following
                if head + 1 < group:
                    following = products(head + 1)
                rows = slice(head * dim, (head + 1) * dim)
                probs = jnp.exp2(scores * factor - lse_ref[0, first_head + head:first_head + head + 1, cols])
                grad_s = (probs * (grad_p - delta_ref[head:head + 1, :])).astype(BF16)
                grad_v = grad_v + dot_nt(do_ref[rows, cols], probs.astype(BF16))
                grad_k = grad_k + dot_nt(q_ref[rows, cols], grad_s)
                acc_ref[rows, :] += dot_nn(keys_t, grad_s)
            dkv_ref[slot, 1] += grad_v
            dkv_ref[slot, 0] += scale * grad_k

        @pl.when(tab[2, pair] == 0)
        def _():
            run(False)

        @pl.when(tab[2, pair] == 1)
        def _():
            run(True)
            dq_ref[:, cols] = (scale * acc_ref[...]).astype(BF16)

        return carry

    lax.fori_loop(0, tab.shape[1], pair_step, 0)


def attn_backward(tab, q_t, do_t, o_f32, lse, kv_all, kv_heads, head_dim, kv_head, piece=0, n_pieces=1, carry=()):
    width, seq = q_t.shape
    half = seq // 2
    group = width // (kv_heads * head_dim)
    heads = group // n_pieces
    rows = heads * head_dim
    n_slots = kv_all.shape[0] // half
    n_pairs = tab.shape[1]
    q_spec = pl.BlockSpec((rows, seq), lambda p, t: (kv_head * n_pieces + piece, 0))
    dkv_spec = pl.BlockSpec((n_slots, 2, head_dim, half), lambda p, t: (0, 0, 0, 0))
    return pl.pallas_call(
        functools.partial(attn_bwd_kernel, heads, piece * heads, head_dim ** -0.5),
        grid_spec=pltpu.PrefetchScalarGridSpec(
            num_scalar_prefetch=1,
            grid=(1,),
            in_specs=[q_spec, q_spec, q_spec,
                      pl.BlockSpec((1, group, seq), lambda p, t: (kv_head, 0, 0)),
                      pl.BlockSpec((kv_all.shape[0], head_dim), lambda p, t: (0, kv_head)),
                      pl.BlockSpec((kv_all.shape[0], head_dim), lambda p, t: (0, kv_heads + kv_head))]
            + [dkv_spec] * len(carry),
            out_specs=[pl.BlockSpec((rows, seq), lambda p, t: (0, 0)),
                       dkv_spec],
            scratch_shapes=[pltpu.VMEM((heads, half), F32), pltpu.VMEM((rows, half), F32)]),
        out_shape=[jax.ShapeDtypeStruct((rows, seq), BF16),
                   jax.ShapeDtypeStruct((n_slots, 2, head_dim, half), F32)],
        compiler_params=pltpu.CompilerParams(vmem_limit_bytes=56 * 2 ** 20),
        cost_estimate=pl.CostEstimate(flops=10 * rows * half * half * n_pairs,
                                      bytes_accessed=12 * rows * seq, transcendentals=heads * half * half * n_pairs),
    )(tab, q_t, do_t, o_f32, lse, kv_all, kv_all, *carry)


def gelu_parts(values):
    curve = math.sqrt(2 / math.pi)
    square = values * values
    tanh = jnp.tanh(values * (curve + (curve * 0.044715) * square))
    cdf = 0.5 + 0.5 * tanh
    slope = cdf + (0.5 * values) * (1.0 - tanh * tanh) * (curve + (3 * curve * 0.044715) * square)
    return values * cdf, slope


def prep_kernel(segs, parts, idx_ref, *refs):
    n_blocks = sum(seg[3] + 1 for seg in segs)
    blocks, down_ref = refs[:n_blocks], refs[n_blocks]
    n_parts = len(parts)
    up_refs, down_refs = refs[n_blocks + 1:n_blocks + 1 + n_parts], refs[n_blocks + 1 + n_parts:n_blocks + 1 + 2 * n_parts]
    buf_ref, zero_ref, in_sem, out_sem = refs[n_blocks + 1 + 2 * n_parts:]
    step = pl.program_id(0)
    n_own, own_rows = buf_ref.shape[0], buf_ref.shape[1]
    ins = [pltpu.make_async_copy(down_ref.at[pl.ds(pl.multiple_of(idx_ref[0, own], 16), own_rows)], buf_ref.at[own], in_sem.at[own])
           for own in range(n_own)]
    outs = []
    for part, down_out in zip(parts, down_refs):
        for own in range(n_own):
            outs.append(pltpu.make_async_copy(buf_ref.at[own, pl.ds(part[0], part[1])],
                                              down_out.at[pl.ds(own * part[1], part[1])], out_sem.at[len(outs)]))
        if part[2]:
            outs.append(pltpu.make_async_copy(zero_ref.at[pl.ds(0, part[2])],
                                              down_out.at[pl.ds(n_own * part[1], part[2])], out_sem.at[len(outs)]))

    @pl.when(step == 0)
    def _():
        zero_ref[...] = jnp.zeros(zero_ref.shape, BF16)
        for copy in ins:
            copy.start()

    @pl.when(step == 1)
    def _():
        for copy in ins:
            copy.wait()
        for copy in outs:
            copy.start()

    rows = blocks[0].shape[0]
    lanes = lax.broadcasted_iota(jnp.int32, (rows, 128), 1)
    cover = [{} for _ in parts]
    pos = 0
    for number, seg in enumerate(segs):
        shift = idx_ref[1, number]
        turned = [pltpu.roll(blocks[pos + tile][...].astype(F32), (128 - shift) % 128, 1) for tile in range(seg[3] + 1)]
        pos += seg[3] + 1
        for tile in range(seg[3]):
            cover[seg[0]].setdefault(seg[2] + tile, []).append(
                (seg[1], jnp.where(lanes < 128 - shift, turned[tile], turned[tile + 1])))
    for part, tiles, up_ref in zip(parts, cover, up_refs):
        used = n_own * part[1]
        for tile in range(up_ref.shape[1] // 128):
            value = jnp.zeros((rows, 128), F32)
            for start, piece in tiles.get(tile, []):
                value = piece if start <= tile * 128 else jnp.where(lanes >= start - tile * 128, piece, value)
            if used < (tile + 1) * 128:
                value = jnp.where(lanes < used - tile * 128, value, 0.0)
            up_ref[:, tile * 128:(tile + 1) * 128] = value.astype(BF16)

    @pl.when(step == pl.num_programs(0) - 1)
    def _():
        for copy in outs:
            copy.wait()


def prepare(starts, splits, w_up, w_down):
    d_model, own_rows = w_up.shape[0], splits[-1][0] + splits[-1][1]
    n_own = starts.shape[0]
    parts = [(first, count, -(n_own * count) % FF_TILE) for first, count in splits]
    segs, shifts, bases = [], [], []
    for number, part in enumerate(parts):
        for own in range(n_own):
            dest = own * part[1]
            segs.append((number, dest, dest // 128, -(-(dest % 128 + part[1]) // 128)))
            source = starts[own] + part[0] - dest % 128
            shifts.append(source % 128)
            bases.append(source // 128)
    table = jnp.stack([jnp.pad(starts, (0, len(segs) - n_own)), jnp.stack(shifts), jnp.stack(bases)]).astype(jnp.int32)
    rows = 512
    last = w_up.shape[1] // 128 - 1
    in_specs = []
    for number, seg in enumerate(segs):
        for tile in range(seg[3] + 1):
            in_specs.append(pl.BlockSpec((rows, 128), lambda i, t, number=number, tile=tile:
                                         (i, jnp.clip(t[2, number] + tile, 0, last))))
    widths = [n_own * part[1] + part[2] for part in parts]
    outs = pl.pallas_call(
        functools.partial(prep_kernel, segs, parts),
        grid_spec=pltpu.PrefetchScalarGridSpec(
            num_scalar_prefetch=1,
            grid=(d_model // rows,),
            in_specs=in_specs + [pl.BlockSpec(memory_space=pl.ANY)],
            out_specs=[pl.BlockSpec((rows, width), lambda i, t: (i, 0)) for width in widths]
            + [pl.BlockSpec(memory_space=pl.ANY) for _ in widths],
            scratch_shapes=[pltpu.VMEM((n_own, own_rows, d_model), BF16), pltpu.VMEM((64, d_model), BF16),
                            pltpu.SemaphoreType.DMA((n_own,)), pltpu.SemaphoreType.DMA((n_own * len(parts) + len(parts),))]),
        out_shape=[jax.ShapeDtypeStruct((d_model, width), BF16) for width in widths]
        + [jax.ShapeDtypeStruct((width, d_model), BF16) for width in widths],
        compiler_params=pltpu.CompilerParams(vmem_limit_bytes=56 * 2 ** 20),
        cost_estimate=pl.CostEstimate(flops=8 * d_model * sum(widths), bytes_accessed=9 * d_model * sum(widths), transcendentals=0),
    )(table, *([w_up] * len(in_specs)), w_down)
    return outs[:len(parts)], outs[len(parts):]


def ff_kernel(step_rows, copies, first_row, n_pieces, *refs):
    pieces = [(refs[2 * piece], refs[2 * piece + 1]) for piece in range(n_pieces)]
    up_ref, down_ref = refs[2 * n_pieces:2 * n_pieces + 2]
    if copies:
        act_ref, du_ref, h_out, cot_out, sem = refs[-5:]
        moves, row = [], first_row
        for h_ref, cot_ref in pieces:
            rows = pl.ds(row, h_ref.shape[0])
            moves.append(pltpu.make_async_copy(h_ref, h_out.at[rows], sem.at[len(moves)]))
            moves.append(pltpu.make_async_copy(cot_ref, cot_out.at[rows], sem.at[len(moves)]))
            row += h_ref.shape[0]

        @pl.when(pl.program_id(0) == 0)
        def _():
            for move in moves:
                move.start()
    else:
        act_ref, du_ref = refs[-2:]

    places, base = [], 0
    for h_ref, cot_ref in pieces:
        places += [(h_ref, cot_ref, first, base + first) for first in range(0, h_ref.shape[0], step_rows)]
        base += h_ref.shape[0]

    def products(h_ref, cot_ref, first, _):
        rows = slice(first, first + step_rows)
        return dot_nn(h_ref[rows, :], up_ref[...]), dot_nt(cot_ref[rows, :], down_ref[...])

    following = products(*places[0])
    for number, place in enumerate(places):
        hidden, grad_act = following
        if number + 1 < len(places):
            following = products(*places[number + 1])
        out_rows = slice(place[3], place[3] + step_rows)
        act, slope = gelu_parts(hidden)
        act_ref[out_rows, :] = act.astype(BF16)
        du_ref[out_rows, :] = (grad_act.astype(BF16).astype(F32) * slope).astype(BF16)

    if copies:
        @pl.when(pl.program_id(0) == pl.num_programs(0) - 1)
        def _():
            for move in moves:
                move.wait()


def ff_forward(index, count, pieces, up, down, copies, carry):
    tokens = sum(piece[0].shape[0] for piece in pieces)
    d_model, width = up.shape
    tile = FF_TILE
    shapes = [jax.ShapeDtypeStruct((count * tokens, width), BF16)] * 2
    specs = [pl.BlockSpec((tokens, tile), lambda n: (index, n))] * 2
    if copies:
        shapes = shapes + [jax.ShapeDtypeStruct((count * tokens, d_model), BF16)] * 2
        specs = specs + [pl.BlockSpec(memory_space=pl.ANY)] * 2
    in_specs, args = [], []
    for h_blk, cot_blk, row_blk in pieces:
        in_specs += [pl.BlockSpec(h_blk.shape, lambda n: (0, 0)),
                     pl.BlockSpec(h_blk.shape, lambda n, row_blk=row_blk: (row_blk, 0))]
        args += [h_blk, cot_blk]
    carry = list(carry)
    return pl.pallas_call(
        functools.partial(ff_kernel, FF_ROWS, copies, index * tokens, len(pieces)),
        grid=(width // tile,),
        in_specs=in_specs + [pl.BlockSpec((d_model, tile), lambda n: (0, n)), pl.BlockSpec((tile, d_model), lambda n: (n, 0))]
        + [pl.BlockSpec(memory_space=pl.ANY)] * len(carry),
        out_specs=specs,
        out_shape=shapes,
        input_output_aliases={len(args) + 2 + pos: pos for pos in range(len(carry))},
        scratch_shapes=[pltpu.SemaphoreType.DMA((2 * len(pieces),))] if copies else [],
        compiler_params=pltpu.CompilerParams(vmem_limit_bytes=56 * 2 ** 20),
        cost_estimate=pl.CostEstimate(flops=4 * tokens * d_model * width, bytes_accessed=4 * d_model * (width + 2 * tokens),
                                      transcendentals=tokens * width),
    )(*args, up, down, *carry)


def grad_h_kernel(n_parts, *refs):
    total = sum(dot_nt(refs[2 * part][...], refs[2 * part + 1][...]) for part in range(n_parts))
    halves = []
    for extra in refs[2 * n_parts:-1]:
        if extra.shape == total.shape:
            total = total + extra[...]
        else:
            halves.append(extra[...])
    if halves:
        total = total + jnp.concatenate(halves, axis=0)
    refs[-1][...] = total.astype(refs[-1].dtype)


def grad_h_block(index, tokens, grad_u, up, extras, dtype):
    d_model = up[0].shape[0]
    width = sum(part.shape[1] for part in up)
    tile = 256
    in_specs, args = [], []
    for left, right in zip(grad_u, up):
        in_specs += [pl.BlockSpec((tokens, left.shape[1]), lambda n: (index, 0)), pl.BlockSpec((tile, right.shape[1]), lambda n: (n, 0))]
        args += [left, right]
    return pl.pallas_call(
        functools.partial(grad_h_kernel, len(up)),
        grid=(d_model // tile,),
        in_specs=in_specs + [pl.BlockSpec((extra.shape[0], tile), lambda n: (0, n)) for extra in extras],
        out_specs=pl.BlockSpec((tokens, tile), lambda n: (0, n)),
        out_shape=jax.ShapeDtypeStruct((tokens, d_model), dtype),
        compiler_params=pltpu.CompilerParams(vmem_limit_bytes=48 * 2 ** 20),
        cost_estimate=pl.CostEstimate(flops=2 * tokens * d_model * width, bytes_accessed=2 * width * (d_model + tokens) + 4 * tokens * d_model,
                                      transcendentals=0),
    )(*args, *extras)


def spread_kernel(splits, idx_ref, *refs):
    got_refs, out_ref = refs[:-1], refs[-1]
    count = got_refs[0].shape[0]
    block = splits[-1][0] + splits[-1][1]
    for dest in range(out_ref.shape[1] // block):
        row, src = dest // count, dest % count
        for (first, cols), got_ref in zip(splits, got_refs):
            out_ref[:, dest * block + first:dest * block + first + cols] = got_ref[idx_ref[0] ^ src, :, row * cols:(row + 1) * cols]


def spread_columns(my_idx, got, splits):
    count, rows = got[0].shape[:2]
    width = count * sum(part.shape[2] for part in got)
    return pl.pallas_call(
        functools.partial(spread_kernel, splits),
        in_specs=[pl.BlockSpec(memory_space=pltpu.SMEM)] + [pl.BlockSpec(memory_space=pltpu.VMEM)] * len(got),
        out_specs=pl.BlockSpec(memory_space=pltpu.VMEM),
        out_shape=jax.ShapeDtypeStruct((rows, width), F32),
        cost_estimate=pl.CostEstimate(flops=rows * width, bytes_accessed=8 * rows * width, transcendentals=0),
    )(my_idx.reshape(1), *got)


def solution(mesh):
    cp_size = mesh.shape['cp']
    dp_size = mesh.shape['dp']
    dev_count = cp_size * dp_size

    def swap(values, bits):
        return lax.ppermute(values, 'cp', [(src, src ^ bits) for src in range(cp_size)])

    def dp_reduce(grad):
        return lax.psum_scatter(grad, 'dp', scatter_dimension=0, tiled=True)

    def after(value, *earlier):
        return lax.optimization_barrier((value,) + earlier)[0]

    def per_device(x_loc, cot_loc, w_q, w_k, w_v, w_o, w_up, w_down):
        d_model = x_loc.shape[2]
        seq_len = x_loc.shape[1]
        kv_heads, head_dim = w_k.shape[1], w_k.shape[2]
        n_heads = w_q.shape[1]
        group = n_heads // kv_heads
        half = seq_len // 2
        kv_width = kv_heads * head_dim
        rows = group * head_dim
        ff_dim = w_up.shape[1]
        ff_part = ff_dim // dev_count
        my_idx = lax.axis_index('cp')
        x = x_loc[0]
        cot = cot_loc[0]
        w_q = w_q.reshape(d_model, n_heads * head_dim)
        w_o = w_o.reshape(d_model, n_heads * head_dim)
        w_kv = jnp.concatenate([w_k.reshape(d_model, kv_width), w_v.reshape(d_model, kv_width)], axis=1)
        tab = pair_table(my_idx, cp_size)

        inv_count = 1.0 / dev_count

        def own_cols(values, bits):
            width = d_model // dev_count
            return jnp.concatenate([lax.dynamic_slice_in_dim(values, (part * cp_size + (my_idx ^ bits)) * width, width, axis=1)
                                    for part in range(dp_size)], axis=1)

        kv_own = dot_nn(x, w_kv).astype(BF16)
        kv_all = lax.all_gather(kv_own, 'cp', axis=0, tiled=True)
        cot_near = swap(cot, 1)

        first_part = FF_TILE * (dp_size * ff_part // (2 * FF_TILE)) // dp_size
        splits = ((0, first_part), (first_part, ff_part - first_part))
        used = [dp_size * count for _, count in splits]
        starts = (jnp.arange(dp_size) * cp_size + my_idx) * ff_part
        w_up_own, w_down_own = prepare(starts, splits, w_up, w_down)
        cot_far = swap(after(cot, w_up_own[0]), 2)
        later = after(x, w_up_own[0])
        q_t = dot_tt(w_q, later).astype(BF16)

        kv_all = after(kv_all, q_t, w_up_own[0])
        o_f32, o_t, lse = attn_forward(tab, q_t, kv_all, kv_heads, head_dim)

        h_act = (x + dot_tt(o_t, w_o)).astype(BF16)
        h_far0 = swap(h_act[:half], 2)
        h_near = swap(h_act, 1)
        o_near = swap(o_t, 1)

        def ff_call(index, part, pieces, carry, *earlier):
            first = after(pieces[0][0], *earlier) if earlier else pieces[0][0]
            pieces = [(first,) + pieces[0][1:]] + pieces[1:]
            return ff_forward(index, cp_size, pieces, w_up_own[part], w_down_own[part], part == 0, carry)

        def remote(piece, far_piece):
            return [(far_piece, cot_far, piece), (swap(far_piece, 1), cot_last, piece)]

        own, near = [(h_act, cot, 0)], [(h_near, cot_near, 0)]
        state = ff_call(0, 0, own, ())
        h_far1 = swap(after(h_act, state[0])[half:], 2)
        cot_last = swap(after(cot_far, state[0]), 1)
        state = ff_call(1, 0, near, state)
        more = ff_call(0, 1, own, (), state[0])
        block = remote(0, after(h_far0, more[0]))
        state = ff_call(2, 0, block, state)
        act1, grad_u1 = ff_call(2, 1, block, more, state[0])

        def grad_h(index, tokens, earlier, extras, dtype):
            later = after(grad_u1, earlier)
            return grad_h_block(index, tokens, (state[1], later), w_up_own, extras, dtype)

        h_far1 = after(h_far1, act1)
        block = remote(1, h_far1)
        o_far = swap(after(o_t, h_far1), 2)
        state = ff_call(3, 0, block, state, act1)
        o_last = swap(o_far, 1)
        act0, grad_u0, h_all, cot_all = state
        part = row_major(inv_count * dot_tn(h_all, grad_u0))
        up_rows = [dp_reduce(part)]
        part = grad_h(5, half, part, [], F32)
        near0 = swap(part, 1)
        act1, grad_u1 = ff_call(3, 1, block, (act1, grad_u1), part)
        part = grad_h(4, half, act1, [near0], F32)
        far0 = swap(part, 2)
        act1, grad_u1 = ff_call(1, 1, near, (act1, grad_u1), part)
        part = grad_h(7, half, act1, [], F32)
        near1 = swap(part, 1)
        later = after(grad_u1, part)
        part = row_major(inv_count * dot_tn(h_all, later[:, :used[1]]))
        up_rows.append(dp_reduce(part))
        part = grad_h(6, half, part, [near1], F32)
        far1 = swap(part, 2)
        later = after(act0, part)
        part = row_major(inv_count * dot_tn(later, cot_all))
        down_rows = [dp_reduce(part)]
        part = grad_h(1, seq_len, part, [], F32)
        side = swap(part, 1)
        later = after(act1, part)
        part = row_major(inv_count * dot_tn(later[:, :used[1]], cot_all))
        down_rows.append(dp_reduce(part))
        far0 = after(far0, part)

        own_rows = d_model // dev_count
        up_got = []
        for rows_of in up_rows:
            blocks = [lax.dynamic_slice_in_dim(rows_of, (my_idx ^ bits) * own_rows, own_rows, axis=0) for bits in range(cp_size)]
            up_got.append(jnp.stack([blocks[0]] + [row_major(swap(row_major(blocks[bits]), bits))
                                                   for bits in range(1, cp_size)]))
        grad_h_bf = grad_h(0, seq_len, part, [cot, side, far0, far1], BF16)
        grad_w_up = spread_columns(my_idx, up_got, splits)

        def block_sum(left, right_t):
            def block(bits):
                return inv_count * dot_tt(own_cols(left, bits), right_t)

            return block

        def first_sends(block):
            parts = block(3), block(1)
            return (swap(parts[0], 1), swap(parts[1], 1)), parts

        def second_send(block, sent):
            part = block(2) + sent[0]
            return swap(part, 2), part

        mine = [own_cols(grad_h_bf, bits) for bits in range(cp_size)]
        mine = [mine[0]] + [swap(mine[bits], bits) for bits in range(1, cp_size)]
        do_t = dot_tt(w_o, grad_h_bf).astype(BF16)

        def kv_block(dkv):
            blocks = dkv.reshape((cp_size, 2) + dkv.shape[1:])
            return lambda bits: lax.dynamic_index_in_dim(blocks, my_idx ^ bits, axis=0, keepdims=False)

        dq0_t, dkv0 = attn_backward(tab, q_t, do_t, o_f32, lse, kv_all, kv_heads, head_dim, 0)
        kv0_block, q0_block = kv_block(dkv0), block_sum(x, dq0_t)
        kv0_sent, parts_kv = first_sends(kv0_block)
        q0_sent, parts_q = first_sends(q0_block)
        kv0_far, part_kv = second_send(kv0_block, (after(kv0_sent[0], *parts_q), kv0_sent[1]))
        q0_far, part_q = second_send(q0_block, q0_sent)
        do_t = after(do_t, part_kv, part_q)
        dq1_t, dkv1 = attn_backward(tab, q_t, do_t, o_f32, lse, kv_all, kv_heads, head_dim, 1, 0, 2)
        q1_block = block_sum(x, dq1_t)
        q1_sent, parts_q = first_sends(q1_block)
        base_q = q0_block(0)
        sum_o = sum(dot_tt(cols, rows_t) for cols, rows_t in zip(mine, (o_t, o_near, o_far, o_last))) * inv_count
        q1_far, part_q = second_send(q1_block, (after(q1_sent[0], sum_o, base_q), q1_sent[1]))
        do_t = after(do_t, part_q, *parts_q)
        dq2_t, dkv1 = attn_backward(tab, q_t, do_t, o_f32, lse, kv_all, kv_heads, head_dim, 1, 1, 2, (dkv1,))
        kv1_block, q2_block = kv_block(dkv1), block_sum(x, dq2_t)
        kv1_sent, parts_kv = first_sends(kv1_block)
        q2_sent, parts_q = first_sends(q2_block)
        kv1_far, part_kv = second_send(kv1_block, (after(kv1_sent[0], *parts_q), kv1_sent[1]))
        q2_far, part_q = second_send(q2_block, (after(q2_sent[0], part_kv), q2_sent[1]))
        q0_far = after(q0_far, part_q)
        sum_q0 = base_q + q0_sent[1] + q0_far
        grad_oq = dp_reduce(jnp.concatenate([sum_o, sum_q0], axis=1))
        kv0_own = (kv0_block(0) + kv0_sent[1] + after(kv0_far, part_q)).astype(BF16)
        kv1_own = (kv1_block(0) + kv1_sent[1] + after(kv1_far, kv0_own)).astype(BF16)
        dkv_t = jnp.concatenate([jnp.concatenate([part[0, which], part[1, which]], axis=1)
                                 for which in range(2) for part in (kv0_own, kv1_own)], axis=0)
        w_block = block_sum(x, dkv_t)
        w_sent, _ = first_sends(w_block)
        w_far, part_w = second_send(w_block, w_sent)
        later = jnp.concatenate([after(dq0_t, part_w), dq1_t, dq2_t], axis=0)
        grad_x = dot_tt(later, w_q)
        grad_x = grad_h_bf + grad_x + dot_tt(after(dkv_t, part_w), w_kv)
        sum_q1 = q1_block(0) + q1_sent[1] + after(q1_far, part_w)
        sum_q2 = q2_block(0) + q2_sent[1] + after(q2_far, part_w)
        grad_qk = dp_reduce(jnp.concatenate([sum_q1, sum_q2, w_block(0) + w_sent[1] + w_far], axis=1))
        grad_w_down = jnp.concatenate(down_rows, axis=0)
        o_width = n_heads * head_dim

        grad_w_q = jnp.concatenate([grad_oq[:, o_width:], grad_qk[:, :rows]], axis=1).reshape(own_rows, n_heads, head_dim)
        grad_w_k = grad_qk[:, rows:rows + kv_width].reshape(own_rows, kv_heads, head_dim)
        grad_w_v = grad_qk[:, rows + kv_width:].reshape(own_rows, kv_heads, head_dim)
        grad_w_o = grad_oq[:, :o_width].reshape(own_rows, n_heads, head_dim)
        return grad_x.astype(BF16)[None], grad_w_q, grad_w_k, grad_w_v, grad_w_o, grad_w_up, grad_w_down

    act_spec = P('dp', 'cp', None)
    rep_three = P(None, None, None)
    rep_two = P(None, None)
    grad_three = P(('dp', 'cp'), None, None)
    grad_two = P(('dp', 'cp'), None)
    return jax.shard_map(per_device, mesh=mesh,
                         in_specs=(act_spec, act_spec, rep_three, rep_three, rep_three, rep_three, rep_two, rep_two),
                         out_specs=(act_spec, grad_three, grad_three, grad_three, grad_three, grad_two, grad_two),
                         check_vma=False)
```

```python
import functools
import math

import jax
import jax.numpy as jnp
from jax import lax
from jax.experimental import pallas as pl
from jax.experimental.pallas import tpu as pltpu
from jax.experimental.layout import Layout, with_layout_constraint
from jax.sharding import PartitionSpec as P


NEG_BIG = -1e30
LOG2E = math.log2(math.e)
F32 = jnp.float32
FF_TILE = 256
FF_ROWS = 512
BF16 = jnp.bfloat16


def row_major(values):
    return with_layout_constraint(values, Layout(major_to_minor=(0, 1)))


def dot_nn(lhs, rhs):
    return lax.dot_general(lhs, rhs, (((1,), (0,)), ((), ())), preferred_element_type=F32)


def dot_nt(lhs, rhs):
    return lax.dot_general(lhs, rhs, (((1,), (1,)), ((), ())), preferred_element_type=F32)


def dot_tn(lhs, rhs):
    return lax.dot_general(lhs, rhs, (((0,), (0,)), ((), ())), preferred_element_type=F32)


def dot_tt(lhs, rhs):
    return lax.dot_general(lhs, rhs, (((0,), (1,)), ((), ())), preferred_element_type=F32)


def pair_table(my_idx, cp_size):
    steps = jnp.arange(2 * cp_size + 1)
    late = steps > my_idx
    key_block = jnp.where(late, steps - my_idx - 1, steps)
    key_slot = jnp.where(key_block < cp_size, 2 * key_block, 2 * (2 * cp_size - 1 - key_block) + 1)
    last = (steps == my_idx) | (steps == 2 * cp_size)
    first = (steps == 0) | (steps == my_idx + 1)
    return jnp.stack([late, key_slot, last, first]).astype(jnp.int32)


def causal_keep(half):
    keys = lax.broadcasted_iota(jnp.int32, (half, half), 0)
    queries = lax.broadcasted_iota(jnp.int32, (half, half), 1)
    return keys <= queries


def attn_fwd_kernel(group, scale, tab, q_ref, k_ref, v_ref, of_ref, ob_ref, lse_ref, m_ref, l_ref, acc_ref):
    dim = k_ref.shape[1]
    half = q_ref.shape[1] // 2
    factor = scale * LOG2E

    def pair_step(pair, carry):
        cols = pl.ds(pl.multiple_of(tab[0, pair] * half, half), half)
        slot = pl.ds(pl.multiple_of(tab[1, pair] * half, half), half)

        @pl.when(tab[3, pair] == 1)
        def _():
            m_ref[...] = jnp.full(m_ref.shape, NEG_BIG, F32)
            l_ref[...] = jnp.zeros(l_ref.shape, F32)
            acc_ref[...] = jnp.zeros(acc_ref.shape, F32)

        def run(masked):
            keys = k_ref[slot, :]
            vals_t = v_ref[slot, :].T

            def scores_of(head):
                scores = dot_nn(keys, q_ref[head * dim:(head + 1) * dim, cols])
                return jnp.where(causal_keep(half), scores, NEG_BIG) if masked else scores

            following = scores_of(0)
            for head in range(group):
                scores = following
                if head + 1 < group:
                    following = scores_of(head + 1)
                rows = slice(head * dim, (head + 1) * dim)
                old_max = m_ref[head:head + 1, :]
                new_max = jnp.maximum(old_max, jnp.max(scores, axis=0, keepdims=True))
                probs = jnp.exp2(scores * factor - new_max * factor)
                alpha = jnp.exp2((old_max - new_max) * factor)
                m_ref[head:head + 1, :] = new_max
                l_ref[head:head + 1, :] = alpha * l_ref[head:head + 1, :] + jnp.sum(probs, axis=0, keepdims=True)
                acc_ref[rows, :] = alpha * acc_ref[rows, :] + dot_nn(vals_t, probs.astype(BF16))

        @pl.when(tab[2, pair] == 0)
        def _():
            run(False)

        @pl.when(tab[2, pair] == 1)
        def _():
            run(True)
            lse_ref[0, :, cols] = m_ref[...] * factor + jnp.log2(l_ref[...])
            for head in range(group):
                rows = slice(head * dim, (head + 1) * dim)
                out = acc_ref[rows, :] / l_ref[head:head + 1, :]
                of_ref[rows, cols] = out
                ob_ref[rows, cols] = out.astype(BF16)

        return carry

    lax.fori_loop(0, tab.shape[1], pair_step, 0)


def attn_forward(tab, q_t, kv_all, kv_heads, head_dim):
    width, seq = q_t.shape
    half = seq // 2
    group = width // (kv_heads * head_dim)
    rows = group * head_dim
    n_pairs = tab.shape[1]
    q_spec = pl.BlockSpec((rows, seq), lambda k, t: (k, 0))
    return pl.pallas_call(
        functools.partial(attn_fwd_kernel, group, head_dim ** -0.5),
        grid_spec=pltpu.PrefetchScalarGridSpec(
            num_scalar_prefetch=1,
            grid=(kv_heads,),
            in_specs=[q_spec,
                      pl.BlockSpec((kv_all.shape[0], head_dim), lambda k, t: (0, k)),
                      pl.BlockSpec((kv_all.shape[0], head_dim), lambda k, t: (0, kv_heads + k))],
            out_specs=[q_spec, q_spec,
                       pl.BlockSpec((1, group, seq), lambda k, t: (k, 0, 0))],
            scratch_shapes=[pltpu.VMEM((group, half), F32), pltpu.VMEM((group, half), F32), pltpu.VMEM((rows, half), F32)]),
        out_shape=[jax.ShapeDtypeStruct((width, seq), F32), jax.ShapeDtypeStruct((width, seq), BF16),
                   jax.ShapeDtypeStruct((kv_heads, group, seq), F32)],
        compiler_params=pltpu.CompilerParams(vmem_limit_bytes=56 * 2 ** 20),
        cost_estimate=pl.CostEstimate(flops=4 * width * half * half * n_pairs,
                                      bytes_accessed=12 * width * seq, transcendentals=width // head_dim * half * half * n_pairs),
    )(tab, q_t, kv_all, kv_all)


def attn_bwd_kernel(group, first_head, scale, tab, q_ref, do_ref, of_ref, lse_ref, k_ref, v_ref, *refs):
    dim = k_ref.shape[1]
    half = q_ref.shape[1] // 2
    factor = scale * LOG2E
    dq_ref, dkv_ref, delta_ref, acc_ref = refs[-4:]
    dkv_ref[...] = refs[0][...] if len(refs) > 4 else jnp.zeros(dkv_ref.shape, F32)

    def pair_step(pair, carry):
        cols = pl.ds(pl.multiple_of(tab[0, pair] * half, half), half)
        slot = tab[1, pair]
        slot_rows = pl.ds(pl.multiple_of(slot * half, half), half)

        @pl.when(tab[3, pair] == 1)
        def _():
            acc_ref[...] = jnp.zeros(acc_ref.shape, F32)
            for head in range(group):
                rows = slice(head * dim, (head + 1) * dim)
                delta_ref[head:head + 1, :] = jnp.sum(do_ref[rows, cols].astype(F32) * of_ref[rows, cols], axis=0, keepdims=True)

        def run(masked):
            keys = k_ref[slot_rows, :]
            vals = v_ref[slot_rows, :]
            keys_t = keys.T

            def products(head):
                rows = slice(head * dim, (head + 1) * dim)
                scores = dot_nn(keys, q_ref[rows, cols])
                if masked:
                    scores = jnp.where(causal_keep(half), scores, NEG_BIG)
                return scores, dot_nn(vals, do_ref[rows, cols])

            following = products(0)
            grad_v = grad_k = jnp.zeros((dim, half), F32)
            for head in range(group):
                scores, grad_p = following
                if head + 1 < group:
                    following = products(head + 1)
                rows = slice(head * dim, (head + 1) * dim)
                probs = jnp.exp2(scores * factor - lse_ref[0, first_head + head:first_head + head + 1, cols])
                grad_s = (probs * (grad_p - delta_ref[head:head + 1, :])).astype(BF16)
                grad_v = grad_v + dot_nt(do_ref[rows, cols], probs.astype(BF16))
                grad_k = grad_k + dot_nt(q_ref[rows, cols], grad_s)
                acc_ref[rows, :] += dot_nn(keys_t, grad_s)
            dkv_ref[slot, 1] += grad_v
            dkv_ref[slot, 0] += scale * grad_k

        @pl.when(tab[2, pair] == 0)
        def _():
            run(False)

        @pl.when(tab[2, pair] == 1)
        def _():
            run(True)
            dq_ref[:, cols] = (scale * acc_ref[...]).astype(BF16)

        return carry

    lax.fori_loop(0, tab.shape[1], pair_step, 0)


def attn_backward(tab, q_t, do_t, o_f32, lse, kv_all, kv_heads, head_dim, kv_head, piece=0, n_pieces=1, carry=()):
    width, seq = q_t.shape
    half = seq // 2
    group = width // (kv_heads * head_dim)
    heads = group // n_pieces
    rows = heads * head_dim
    n_slots = kv_all.shape[0] // half
    n_pairs = tab.shape[1]
    q_spec = pl.BlockSpec((rows, seq), lambda p, t: (kv_head * n_pieces + piece, 0))
    dkv_spec = pl.BlockSpec((n_slots, 2, head_dim, half), lambda p, t: (0, 0, 0, 0))
    return pl.pallas_call(
        functools.partial(attn_bwd_kernel, heads, piece * heads, head_dim ** -0.5),
        grid_spec=pltpu.PrefetchScalarGridSpec(
            num_scalar_prefetch=1,
            grid=(1,),
            in_specs=[q_spec, q_spec, q_spec,
                      pl.BlockSpec((1, group, seq), lambda p, t: (kv_head, 0, 0)),
                      pl.BlockSpec((kv_all.shape[0], head_dim), lambda p, t: (0, kv_head)),
                      pl.BlockSpec((kv_all.shape[0], head_dim), lambda p, t: (0, kv_heads + kv_head))]
            + [dkv_spec] * len(carry),
            out_specs=[pl.BlockSpec((rows, seq), lambda p, t: (0, 0)),
                       dkv_spec],
            scratch_shapes=[pltpu.VMEM((heads, half), F32), pltpu.VMEM((rows, half), F32)]),
        out_shape=[jax.ShapeDtypeStruct((rows, seq), BF16),
                   jax.ShapeDtypeStruct((n_slots, 2, head_dim, half), F32)],
        compiler_params=pltpu.CompilerParams(vmem_limit_bytes=56 * 2 ** 20),
        cost_estimate=pl.CostEstimate(flops=10 * rows * half * half * n_pairs,
                                      bytes_accessed=12 * rows * seq, transcendentals=heads * half * half * n_pairs),
    )(tab, q_t, do_t, o_f32, lse, kv_all, kv_all, *carry)


def gelu_parts(values):
    curve = math.sqrt(2 / math.pi)
    square = values * values
    tanh = jnp.tanh(values * (curve + (curve * 0.044715) * square))
    cdf = 0.5 + 0.5 * tanh
    slope = cdf + (0.5 * values) * (1.0 - tanh * tanh) * (curve + (3 * curve * 0.044715) * square)
    return values * cdf, slope


def prep_kernel(segs, parts, idx_ref, *refs):
    n_blocks = sum(seg[3] + 1 for seg in segs)
    blocks, down_ref = refs[:n_blocks], refs[n_blocks]
    n_parts = len(parts)
    up_refs, down_refs = refs[n_blocks + 1:n_blocks + 1 + n_parts], refs[n_blocks + 1 + n_parts:n_blocks + 1 + 2 * n_parts]
    buf_ref, zero_ref, in_sem, out_sem = refs[n_blocks + 1 + 2 * n_parts:]
    step = pl.program_id(0)
    n_own, own_rows = buf_ref.shape[0], buf_ref.shape[1]
    ins = [pltpu.make_async_copy(down_ref.at[pl.ds(pl.multiple_of(idx_ref[0, own], 16), own_rows)], buf_ref.at[own], in_sem.at[own])
           for own in range(n_own)]
    outs = []
    for part, down_out in zip(parts, down_refs):
        for own in range(n_own):
            outs.append(pltpu.make_async_copy(buf_ref.at[own, pl.ds(part[0], part[1])],
                                              down_out.at[pl.ds(own * part[1], part[1])], out_sem.at[len(outs)]))
        if part[2]:
            outs.append(pltpu.make_async_copy(zero_ref.at[pl.ds(0, part[2])],
                                              down_out.at[pl.ds(n_own * part[1], part[2])], out_sem.at[len(outs)]))

    @pl.when(step == 0)
    def _():
        zero_ref[...] = jnp.zeros(zero_ref.shape, BF16)
        for copy in ins:
            copy.start()

    @pl.when(step == 1)
    def _():
        for copy in ins:
            copy.wait()
        for copy in outs:
            copy.start()

    rows = blocks[0].shape[0]
    lanes = lax.broadcasted_iota(jnp.int32, (rows, 128), 1)
    cover = [{} for _ in parts]
    pos = 0
    for number, seg in enumerate(segs):
        shift = idx_ref[1, number]
        turned = [pltpu.roll(blocks[pos + tile][...].astype(F32), (128 - shift) % 128, 1) for tile in range(seg[3] + 1)]
        pos += seg[3] + 1
        for tile in range(seg[3]):
            cover[seg[0]].setdefault(seg[2] + tile, []).append(
                (seg[1], jnp.where(lanes < 128 - shift, turned[tile], turned[tile + 1])))
    for part, tiles, up_ref in zip(parts, cover, up_refs):
        used = n_own * part[1]
        for tile in range(up_ref.shape[1] // 128):
            value = jnp.zeros((rows, 128), F32)
            for start, piece in tiles.get(tile, []):
                value = piece if start <= tile * 128 else jnp.where(lanes >= start - tile * 128, piece, value)
            if used < (tile + 1) * 128:
                value = jnp.where(lanes < used - tile * 128, value, 0.0)
            up_ref[:, tile * 128:(tile + 1) * 128] = value.astype(BF16)

    @pl.when(step == pl.num_programs(0) - 1)
    def _():
        for copy in outs:
            copy.wait()


def prepare(starts, splits, w_up, w_down):
    d_model, own_rows = w_up.shape[0], splits[-1][0] + splits[-1][1]
    n_own = starts.shape[0]
    parts = [(first, count, -(n_own * count) % FF_TILE) for first, count in splits]
    segs, shifts, bases = [], [], []
    for number, part in enumerate(parts):
        for own in range(n_own):
            dest = own * part[1]
            segs.append((number, dest, dest // 128, -(-(dest % 128 + part[1]) // 128)))
            source = starts[own] + part[0] - dest % 128
            shifts.append(source % 128)
            bases.append(source // 128)
    table = jnp.stack([jnp.pad(starts, (0, len(segs) - n_own)), jnp.stack(shifts), jnp.stack(bases)]).astype(jnp.int32)
    rows = 512
    last = w_up.shape[1] // 128 - 1
    in_specs = []
    for number, seg in enumerate(segs):
        for tile in range(seg[3] + 1):
            in_specs.append(pl.BlockSpec((rows, 128), lambda i, t, number=number, tile=tile:
                                         (i, jnp.clip(t[2, number] + tile, 0, last))))
    widths = [n_own * part[1] + part[2] for part in parts]
    outs = pl.pallas_call(
        functools.partial(prep_kernel, segs, parts),
        grid_spec=pltpu.PrefetchScalarGridSpec(
            num_scalar_prefetch=1,
            grid=(d_model // rows,),
            in_specs=in_specs + [pl.BlockSpec(memory_space=pl.ANY)],
            out_specs=[pl.BlockSpec((rows, width), lambda i, t: (i, 0)) for width in widths]
            + [pl.BlockSpec(memory_space=pl.ANY) for _ in widths],
            scratch_shapes=[pltpu.VMEM((n_own, own_rows, d_model), BF16), pltpu.VMEM((64, d_model), BF16),
                            pltpu.SemaphoreType.DMA((n_own,)), pltpu.SemaphoreType.DMA((n_own * len(parts) + len(parts),))]),
        out_shape=[jax.ShapeDtypeStruct((d_model, width), BF16) for width in widths]
        + [jax.ShapeDtypeStruct((width, d_model), BF16) for width in widths],
        compiler_params=pltpu.CompilerParams(vmem_limit_bytes=56 * 2 ** 20),
        cost_estimate=pl.CostEstimate(flops=8 * d_model * sum(widths), bytes_accessed=9 * d_model * sum(widths), transcendentals=0),
    )(table, *([w_up] * len(in_specs)), w_down)
    return outs[:len(parts)], outs[len(parts):]


def ff_kernel(step_rows, copies, first_row, n_pieces, *refs):
    pieces = [(refs[2 * piece], refs[2 * piece + 1]) for piece in range(n_pieces)]
    up_ref, down_ref = refs[2 * n_pieces:2 * n_pieces + 2]
    if copies:
        act_ref, du_ref, h_out, cot_out, sem = refs[-5:]
        moves, row = [], first_row
        for h_ref, cot_ref in pieces:
            rows = pl.ds(row, h_ref.shape[0])
            moves.append(pltpu.make_async_copy(h_ref, h_out.at[rows], sem.at[len(moves)]))
            moves.append(pltpu.make_async_copy(cot_ref, cot_out.at[rows], sem.at[len(moves)]))
            row += h_ref.shape[0]

        @pl.when(pl.program_id(0) == 0)
        def _():
            for move in moves:
                move.start()
    else:
        act_ref, du_ref = refs[-2:]

    places, base = [], 0
    for h_ref, cot_ref in pieces:
        places += [(h_ref, cot_ref, first, base + first) for first in range(0, h_ref.shape[0], step_rows)]
        base += h_ref.shape[0]

    def products(h_ref, cot_ref, first, _):
        rows = slice(first, first + step_rows)
        return dot_nn(h_ref[rows, :], up_ref[...]), dot_nt(cot_ref[rows, :], down_ref[...])

    following = products(*places[0])
    for number, place in enumerate(places):
        hidden, grad_act = following
        if number + 1 < len(places):
            following = products(*places[number + 1])
        out_rows = slice(place[3], place[3] + step_rows)
        act, slope = gelu_parts(hidden)
        act_ref[out_rows, :] = act.astype(BF16)
        du_ref[out_rows, :] = (grad_act.astype(BF16).astype(F32) * slope).astype(BF16)

    if copies:
        @pl.when(pl.program_id(0) == pl.num_programs(0) - 1)
        def _():
            for move in moves:
                move.wait()


def ff_forward(index, count, pieces, up, down, copies, carry):
    tokens = sum(piece[0].shape[0] for piece in pieces)
    d_model, width = up.shape
    tile = FF_TILE
    shapes = [jax.ShapeDtypeStruct((count * tokens, width), BF16)] * 2
    specs = [pl.BlockSpec((tokens, tile), lambda n: (index, n))] * 2
    if copies:
        shapes = shapes + [jax.ShapeDtypeStruct((count * tokens, d_model), BF16)] * 2
        specs = specs + [pl.BlockSpec(memory_space=pl.ANY)] * 2
    in_specs, args = [], []
    for h_blk, cot_blk, row_blk in pieces:
        in_specs += [pl.BlockSpec(h_blk.shape, lambda n: (0, 0)),
                     pl.BlockSpec(h_blk.shape, lambda n, row_blk=row_blk: (row_blk, 0))]
        args += [h_blk, cot_blk]
    carry = list(carry)
    return pl.pallas_call(
        functools.partial(ff_kernel, FF_ROWS, copies, index * tokens, len(pieces)),
        grid=(width // tile,),
        in_specs=in_specs + [pl.BlockSpec((d_model, tile), lambda n: (0, n)), pl.BlockSpec((tile, d_model), lambda n: (n, 0))]
        + [pl.BlockSpec(memory_space=pl.ANY)] * len(carry),
        out_specs=specs,
        out_shape=shapes,
        input_output_aliases={len(args) + 2 + pos: pos for pos in range(len(carry))},
        scratch_shapes=[pltpu.SemaphoreType.DMA((2 * len(pieces),))] if copies else [],
        compiler_params=pltpu.CompilerParams(vmem_limit_bytes=56 * 2 ** 20),
        cost_estimate=pl.CostEstimate(flops=4 * tokens * d_model * width, bytes_accessed=4 * d_model * (width + 2 * tokens),
                                      transcendentals=tokens * width),
    )(*args, up, down, *carry)


def grad_h_kernel(n_parts, *refs):
    total = sum(dot_nt(refs[2 * part][...], refs[2 * part + 1][...]) for part in range(n_parts))
    halves = []
    for extra in refs[2 * n_parts:-1]:
        if extra.shape == total.shape:
            total = total + extra[...]
        else:
            halves.append(extra[...])
    if halves:
        total = total + jnp.concatenate(halves, axis=0)
    refs[-1][...] = total.astype(refs[-1].dtype)


def grad_h_block(index, tokens, grad_u, up, extras, dtype):
    d_model = up[0].shape[0]
    width = sum(part.shape[1] for part in up)
    tile = 256
    in_specs, args = [], []
    for left, right in zip(grad_u, up):
        in_specs += [pl.BlockSpec((tokens, left.shape[1]), lambda n: (index, 0)), pl.BlockSpec((tile, right.shape[1]), lambda n: (n, 0))]
        args += [left, right]
    return pl.pallas_call(
        functools.partial(grad_h_kernel, len(up)),
        grid=(d_model // tile,),
        in_specs=in_specs + [pl.BlockSpec((extra.shape[0], tile), lambda n: (0, n)) for extra in extras],
        out_specs=pl.BlockSpec((tokens, tile), lambda n: (0, n)),
        out_shape=jax.ShapeDtypeStruct((tokens, d_model), dtype),
        compiler_params=pltpu.CompilerParams(vmem_limit_bytes=48 * 2 ** 20),
        cost_estimate=pl.CostEstimate(flops=2 * tokens * d_model * width, bytes_accessed=2 * width * (d_model + tokens) + 4 * tokens * d_model,
                                      transcendentals=0),
    )(*args, *extras)


def head_grad_kernel(scale, n_pairs, *refs):
    total = sum(dot_nn(refs[n_pairs + pair][...], refs[pair][...]) for pair in range(n_pairs))
    refs[-1][...] = (scale * total).T


def head_grad(scale, columns, heads_t):
    n_pairs = len(columns)
    rows, width, tokens = columns[0].shape[1], heads_t[0].shape[0], columns[0].shape[0]
    tile = 512
    return pl.pallas_call(
        functools.partial(head_grad_kernel, scale, n_pairs),
        grid=(width // tile,),
        in_specs=[pl.BlockSpec((tokens, rows), lambda n: (0, 0))] * n_pairs + [pl.BlockSpec((tile, tokens), lambda n: (n, 0))] * n_pairs,
        out_specs=pl.BlockSpec((rows, tile), lambda n: (0, n)),
        out_shape=jax.ShapeDtypeStruct((rows, width), F32),
        compiler_params=pltpu.CompilerParams(vmem_limit_bytes=48 * 2 ** 20),
        cost_estimate=pl.CostEstimate(flops=2 * n_pairs * rows * width * tokens, bytes_accessed=2 * n_pairs * tokens * (rows + width) + 4 * rows * width,
                                      transcendentals=0),
    )(*columns, *heads_t)


def spread_kernel(splits, idx_ref, *refs):
    got_refs, out_ref = refs[:-1], refs[-1]
    count = got_refs[0].shape[0]
    block = splits[-1][0] + splits[-1][1]
    for dest in range(out_ref.shape[1] // block):
        row, src = dest // count, dest % count
        for (first, cols), got_ref in zip(splits, got_refs):
            out_ref[:, dest * block + first:dest * block + first + cols] = got_ref[idx_ref[0] ^ src, :, row * cols:(row + 1) * cols]


def spread_columns(my_idx, got, splits):
    count, rows = got[0].shape[:2]
    width = count * sum(part.shape[2] for part in got)
    return pl.pallas_call(
        functools.partial(spread_kernel, splits),
        in_specs=[pl.BlockSpec(memory_space=pltpu.SMEM)] + [pl.BlockSpec(memory_space=pltpu.VMEM)] * len(got),
        out_specs=pl.BlockSpec(memory_space=pltpu.VMEM),
        out_shape=jax.ShapeDtypeStruct((rows, width), F32),
        cost_estimate=pl.CostEstimate(flops=rows * width, bytes_accessed=8 * rows * width, transcendentals=0),
    )(my_idx.reshape(1), *got)


def solution(mesh):
    cp_size = mesh.shape['cp']
    dp_size = mesh.shape['dp']
    dev_count = cp_size * dp_size

    def swap(values, bits):
        return lax.ppermute(values, 'cp', [(src, src ^ bits) for src in range(cp_size)])

    def dp_reduce(grad):
        return lax.psum_scatter(grad, 'dp', scatter_dimension=0, tiled=True)

    def after(value, *earlier):
        return lax.optimization_barrier((value,) + earlier)[0]

    def per_device(x_loc, cot_loc, w_q, w_k, w_v, w_o, w_up, w_down):
        d_model = x_loc.shape[2]
        seq_len = x_loc.shape[1]
        kv_heads, head_dim = w_k.shape[1], w_k.shape[2]
        n_heads = w_q.shape[1]
        group = n_heads // kv_heads
        half = seq_len // 2
        kv_width = kv_heads * head_dim
        rows = group * head_dim
        ff_dim = w_up.shape[1]
        ff_part = ff_dim // dev_count
        my_idx = lax.axis_index('cp')
        x = x_loc[0]
        cot = cot_loc[0]
        w_q = w_q.reshape(d_model, n_heads * head_dim)
        w_o = w_o.reshape(d_model, n_heads * head_dim)
        w_kv = jnp.concatenate([w_k.reshape(d_model, kv_width), w_v.reshape(d_model, kv_width)], axis=1)
        tab = pair_table(my_idx, cp_size)

        inv_count = 1.0 / dev_count

        def own_cols(values, bits):
            width = d_model // dev_count
            return jnp.concatenate([lax.dynamic_slice_in_dim(values, (part * cp_size + (my_idx ^ bits)) * width, width, axis=1)
                                    for part in range(dp_size)], axis=1)

        kv_own = dot_nn(x, w_kv).astype(BF16)
        kv_all = lax.all_gather(kv_own, 'cp', axis=0, tiled=True)
        cot_near = swap(cot, 1)

        first_part = FF_TILE * (dp_size * ff_part // (2 * FF_TILE)) // dp_size
        splits = ((0, first_part), (first_part, ff_part - first_part))
        used = [dp_size * count for _, count in splits]
        starts = (jnp.arange(dp_size) * cp_size + my_idx) * ff_part
        w_up_own, w_down_own = prepare(starts, splits, w_up, w_down)
        cot_far = swap(after(cot, w_up_own[0]), 2)
        later = after(x, w_up_own[0])
        q_t = dot_tt(w_q, later).astype(BF16)

        kv_all = after(kv_all, q_t, w_up_own[0])
        o_f32, o_t, lse = attn_forward(tab, q_t, kv_all, kv_heads, head_dim)

        h_act = (x + dot_tt(o_t, w_o)).astype(BF16)
        h_far0 = swap(h_act[:half], 2)
        h_near = swap(h_act, 1)
        o_near = swap(o_t, 1)

        def ff_call(index, part, pieces, carry, *earlier):
            first = after(pieces[0][0], *earlier) if earlier else pieces[0][0]
            pieces = [(first,) + pieces[0][1:]] + pieces[1:]
            return ff_forward(index, cp_size, pieces, w_up_own[part], w_down_own[part], part == 0, carry)

        def remote(piece, far_piece):
            return [(far_piece, cot_far, piece), (swap(far_piece, 1), cot_last, piece)]

        own, near = [(h_act, cot, 0)], [(h_near, cot_near, 0)]
        state = ff_call(0, 0, own, ())
        h_far1 = swap(after(h_act, state[0])[half:], 2)
        cot_last = swap(after(cot_far, state[0]), 1)
        state = ff_call(1, 0, near, state)
        more = ff_call(0, 1, own, (), state[0])
        block = remote(0, after(h_far0, more[0]))
        state = ff_call(2, 0, block, state)
        act1, grad_u1 = ff_call(2, 1, block, more, state[0])

        def grad_h(index, tokens, earlier, extras, dtype):
            later = after(grad_u1, earlier)
            return grad_h_block(index, tokens, (state[1], later), w_up_own, extras, dtype)

        h_far1 = after(h_far1, act1)
        block = remote(1, h_far1)
        o_far = swap(after(o_t, h_far1), 2)
        state = ff_call(3, 0, block, state, act1)
        o_last = swap(o_far, 1)
        act0, grad_u0, h_all, cot_all = state
        part = row_major(inv_count * dot_tn(h_all, grad_u0))
        up_rows = [dp_reduce(part)]
        part = grad_h(5, half, part, [], F32)
        near0 = swap(part, 1)
        act1, grad_u1 = ff_call(3, 1, block, (act1, grad_u1), part)
        part = grad_h(4, half, act1, [near0], F32)
        far0 = swap(part, 2)
        act1, grad_u1 = ff_call(1, 1, near, (act1, grad_u1), part)
        part = grad_h(7, half, act1, [], F32)
        near1 = swap(part, 1)
        later = after(grad_u1, part)
        part = row_major(inv_count * dot_tn(h_all, later[:, :used[1]]))
        up_rows.append(dp_reduce(part))
        part = grad_h(6, half, part, [near1], F32)
        far1 = swap(part, 2)
        later = after(act0, part)
        part = row_major(inv_count * dot_tn(later, cot_all))
        down_rows = [dp_reduce(part)]
        part = grad_h(1, seq_len, part, [], F32)
        side = swap(part, 1)
        later = after(act1, part)
        part = row_major(inv_count * dot_tn(later[:, :used[1]], cot_all))
        down_rows.append(dp_reduce(part))
        far0 = after(far0, part)

        own_rows = d_model // dev_count

        def exchange(rows_of):
            blocks = [lax.dynamic_slice_in_dim(rows_of, (my_idx ^ bits) * own_rows, own_rows, axis=0) for bits in range(cp_size)]
            return jnp.stack([blocks[0]] + [row_major(swap(row_major(blocks[bits]), bits)) for bits in range(1, cp_size)])

        up_got = [exchange(up_rows[0])]
        grad_h_bf = grad_h(0, seq_len, part, [cot, side, far0, far1], BF16)

        def block_sum(left, right_t):
            def block(bits):
                return inv_count * dot_tt(own_cols(left, bits), right_t)

            return block

        def first_sends(block):
            parts = block(3), block(1)
            return (swap(parts[0], 1), swap(parts[1], 1)), parts

        def second_send(block, sent):
            part = block(2) + sent[0]
            return swap(part, 2), part

        mine = [None] + [swap(own_cols(grad_h_bf, bits), bits) for bits in range(1, cp_size)]
        do_t = dot_tt(w_o, grad_h_bf).astype(BF16)

        def kv_block(dkv):
            blocks = dkv.reshape((cp_size, 2) + dkv.shape[1:])
            return lambda bits: lax.dynamic_index_in_dim(blocks, my_idx ^ bits, axis=0, keepdims=False)

        dq0_t, dkv0 = attn_backward(tab, q_t, do_t, o_f32, lse, kv_all, kv_heads, head_dim, 0)
        kv0_block, q0_block = kv_block(dkv0), block_sum(x, dq0_t)
        kv0_sent, parts_kv = first_sends(kv0_block)
        q0_sent, parts_q = first_sends(q0_block)
        kv0_far, part_kv = second_send(kv0_block, (after(kv0_sent[0], *parts_q), kv0_sent[1]))
        q0_far, part_q = second_send(q0_block, q0_sent)
        do_t = after(do_t, part_kv, part_q)
        dq1_t, dkv1 = attn_backward(tab, q_t, do_t, o_f32, lse, kv_all, kv_heads, head_dim, 1, 0, 2)
        q1_block = block_sum(x, dq1_t)
        q1_sent, parts_q = first_sends(q1_block)
        base_q = q0_block(0)
        q1_far, part_q = second_send(q1_block, (after(q1_sent[0], base_q), q1_sent[1]))
        do_t = after(do_t, part_q, *parts_q)
        dq2_t, dkv1 = attn_backward(tab, q_t, do_t, o_f32, lse, kv_all, kv_heads, head_dim, 1, 1, 2, (dkv1,))
        kv1_block, q2_block = kv_block(dkv1), block_sum(x, dq2_t)
        kv1_sent, parts_kv = first_sends(kv1_block)
        q2_sent, parts_q = first_sends(q2_block)
        kv1_far, part_kv = second_send(kv1_block, (after(kv1_sent[0], *parts_q), kv1_sent[1]))
        q2_far, part_q = second_send(q2_block, (after(q2_sent[0], part_kv), q2_sent[1]))
        mine[0] = own_cols(after(grad_h_bf, part_q), 0)
        sum_o = head_grad(inv_count, mine, (o_t, o_near, o_far, o_last))
        q0_far = after(q0_far, sum_o)
        sum_q0 = base_q + q0_sent[1] + q0_far
        grad_oq = dp_reduce(jnp.concatenate([sum_o, sum_q0], axis=1))
        kv0_own = (kv0_block(0) + kv0_sent[1] + after(kv0_far, sum_o)).astype(BF16)
        kv1_own = (kv1_block(0) + kv1_sent[1] + after(kv1_far, kv0_own)).astype(BF16)
        dkv_t = jnp.concatenate([jnp.concatenate([part[0, which], part[1, which]], axis=1)
                                 for which in range(2) for part in (kv0_own, kv1_own)], axis=0)
        w_block = block_sum(x, dkv_t)
        w_sent, _ = first_sends(w_block)
        w_far, part_w = second_send(w_block, w_sent)
        up_got.append(exchange(after(up_rows[1], part_w)))
        grad_w_up = spread_columns(my_idx, up_got, splits)
        later = jnp.concatenate([after(dq0_t, part_w), dq1_t, dq2_t], axis=0)
        grad_x = dot_tt(later, w_q)
        grad_x = grad_h_bf + grad_x + dot_tt(after(dkv_t, part_w), w_kv)
        sum_q1 = q1_block(0) + q1_sent[1] + after(q1_far, part_w)
        sum_q2 = q2_block(0) + q2_sent[1] + after(q2_far, part_w)
        grad_qk = dp_reduce(jnp.concatenate([sum_q1, sum_q2, w_block(0) + w_sent[1] + w_far], axis=1))
        grad_w_down = jnp.concatenate(down_rows, axis=0)
        o_width = n_heads * head_dim

        grad_w_q = jnp.concatenate([grad_oq[:, o_width:], grad_qk[:, :rows]], axis=1).reshape(own_rows, n_heads, head_dim)
        grad_w_k = grad_qk[:, rows:rows + kv_width].reshape(own_rows, kv_heads, head_dim)
        grad_w_v = grad_qk[:, rows + kv_width:].reshape(own_rows, kv_heads, head_dim)
        grad_w_o = grad_oq[:, :o_width].reshape(own_rows, n_heads, head_dim)
        return grad_x.astype(BF16)[None], grad_w_q, grad_w_k, grad_w_v, grad_w_o, grad_w_up, grad_w_down

    act_spec = P('dp', 'cp', None)
    rep_three = P(None, None, None)
    rep_two = P(None, None)
    grad_three = P(('dp', 'cp'), None, None)
    grad_two = P(('dp', 'cp'), None)
    return jax.shard_map(per_device, mesh=mesh,
                         in_specs=(act_spec, act_spec, rep_three, rep_three, rep_three, rep_three, rep_two, rep_two),
                         out_specs=(act_spec, grad_three, grad_three, grad_three, grad_three, grad_two, grad_two),
                         check_vma=False)
```

```python
import functools
import math

import jax
import jax.numpy as jnp
from jax import lax
from jax.experimental import pallas as pl
from jax.experimental.pallas import tpu as pltpu
from jax.experimental.layout import Layout, with_layout_constraint
from jax.sharding import PartitionSpec as P


NEG_BIG = -1e30
LOG2E = math.log2(math.e)
F32 = jnp.float32
FF_TILE = 256
VMEM_BYTES = 56 * 2 ** 20
FF_ROWS = 512
BF16 = jnp.bfloat16


def row_major(values):
    return with_layout_constraint(values, Layout(major_to_minor=(0, 1)))


def dot_nn(lhs, rhs):
    return lax.dot_general(lhs, rhs, (((1,), (0,)), ((), ())), preferred_element_type=F32)


def dot_nt(lhs, rhs):
    return lax.dot_general(lhs, rhs, (((1,), (1,)), ((), ())), preferred_element_type=F32)


def dot_tn(lhs, rhs):
    return lax.dot_general(lhs, rhs, (((0,), (0,)), ((), ())), preferred_element_type=F32)


def dot_tt(lhs, rhs):
    return lax.dot_general(lhs, rhs, (((0,), (1,)), ((), ())), preferred_element_type=F32)


def pair_table(my_idx, cp_size):
    steps = jnp.arange(2 * cp_size + 1)
    late = steps > my_idx
    key_block = jnp.where(late, steps - my_idx - 1, steps)
    key_slot = jnp.where(key_block < cp_size, 2 * key_block, 2 * (2 * cp_size - 1 - key_block) + 1)
    last = (steps == my_idx) | (steps == 2 * cp_size)
    first = (steps == 0) | (steps == my_idx + 1)
    return jnp.stack([late, key_slot, last, first]).astype(jnp.int32)


def causal_keep(half):
    keys = lax.broadcasted_iota(jnp.int32, (half, half), 0)
    queries = lax.broadcasted_iota(jnp.int32, (half, half), 1)
    return keys <= queries


def attn_fwd_kernel(group, scale, tab, q_ref, k_ref, v_ref, of_ref, ob_ref, lse_ref, m_ref, l_ref, acc_ref):
    dim = k_ref.shape[1]
    half = q_ref.shape[1] // 2
    factor = scale * LOG2E

    def pair_step(pair, carry):
        cols = pl.ds(pl.multiple_of(tab[0, pair] * half, half), half)
        slot = pl.ds(pl.multiple_of(tab[1, pair] * half, half), half)

        @pl.when(tab[3, pair] == 1)
        def _():
            m_ref[...] = jnp.full(m_ref.shape, NEG_BIG, F32)
            l_ref[...] = jnp.zeros(l_ref.shape, F32)
            acc_ref[...] = jnp.zeros(acc_ref.shape, F32)

        def run(masked):
            keys = k_ref[slot, :]
            vals_t = v_ref[slot, :].T

            def scores_of(head):
                scores = dot_nn(keys, q_ref[head * dim:(head + 1) * dim, cols])
                return jnp.where(causal_keep(half), scores, NEG_BIG) if masked else scores

            following = scores_of(0)
            for head in range(group):
                scores = following
                if head + 1 < group:
                    following = scores_of(head + 1)
                rows = slice(head * dim, (head + 1) * dim)
                old_max = m_ref[head:head + 1, :]
                new_max = jnp.maximum(old_max, jnp.max(scores, axis=0, keepdims=True))
                probs = jnp.exp2(scores * factor - new_max * factor)
                alpha = jnp.exp2((old_max - new_max) * factor)
                m_ref[head:head + 1, :] = new_max
                l_ref[head:head + 1, :] = alpha * l_ref[head:head + 1, :] + jnp.sum(probs, axis=0, keepdims=True)
                acc_ref[rows, :] = alpha * acc_ref[rows, :] + dot_nn(vals_t, probs.astype(BF16))

        @pl.when(tab[2, pair] == 0)
        def _():
            run(False)

        @pl.when(tab[2, pair] == 1)
        def _():
            run(True)
            lse_ref[0, :, cols] = m_ref[...] * factor + jnp.log2(l_ref[...])
            for head in range(group):
                rows = slice(head * dim, (head + 1) * dim)
                out = acc_ref[rows, :] / l_ref[head:head + 1, :]
                of_ref[rows, cols] = out
                ob_ref[rows, cols] = out.astype(BF16)

        return carry

    lax.fori_loop(0, tab.shape[1], pair_step, 0)


def attn_forward(tab, q_t, kv_all, kv_heads, head_dim):
    width, seq = q_t.shape
    half = seq // 2
    group = width // (kv_heads * head_dim)
    rows = group * head_dim
    n_pairs = tab.shape[1]
    q_spec = pl.BlockSpec((rows, seq), lambda k, t: (k, 0))
    return pl.pallas_call(
        functools.partial(attn_fwd_kernel, group, head_dim ** -0.5),
        grid_spec=pltpu.PrefetchScalarGridSpec(
            num_scalar_prefetch=1,
            grid=(kv_heads,),
            in_specs=[q_spec,
                      pl.BlockSpec((kv_all.shape[0], head_dim), lambda k, t: (0, k)),
                      pl.BlockSpec((kv_all.shape[0], head_dim), lambda k, t: (0, kv_heads + k))],
            out_specs=[q_spec, q_spec,
                       pl.BlockSpec((1, group, seq), lambda k, t: (k, 0, 0))],
            scratch_shapes=[pltpu.VMEM((group, half), F32), pltpu.VMEM((group, half), F32), pltpu.VMEM((rows, half), F32)]),
        out_shape=[jax.ShapeDtypeStruct((width, seq), F32), jax.ShapeDtypeStruct((width, seq), BF16),
                   jax.ShapeDtypeStruct((kv_heads, group, seq), F32)],
        compiler_params=pltpu.CompilerParams(vmem_limit_bytes=VMEM_BYTES),
        cost_estimate=pl.CostEstimate(flops=4 * width * half * half * n_pairs,
                                      bytes_accessed=12 * width * seq, transcendentals=width // head_dim * half * half * n_pairs),
    )(tab, q_t, kv_all, kv_all)


def attn_bwd_kernel(group, first_head, scale, tab, q_ref, do_ref, of_ref, lse_ref, k_ref, v_ref, *refs):
    dim = k_ref.shape[1]
    half = q_ref.shape[1] // 2
    factor = scale * LOG2E
    dq_ref, dkv_ref, delta_ref, acc_ref = refs[-4:]
    dkv_ref[...] = refs[0][...] if len(refs) > 4 else jnp.zeros(dkv_ref.shape, F32)

    def pair_step(pair, carry):
        cols = pl.ds(pl.multiple_of(tab[0, pair] * half, half), half)
        slot = tab[1, pair]
        slot_rows = pl.ds(pl.multiple_of(slot * half, half), half)

        @pl.when(tab[3, pair] == 1)
        def _():
            acc_ref[...] = jnp.zeros(acc_ref.shape, F32)
            for head in range(group):
                rows = slice(head * dim, (head + 1) * dim)
                delta_ref[head:head + 1, :] = jnp.sum(do_ref[rows, cols].astype(F32) * of_ref[rows, cols], axis=0, keepdims=True)

        def run(masked):
            keys = k_ref[slot_rows, :]
            vals = v_ref[slot_rows, :]
            keys_t = keys.T
            for head in range(group):
                rows = slice(head * dim, (head + 1) * dim)
                q_head = q_ref[rows, cols]
                do_head = do_ref[rows, cols]
                scores = dot_nn(keys, q_head)
                if masked:
                    scores = jnp.where(causal_keep(half), scores, NEG_BIG)
                probs = jnp.exp2(scores * factor - lse_ref[0, first_head + head:first_head + head + 1, cols])
                grad_p = dot_nn(vals, do_head)
                grad_s = (probs * (grad_p - delta_ref[head:head + 1, :])).astype(BF16)
                dkv_ref[slot, 1] += dot_nt(do_head, probs.astype(BF16))
                dkv_ref[slot, 0] += scale * dot_nt(q_head, grad_s)
                acc_ref[rows, :] += dot_nn(keys_t, grad_s)

        @pl.when(tab[2, pair] == 0)
        def _():
            run(False)

        @pl.when(tab[2, pair] == 1)
        def _():
            run(True)
            dq_ref[:, cols] = (scale * acc_ref[...]).astype(BF16)

        return carry

    lax.fori_loop(0, tab.shape[1], pair_step, 0)


def attn_backward(tab, q_t, do_t, o_f32, lse, kv_all, kv_heads, head_dim, kv_head, piece=0, n_pieces=1, carry=()):
    width, seq = q_t.shape
    half = seq // 2
    group = width // (kv_heads * head_dim)
    heads = group // n_pieces
    rows = heads * head_dim
    n_slots = kv_all.shape[0] // half
    n_pairs = tab.shape[1]
    q_spec = pl.BlockSpec((rows, seq), lambda p, t: (kv_head * n_pieces + piece, 0))
    dkv_spec = pl.BlockSpec((n_slots, 2, head_dim, half), lambda p, t: (0, 0, 0, 0))
    return pl.pallas_call(
        functools.partial(attn_bwd_kernel, heads, piece * heads, head_dim ** -0.5),
        grid_spec=pltpu.PrefetchScalarGridSpec(
            num_scalar_prefetch=1,
            grid=(1,),
            in_specs=[q_spec, q_spec, q_spec,
                      pl.BlockSpec((1, group, seq), lambda p, t: (kv_head, 0, 0)),
                      pl.BlockSpec((kv_all.shape[0], head_dim), lambda p, t: (0, kv_head)),
                      pl.BlockSpec((kv_all.shape[0], head_dim), lambda p, t: (0, kv_heads + kv_head))]
            + [dkv_spec] * len(carry),
            out_specs=[pl.BlockSpec((rows, seq), lambda p, t: (0, 0)),
                       dkv_spec],
            scratch_shapes=[pltpu.VMEM((heads, half), F32), pltpu.VMEM((rows, half), F32)]),
        out_shape=[jax.ShapeDtypeStruct((rows, seq), BF16),
                   jax.ShapeDtypeStruct((n_slots, 2, head_dim, half), F32)],
        compiler_params=pltpu.CompilerParams(vmem_limit_bytes=VMEM_BYTES),
        cost_estimate=pl.CostEstimate(flops=10 * rows * half * half * n_pairs,
                                      bytes_accessed=12 * rows * seq, transcendentals=heads * half * half * n_pairs),
    )(tab, q_t, do_t, o_f32, lse, kv_all, kv_all, *carry)


def gelu_parts(values):
    curve = math.sqrt(2 / math.pi)
    square = values * values
    tanh = jnp.tanh(values * (curve + (curve * 0.044715) * square))
    cdf = 0.5 + 0.5 * tanh
    slope = cdf + (0.5 * values) * (1.0 - tanh * tanh) * (curve + (3 * curve * 0.044715) * square)
    return values * cdf, slope


def prep_kernel(segs, parts, idx_ref, *refs):
    n_blocks = sum(seg[3] + 1 for seg in segs)
    blocks, down_ref = refs[:n_blocks], refs[n_blocks]
    n_parts = len(parts)
    up_refs, down_refs = refs[n_blocks + 1:n_blocks + 1 + n_parts], refs[n_blocks + 1 + n_parts:n_blocks + 1 + 2 * n_parts]
    buf_ref, zero_ref, in_sem, out_sem = refs[n_blocks + 1 + 2 * n_parts:]
    step = pl.program_id(0)
    n_own, own_rows = buf_ref.shape[0], buf_ref.shape[1]
    ins = [pltpu.make_async_copy(down_ref.at[pl.ds(pl.multiple_of(idx_ref[0, own], 16), own_rows)], buf_ref.at[own], in_sem.at[own])
           for own in range(n_own)]
    outs = []
    for part, down_out in zip(parts, down_refs):
        for own in range(n_own):
            outs.append(pltpu.make_async_copy(buf_ref.at[own, pl.ds(part[0], part[1])],
                                              down_out.at[pl.ds(own * part[1], part[1])], out_sem.at[len(outs)]))
        if part[2]:
            outs.append(pltpu.make_async_copy(zero_ref.at[pl.ds(0, part[2])],
                                              down_out.at[pl.ds(n_own * part[1], part[2])], out_sem.at[len(outs)]))

    @pl.when(step == 0)
    def _():
        zero_ref[...] = jnp.zeros(zero_ref.shape, BF16)
        for copy in ins:
            copy.start()

    @pl.when(step == 1)
    def _():
        for copy in ins:
            copy.wait()
        for copy in outs:
            copy.start()

    rows = blocks[0].shape[0]
    lanes = lax.broadcasted_iota(jnp.int32, (rows, 128), 1)
    cover = [{} for _ in parts]
    pos = 0
    for number, seg in enumerate(segs):
        shift = idx_ref[1, number]
        turned = [pltpu.roll(blocks[pos + tile][...].astype(F32), (128 - shift) % 128, 1) for tile in range(seg[3] + 1)]
        pos += seg[3] + 1
        for tile in range(seg[3]):
            cover[seg[0]].setdefault(seg[2] + tile, []).append(
                (seg[1], jnp.where(lanes < 128 - shift, turned[tile], turned[tile + 1])))
    for part, tiles, up_ref in zip(parts, cover, up_refs):
        used = n_own * part[1]
        for tile in range(up_ref.shape[1] // 128):
            value = jnp.zeros((rows, 128), F32)
            for start, piece in tiles.get(tile, []):
                value = piece if start <= tile * 128 else jnp.where(lanes >= start - tile * 128, piece, value)
            if used < (tile + 1) * 128:
                value = jnp.where(lanes < used - tile * 128, value, 0.0)
            up_ref[:, tile * 128:(tile + 1) * 128] = value.astype(BF16)

    @pl.when(step == pl.num_programs(0) - 1)
    def _():
        for copy in outs:
            copy.wait()


def prepare(starts, splits, w_up, w_down):
    d_model, own_rows = w_up.shape[0], splits[-1][0] + splits[-1][1]
    n_own = starts.shape[0]
    parts = [(first, count, -(n_own * count) % FF_TILE) for first, count in splits]
    segs, shifts, bases = [], [], []
    for number, part in enumerate(parts):
        for own in range(n_own):
            dest = own * part[1]
            segs.append((number, dest, dest // 128, -(-(dest % 128 + part[1]) // 128)))
            source = starts[own] + part[0] - dest % 128
            shifts.append(source % 128)
            bases.append(source // 128)
    table = jnp.stack([jnp.pad(starts, (0, len(segs) - n_own)), jnp.stack(shifts), jnp.stack(bases)]).astype(jnp.int32)
    rows = 512
    last = w_up.shape[1] // 128 - 1
    in_specs = []
    for number, seg in enumerate(segs):
        for tile in range(seg[3] + 1):
            in_specs.append(pl.BlockSpec((rows, 128), lambda i, t, number=number, tile=tile:
                                         (i, jnp.clip(t[2, number] + tile, 0, last))))
    widths = [n_own * part[1] + part[2] for part in parts]
    outs = pl.pallas_call(
        functools.partial(prep_kernel, segs, parts),
        grid_spec=pltpu.PrefetchScalarGridSpec(
            num_scalar_prefetch=1,
            grid=(d_model // rows,),
            in_specs=in_specs + [pl.BlockSpec(memory_space=pl.ANY)],
            out_specs=[pl.BlockSpec((rows, width), lambda i, t: (i, 0)) for width in widths]
            + [pl.BlockSpec(memory_space=pl.ANY) for _ in widths],
            scratch_shapes=[pltpu.VMEM((n_own, own_rows, d_model), BF16), pltpu.VMEM((64, d_model), BF16),
                            pltpu.SemaphoreType.DMA((n_own,)), pltpu.SemaphoreType.DMA((n_own * len(parts) + len(parts),))]),
        out_shape=[jax.ShapeDtypeStruct((d_model, width), BF16) for width in widths]
        + [jax.ShapeDtypeStruct((width, d_model), BF16) for width in widths],
        compiler_params=pltpu.CompilerParams(vmem_limit_bytes=VMEM_BYTES),
        cost_estimate=pl.CostEstimate(flops=8 * d_model * sum(widths), bytes_accessed=9 * d_model * sum(widths), transcendentals=0),
    )(table, *([w_up] * len(in_specs)), w_down)
    return outs[:len(parts)], outs[len(parts):]


def ff_kernel(step_rows, copies, first_row, n_pieces, *refs):
    pieces = [(refs[2 * piece], refs[2 * piece + 1]) for piece in range(n_pieces)]
    up_ref, down_ref = refs[2 * n_pieces:2 * n_pieces + 2]
    if copies:
        act_ref, du_ref, h_out, cot_out, sem = refs[-5:]
        moves, row = [], first_row
        for h_ref, cot_ref in pieces:
            rows = pl.ds(row, h_ref.shape[0])
            moves.append(pltpu.make_async_copy(h_ref, h_out.at[rows], sem.at[len(moves)]))
            moves.append(pltpu.make_async_copy(cot_ref, cot_out.at[rows], sem.at[len(moves)]))
            row += h_ref.shape[0]

        @pl.when(pl.program_id(0) == 0)
        def _():
            for move in moves:
                move.start()
    else:
        act_ref, du_ref = refs[-2:]

    places, base = [], 0
    for h_ref, cot_ref in pieces:
        places += [(h_ref, cot_ref, first, base + first) for first in range(0, h_ref.shape[0], step_rows)]
        base += h_ref.shape[0]

    def products(h_ref, cot_ref, first, _):
        rows = slice(first, first + step_rows)
        return dot_nn(h_ref[rows, :], up_ref[...]), dot_nt(cot_ref[rows, :], down_ref[...])

    following = products(*places[0])
    for number, place in enumerate(places):
        hidden, grad_act = following
        if number + 1 < len(places):
            following = products(*places[number + 1])
        out_rows = slice(place[3], place[3] + step_rows)
        act, slope = gelu_parts(hidden)
        act_ref[out_rows, :] = act.astype(BF16)
        du_ref[out_rows, :] = (grad_act.astype(BF16).astype(F32) * slope).astype(BF16)

    if copies:
        @pl.when(pl.program_id(0) == pl.num_programs(0) - 1)
        def _():
            for move in moves:
                move.wait()


def ff_forward(index, count, pieces, up, down, copies, carry):
    tokens = sum(piece[0].shape[0] for piece in pieces)
    d_model, width = up.shape
    tile = FF_TILE
    shapes = [jax.ShapeDtypeStruct((count * tokens, width), BF16)] * 2
    specs = [pl.BlockSpec((tokens, tile), lambda n: (index, n))] * 2
    if copies:
        shapes = shapes + [jax.ShapeDtypeStruct((count * tokens, d_model), BF16)] * 2
        specs = specs + [pl.BlockSpec(memory_space=pl.ANY)] * 2
    in_specs, args = [], []
    for h_blk, cot_blk, row_blk in pieces:
        in_specs += [pl.BlockSpec(h_blk.shape, lambda n: (0, 0)),
                     pl.BlockSpec(h_blk.shape, lambda n, row_blk=row_blk: (row_blk, 0))]
        args += [h_blk, cot_blk]
    carry = list(carry)
    return pl.pallas_call(
        functools.partial(ff_kernel, FF_ROWS, copies, index * tokens, len(pieces)),
        grid=(width // tile,),
        in_specs=in_specs + [pl.BlockSpec((d_model, tile), lambda n: (0, n)), pl.BlockSpec((tile, d_model), lambda n: (n, 0))]
        + [pl.BlockSpec(memory_space=pl.ANY)] * len(carry),
        out_specs=specs,
        out_shape=shapes,
        input_output_aliases={len(args) + 2 + pos: pos for pos in range(len(carry))},
        scratch_shapes=[pltpu.SemaphoreType.DMA((2 * len(pieces),))] if copies else [],
        compiler_params=pltpu.CompilerParams(vmem_limit_bytes=VMEM_BYTES),
        cost_estimate=pl.CostEstimate(flops=4 * tokens * d_model * width, bytes_accessed=4 * d_model * (width + 2 * tokens),
                                      transcendentals=tokens * width),
    )(*args, up, down, *carry)


def grad_h_kernel(n_parts, *refs):
    total = sum(dot_nt(refs[2 * part][...], refs[2 * part + 1][...]) for part in range(n_parts))
    halves = []
    for extra in refs[2 * n_parts:-1]:
        if extra.shape == total.shape:
            total = total + extra[...]
        else:
            halves.append(extra[...])
    if halves:
        total = total + jnp.concatenate(halves, axis=0)
    refs[-1][...] = total.astype(refs[-1].dtype)


def grad_h_block(index, tokens, grad_u, up, extras, dtype):
    d_model = up[0].shape[0]
    width = sum(part.shape[1] for part in up)
    tile = 256
    in_specs, args = [], []
    for left, right in zip(grad_u, up):
        in_specs += [pl.BlockSpec((tokens, left.shape[1]), lambda n: (index, 0)), pl.BlockSpec((tile, right.shape[1]), lambda n: (n, 0))]
        args += [left, right]
    return pl.pallas_call(
        functools.partial(grad_h_kernel, len(up)),
        grid=(d_model // tile,),
        in_specs=in_specs + [pl.BlockSpec((extra.shape[0], tile), lambda n: (0, n)) for extra in extras],
        out_specs=pl.BlockSpec((tokens, tile), lambda n: (0, n)),
        out_shape=jax.ShapeDtypeStruct((tokens, d_model), dtype),
        compiler_params=pltpu.CompilerParams(vmem_limit_bytes=VMEM_BYTES),
        cost_estimate=pl.CostEstimate(flops=2 * tokens * d_model * width, bytes_accessed=2 * width * (d_model + tokens) + 4 * tokens * d_model,
                                      transcendentals=0),
    )(*args, *extras)


def head_grad_kernel(scale, n_pairs, n_tiles, *refs):
    step = pl.program_id(0)

    @pl.when(step < n_tiles)
    def _():
        total = sum(dot_nn(refs[n_pairs + pair][...], refs[pair][...]) for pair in range(n_pairs))
        refs[-1][...] = (scale * total).T

    @pl.when(step >= n_tiles)
    def _():
        refs[-1][...] = sum(ref[...] for ref in refs[2 * n_pairs:-1])


def head_grad(scale, columns, heads_t, terms):
    n_pairs = len(columns)
    rows, width, tokens = columns[0].shape[1], heads_t[0].shape[0], columns[0].shape[0]
    tile = rows
    n_tiles, n_more = width // tile, terms[0].shape[1] // tile
    last = n_tiles - 1
    return pl.pallas_call(
        functools.partial(head_grad_kernel, scale, n_pairs, n_tiles),
        grid=(n_tiles + n_more,),
        in_specs=[pl.BlockSpec((tokens, rows), lambda n: (0, 0))] * n_pairs
        + [pl.BlockSpec((tile, tokens), lambda n: (jnp.minimum(n, last), 0))] * n_pairs
        + [pl.BlockSpec((rows, tile), lambda n: (0, jnp.maximum(n - n_tiles, 0)))] * len(terms),
        out_specs=pl.BlockSpec((rows, tile), lambda n: (0, n)),
        out_shape=jax.ShapeDtypeStruct((rows, width + n_more * tile), F32),
        compiler_params=pltpu.CompilerParams(vmem_limit_bytes=VMEM_BYTES),
        cost_estimate=pl.CostEstimate(flops=2 * n_pairs * rows * width * tokens, bytes_accessed=9 * tokens * (rows + width), transcendentals=0),
    )(*columns, *heads_t, *terms)


def spread_kernel(splits, idx_ref, *refs):
    got_refs, out_ref = refs[:-1], refs[-1]
    count = got_refs[0].shape[0]
    block = splits[-1][0] + splits[-1][1]
    for dest in range(out_ref.shape[1] // block):
        row, src = dest // count, dest % count
        for (first, cols), got_ref in zip(splits, got_refs):
            out_ref[:, dest * block + first:dest * block + first + cols] = got_ref[idx_ref[0] ^ src, :, row * cols:(row + 1) * cols]


def spread_columns(my_idx, got, splits):
    count, rows = got[0].shape[:2]
    width = count * sum(part.shape[2] for part in got)
    return pl.pallas_call(
        functools.partial(spread_kernel, splits),
        in_specs=[pl.BlockSpec(memory_space=pltpu.SMEM)] + [pl.BlockSpec(memory_space=pltpu.VMEM)] * len(got),
        out_specs=pl.BlockSpec(memory_space=pltpu.VMEM),
        out_shape=jax.ShapeDtypeStruct((rows, width), F32),
        cost_estimate=pl.CostEstimate(flops=rows * width, bytes_accessed=8 * rows * width, transcendentals=0),
    )(my_idx.reshape(1), *got)


def solution(mesh):
    cp_size = mesh.shape['cp']
    dp_size = mesh.shape['dp']
    dev_count = cp_size * dp_size

    def swap(values, bits):
        return lax.ppermute(values, 'cp', [(src, src ^ bits) for src in range(cp_size)])

    def dp_reduce(grad):
        return lax.psum_scatter(grad, 'dp', scatter_dimension=0, tiled=True)

    def after(value, *earlier):
        return lax.optimization_barrier((value,) + earlier)[0]

    def per_device(x_loc, cot_loc, w_q, w_k, w_v, w_o, w_up, w_down):
        d_model = x_loc.shape[2]
        seq_len = x_loc.shape[1]
        kv_heads, head_dim = w_k.shape[1], w_k.shape[2]
        n_heads = w_q.shape[1]
        group = n_heads // kv_heads
        half = seq_len // 2
        kv_width = kv_heads * head_dim
        rows = group * head_dim
        ff_dim = w_up.shape[1]
        ff_part = ff_dim // dev_count
        my_idx = lax.axis_index('cp')
        x = x_loc[0]
        cot = cot_loc[0]
        w_q = w_q.reshape(d_model, n_heads * head_dim)
        w_o = w_o.reshape(d_model, n_heads * head_dim)
        w_kv = jnp.concatenate([w_k.reshape(d_model, kv_width), w_v.reshape(d_model, kv_width)], axis=1)
        tab = pair_table(my_idx, cp_size)

        inv_count = 1.0 / dev_count

        def own_cols(values, bits):
            width = d_model // dev_count
            return jnp.concatenate([lax.dynamic_slice_in_dim(values, (part * cp_size + (my_idx ^ bits)) * width, width, axis=1)
                                    for part in range(dp_size)], axis=1)

        kv_own = dot_nn(x, w_kv).astype(BF16)
        kv_all = lax.all_gather(kv_own, 'cp', axis=0, tiled=True)
        cot_near = swap(cot, 1)

        first_part = FF_TILE * (dp_size * ff_part // (2 * FF_TILE)) // dp_size
        splits = ((0, first_part), (first_part, ff_part - first_part))
        used = [dp_size * count for _, count in splits]
        starts = (jnp.arange(dp_size) * cp_size + my_idx) * ff_part
        w_up_own, w_down_own = prepare(starts, splits, w_up, w_down)
        cot_far = swap(after(cot, w_up_own[0]), 2)
        later = after(x, w_up_own[0])
        q_t = dot_tt(w_q, later).astype(BF16)

        kv_all = after(kv_all, q_t, w_up_own[0])
        o_f32, o_t, lse = attn_forward(tab, q_t, kv_all, kv_heads, head_dim)

        h_act = (x + dot_tt(o_t, w_o)).astype(BF16)
        h_far0 = swap(h_act[:half], 2)
        h_near = swap(h_act, 1)
        o_near = swap(o_t, 1)

        def ff_call(index, part, pieces, carry, *earlier):
            first = after(pieces[0][0], *earlier) if earlier else pieces[0][0]
            pieces = [(first,) + pieces[0][1:]] + pieces[1:]
            return ff_forward(index, cp_size, pieces, w_up_own[part], w_down_own[part], part == 0, carry)

        def remote(piece, far_piece):
            return [(far_piece, cot_far, piece), (swap(far_piece, 1), cot_last, piece)]

        own, near = [(h_act, cot, 0)], [(h_near, cot_near, 0)]
        state = ff_call(0, 0, own, ())
        h_far1 = swap(after(h_act, state[0])[half:], 2)
        cot_last = swap(after(cot_far, state[0]), 1)
        state = ff_call(1, 0, near, state)
        more = ff_call(0, 1, own, (), state[0])
        block = remote(0, after(h_far0, more[0]))
        state = ff_call(2, 0, block, state)
        act1, grad_u1 = ff_call(2, 1, block, more, state[0])

        def grad_h(index, tokens, earlier, extras, dtype):
            later = after(grad_u1, earlier)
            return grad_h_block(index, tokens, (state[1], later), w_up_own, extras, dtype)

        h_far1 = after(h_far1, act1)
        block = remote(1, h_far1)
        o_far = swap(after(o_t, h_far1), 2)
        state = ff_call(3, 0, block, state, act1)
        o_last = swap(o_far, 1)
        act0, grad_u0, h_all, cot_all = state
        part = row_major(inv_count * dot_tn(h_all, grad_u0))
        up_rows = [dp_reduce(part)]
        part = grad_h(5, half, part, [], F32)
        near0 = swap(part, 1)
        act1, grad_u1 = ff_call(3, 1, block, (act1, grad_u1), part)
        part = grad_h(4, half, act1, [near0], F32)
        far0 = swap(part, 2)
        act1, grad_u1 = ff_call(1, 1, near, (act1, grad_u1), part)
        part = grad_h(7, half, act1, [], F32)
        near1 = swap(part, 1)
        later = after(grad_u1, part)
        part = row_major(inv_count * dot_tn(h_all, later[:, :used[1]]))
        up_rows.append(dp_reduce(part))
        part = grad_h(6, half, part, [near1], F32)
        far1 = swap(part, 2)
        later = after(act0, part)
        part = row_major(inv_count * dot_tn(later, cot_all))
        down_rows = [dp_reduce(part)]
        part = grad_h(1, seq_len, part, [], F32)
        side = swap(part, 1)
        later = after(act1, part)
        part = row_major(inv_count * dot_tn(later[:, :used[1]], cot_all))
        down_rows.append(dp_reduce(part))
        far0 = after(far0, part)

        own_rows = d_model // dev_count

        def exchange(rows_of):
            blocks = [lax.dynamic_slice_in_dim(rows_of, (my_idx ^ bits) * own_rows, own_rows, axis=0) for bits in range(cp_size)]
            return jnp.stack([blocks[0]] + [row_major(swap(row_major(blocks[bits]), bits)) for bits in range(1, cp_size)])

        up_got = [exchange(up_rows[0])]
        grad_h_bf = grad_h(0, seq_len, part, [cot, side, far0, far1], BF16)

        def block_sum(left, right_t):
            def block(bits):
                return inv_count * dot_tt(own_cols(left, bits), right_t)

            return block

        def first_sends(block):
            parts = block(3), block(1)
            return (swap(parts[0], 1), swap(parts[1], 1)), parts

        def second_send(block, sent):
            part = block(2) + sent[0]
            return swap(part, 2), part

        mine = [None] + [swap(own_cols(grad_h_bf, bits), bits) for bits in range(1, cp_size)]
        do_t = dot_tt(w_o, grad_h_bf).astype(BF16)

        def kv_block(dkv):
            blocks = dkv.reshape((cp_size, 2) + dkv.shape[1:])
            return lambda bits: lax.dynamic_index_in_dim(blocks, my_idx ^ bits, axis=0, keepdims=False)

        dq0_t, dkv0 = attn_backward(tab, q_t, do_t, o_f32, lse, kv_all, kv_heads, head_dim, 0)
        kv0_block, q0_block = kv_block(dkv0), block_sum(x, dq0_t)
        kv0_sent, parts_kv = first_sends(kv0_block)
        q0_sent, parts_q = first_sends(q0_block)
        kv0_far, part_kv = second_send(kv0_block, (after(kv0_sent[0], *parts_q), kv0_sent[1]))
        q0_far, part_q = second_send(q0_block, q0_sent)
        do_t = after(do_t, part_kv, part_q)
        dq1_t, dkv1 = attn_backward(tab, q_t, do_t, o_f32, lse, kv_all, kv_heads, head_dim, 1, 0, 2)
        q1_block = block_sum(x, dq1_t)
        q1_sent, parts_q = first_sends(q1_block)
        base_q = q0_block(0)
        q1_far, part_q = second_send(q1_block, (after(q1_sent[0], base_q), q1_sent[1]))
        do_t = after(do_t, part_q, *parts_q)
        dq2_t, dkv1 = attn_backward(tab, q_t, do_t, o_f32, lse, kv_all, kv_heads, head_dim, 1, 1, 2, (dkv1,))
        kv1_block, q2_block = kv_block(dkv1), block_sum(x, dq2_t)
        kv1_sent, parts_kv = first_sends(kv1_block)
        q2_sent, parts_q = first_sends(q2_block)
        kv1_far, part_kv = second_send(kv1_block, (after(kv1_sent[0], *parts_q), kv1_sent[1]))
        q2_far, part_q = second_send(q2_block, (after(q2_sent[0], part_kv), q2_sent[1]))
        mine[0] = own_cols(after(grad_h_bf, part_q), 0)
        sum_oq = head_grad(inv_count, mine, (o_t, o_near, o_far, o_last), (base_q, q0_sent[1], q0_far))
        grad_oq = dp_reduce(sum_oq)
        kv0_own = (kv0_block(0) + kv0_sent[1] + after(kv0_far, sum_oq)).astype(BF16)
        kv1_own = (kv1_block(0) + kv1_sent[1] + after(kv1_far, kv0_own)).astype(BF16)
        dkv_t = jnp.concatenate([jnp.concatenate([part[0, which], part[1, which]], axis=1)
                                 for which in range(2) for part in (kv0_own, kv1_own)], axis=0)
        w_block = block_sum(x, dkv_t)
        w_sent, _ = first_sends(w_block)
        w_far, part_w = second_send(w_block, w_sent)
        up_got.append(exchange(after(up_rows[1], part_w)))
        grad_w_up = spread_columns(my_idx, up_got, splits)
        sum_q1 = q1_block(0) + q1_sent[1] + after(q1_far, part_w)
        sum_q2 = q2_block(0) + q2_sent[1] + after(q2_far, part_w)
        sum_w = w_block(0) + w_sent[1] + w_far
        sum_qk = jnp.concatenate([sum_q1, sum_q2, sum_w], axis=1)
        grad_qk = dp_reduce(sum_qk)
        later = jnp.concatenate([after(dq0_t, sum_qk), dq1_t, dq2_t], axis=0)
        grad_x = dot_tt(later, w_q)
        grad_x = grad_h_bf + grad_x + dot_tt(after(dkv_t, sum_qk), w_kv)
        grad_w_down = jnp.concatenate(down_rows, axis=0)
        o_width = n_heads * head_dim

        grad_w_q = jnp.concatenate([grad_oq[:, o_width:], grad_qk[:, :rows]], axis=1).reshape(own_rows, n_heads, head_dim)
        grad_w_k = grad_qk[:, rows:rows + kv_width].reshape(own_rows, kv_heads, head_dim)
        grad_w_v = grad_qk[:, rows + kv_width:].reshape(own_rows, kv_heads, head_dim)
        grad_w_o = grad_oq[:, :o_width].reshape(own_rows, n_heads, head_dim)
        return grad_x.astype(BF16)[None], grad_w_q, grad_w_k, grad_w_v, grad_w_o, grad_w_up, grad_w_down

    act_spec = P('dp', 'cp', None)
    rep_three = P(None, None, None)
    rep_two = P(None, None)
    grad_three = P(('dp', 'cp'), None, None)
    grad_two = P(('dp', 'cp'), None)
    return jax.shard_map(per_device, mesh=mesh,
                         in_specs=(act_spec, act_spec, rep_three, rep_three, rep_three, rep_three, rep_two, rep_two),
                         out_specs=(act_spec, grad_three, grad_three, grad_three, grad_three, grad_two, grad_two),
                         check_vma=False)
```

```python
import functools
import math

import jax
import jax.numpy as jnp
from jax import lax
from jax.experimental import pallas as pl
from jax.experimental.pallas import tpu as pltpu
from jax.experimental.layout import Layout, with_layout_constraint
from jax.sharding import PartitionSpec as P


NEG_BIG = -1e30
LOG2E = math.log2(math.e)
F32 = jnp.float32
FF_TILE = 256
VMEM_BYTES = 56 * 2 ** 20
FF_ROWS = 512
BF16 = jnp.bfloat16


def row_major(values):
    return with_layout_constraint(values, Layout(major_to_minor=(0, 1)))


def dot_nn(lhs, rhs):
    return lax.dot_general(lhs, rhs, (((1,), (0,)), ((), ())), preferred_element_type=F32)


def dot_nt(lhs, rhs):
    return lax.dot_general(lhs, rhs, (((1,), (1,)), ((), ())), preferred_element_type=F32)


def dot_tn(lhs, rhs):
    return lax.dot_general(lhs, rhs, (((0,), (0,)), ((), ())), preferred_element_type=F32)


def dot_tt(lhs, rhs):
    return lax.dot_general(lhs, rhs, (((0,), (1,)), ((), ())), preferred_element_type=F32)


def pair_table(my_idx, cp_size):
    steps = jnp.arange(2 * cp_size + 1)
    late = steps > my_idx
    key_block = jnp.where(late, steps - my_idx - 1, steps)
    key_slot = jnp.where(key_block < cp_size, 2 * key_block, 2 * (2 * cp_size - 1 - key_block) + 1)
    last = (steps == my_idx) | (steps == 2 * cp_size)
    first = (steps == 0) | (steps == my_idx + 1)
    return jnp.stack([late, key_slot, last, first]).astype(jnp.int32)


def causal_keep(half):
    keys = lax.broadcasted_iota(jnp.int32, (half, half), 0)
    queries = lax.broadcasted_iota(jnp.int32, (half, half), 1)
    return keys <= queries


def attn_fwd_kernel(group, scale, tab, q_ref, k_ref, v_ref, of_ref, ob_ref, lse_ref, m_ref, l_ref, acc_ref):
    dim = k_ref.shape[1]
    half = q_ref.shape[1] // 2
    factor = scale * LOG2E

    def pair_step(pair, carry):
        cols = pl.ds(pl.multiple_of(tab[0, pair] * half, half), half)
        slot = pl.ds(pl.multiple_of(tab[1, pair] * half, half), half)

        @pl.when(tab[3, pair] == 1)
        def _():
            m_ref[...] = jnp.full(m_ref.shape, NEG_BIG, F32)
            l_ref[...] = jnp.zeros(l_ref.shape, F32)
            acc_ref[...] = jnp.zeros(acc_ref.shape, F32)

        def run(masked):
            keys = k_ref[slot, :]
            vals_t = v_ref[slot, :].T

            def scores_of(head):
                scores = dot_nn(keys, q_ref[head * dim:(head + 1) * dim, cols])
                return jnp.where(causal_keep(half), scores, NEG_BIG) if masked else scores

            following = scores_of(0)
            for head in range(group):
                scores = following
                if head + 1 < group:
                    following = scores_of(head + 1)
                rows = slice(head * dim, (head + 1) * dim)
                old_max = m_ref[head:head + 1, :]
                new_max = jnp.maximum(old_max, jnp.max(scores, axis=0, keepdims=True))
                probs = jnp.exp2(scores * factor - new_max * factor)
                alpha = jnp.exp2((old_max - new_max) * factor)
                m_ref[head:head + 1, :] = new_max
                l_ref[head:head + 1, :] = alpha * l_ref[head:head + 1, :] + jnp.sum(probs, axis=0, keepdims=True)
                acc_ref[rows, :] = alpha * acc_ref[rows, :] + dot_nn(vals_t, probs.astype(BF16))

        @pl.when(tab[2, pair] == 0)
        def _():
            run(False)

        @pl.when(tab[2, pair] == 1)
        def _():
            run(True)
            lse_ref[0, :, cols] = m_ref[...] * factor + jnp.log2(l_ref[...])
            for head in range(group):
                rows = slice(head * dim, (head + 1) * dim)
                out = acc_ref[rows, :] / l_ref[head:head + 1, :]
                of_ref[rows, cols] = out
                ob_ref[rows, cols] = out.astype(BF16)

        return carry

    lax.fori_loop(0, tab.shape[1], pair_step, 0)


def attn_forward(tab, q_t, kv_all, kv_heads, head_dim):
    width, seq = q_t.shape
    half = seq // 2
    group = width // (kv_heads * head_dim)
    rows = group * head_dim
    n_pairs = tab.shape[1]
    q_spec = pl.BlockSpec((rows, seq), lambda k, t: (k, 0))
    return pl.pallas_call(
        functools.partial(attn_fwd_kernel, group, head_dim ** -0.5),
        grid_spec=pltpu.PrefetchScalarGridSpec(
            num_scalar_prefetch=1,
            grid=(kv_heads,),
            in_specs=[q_spec,
                      pl.BlockSpec((kv_all.shape[0], head_dim), lambda k, t: (0, k)),
                      pl.BlockSpec((kv_all.shape[0], head_dim), lambda k, t: (0, kv_heads + k))],
            out_specs=[q_spec, q_spec,
                       pl.BlockSpec((1, group, seq), lambda k, t: (k, 0, 0))],
            scratch_shapes=[pltpu.VMEM((group, half), F32), pltpu.VMEM((group, half), F32), pltpu.VMEM((rows, half), F32)]),
        out_shape=[jax.ShapeDtypeStruct((width, seq), F32), jax.ShapeDtypeStruct((width, seq), BF16),
                   jax.ShapeDtypeStruct((kv_heads, group, seq), F32)],
        compiler_params=pltpu.CompilerParams(vmem_limit_bytes=VMEM_BYTES),
        cost_estimate=pl.CostEstimate(flops=4 * width * half * half * n_pairs,
                                      bytes_accessed=12 * width * seq, transcendentals=width // head_dim * half * half * n_pairs),
    )(tab, q_t, kv_all, kv_all)


def attn_bwd_kernel(group, first_head, scale, tab, q_ref, do_ref, of_ref, lse_ref, k_ref, v_ref, *refs):
    dim = k_ref.shape[1]
    half = q_ref.shape[1] // 2
    factor = scale * LOG2E
    dq_ref, dkv_ref, delta_ref, acc_ref = refs[-4:]
    dkv_ref[...] = refs[0][...] if len(refs) > 4 else jnp.zeros(dkv_ref.shape, F32)

    def pair_step(pair, carry):
        cols = pl.ds(pl.multiple_of(tab[0, pair] * half, half), half)
        slot = tab[1, pair]
        slot_rows = pl.ds(pl.multiple_of(slot * half, half), half)

        @pl.when(tab[3, pair] == 1)
        def _():
            acc_ref[...] = jnp.zeros(acc_ref.shape, F32)
            for head in range(group):
                rows = slice(head * dim, (head + 1) * dim)
                delta_ref[head:head + 1, :] = jnp.sum(do_ref[rows, cols].astype(F32) * of_ref[rows, cols], axis=0, keepdims=True)

        def run(masked):
            keys = k_ref[slot_rows, :]
            vals = v_ref[slot_rows, :]
            keys_t = keys.T
            for head in range(group):
                rows = slice(head * dim, (head + 1) * dim)
                q_head = q_ref[rows, cols]
                do_head = do_ref[rows, cols]
                scores = dot_nn(keys, q_head)
                if masked:
                    scores = jnp.where(causal_keep(half), scores, NEG_BIG)
                probs = jnp.exp2(scores * factor - lse_ref[0, first_head + head:first_head + head + 1, cols])
                grad_p = dot_nn(vals, do_head)
                grad_s = (probs * (grad_p - delta_ref[head:head + 1, :])).astype(BF16)
                dkv_ref[slot, 1] += dot_nt(do_head, probs.astype(BF16))
                dkv_ref[slot, 0] += scale * dot_nt(q_head, grad_s)
                acc_ref[rows, :] += dot_nn(keys_t, grad_s)

        @pl.when(tab[2, pair] == 0)
        def _():
            run(False)

        @pl.when(tab[2, pair] == 1)
        def _():
            run(True)
            dq_ref[:, cols] = (scale * acc_ref[...]).astype(BF16)

        return carry

    lax.fori_loop(0, tab.shape[1], pair_step, 0)


def attn_backward(tab, q_t, do_t, o_f32, lse, kv_all, kv_heads, head_dim, kv_head, piece=0, n_pieces=1, carry=()):
    width, seq = q_t.shape
    half = seq // 2
    group = width // (kv_heads * head_dim)
    heads = group // n_pieces
    rows = heads * head_dim
    n_slots = kv_all.shape[0] // half
    n_pairs = tab.shape[1]
    q_spec = pl.BlockSpec((rows, seq), lambda p, t: (kv_head * n_pieces + piece, 0))
    dkv_spec = pl.BlockSpec((n_slots, 2, head_dim, half), lambda p, t: (0, 0, 0, 0))
    return pl.pallas_call(
        functools.partial(attn_bwd_kernel, heads, piece * heads, head_dim ** -0.5),
        grid_spec=pltpu.PrefetchScalarGridSpec(
            num_scalar_prefetch=1,
            grid=(1,),
            in_specs=[q_spec, q_spec, q_spec,
                      pl.BlockSpec((1, group, seq), lambda p, t: (kv_head, 0, 0)),
                      pl.BlockSpec((kv_all.shape[0], head_dim), lambda p, t: (0, kv_head)),
                      pl.BlockSpec((kv_all.shape[0], head_dim), lambda p, t: (0, kv_heads + kv_head))]
            + [dkv_spec] * len(carry),
            out_specs=[pl.BlockSpec((rows, seq), lambda p, t: (0, 0)),
                       dkv_spec],
            scratch_shapes=[pltpu.VMEM((heads, half), F32), pltpu.VMEM((rows, half), F32)]),
        out_shape=[jax.ShapeDtypeStruct((rows, seq), BF16),
                   jax.ShapeDtypeStruct((n_slots, 2, head_dim, half), F32)],
        compiler_params=pltpu.CompilerParams(vmem_limit_bytes=VMEM_BYTES),
        cost_estimate=pl.CostEstimate(flops=10 * rows * half * half * n_pairs,
                                      bytes_accessed=12 * rows * seq, transcendentals=heads * half * half * n_pairs),
    )(tab, q_t, do_t, o_f32, lse, kv_all, kv_all, *carry)


def gelu_parts(values):
    curve = math.sqrt(2 / math.pi)
    square = values * values
    tanh = jnp.tanh(values * (curve + (curve * 0.044715) * square))
    cdf = 0.5 + 0.5 * tanh
    slope = cdf + (0.5 * values) * (1.0 - tanh * tanh) * (curve + (3 * curve * 0.044715) * square)
    return values * cdf, slope


def prep_kernel(segs, parts, idx_ref, *refs):
    n_blocks = sum(seg[3] + 1 for seg in segs)
    blocks, down_ref = refs[:n_blocks], refs[n_blocks]
    n_parts = len(parts)
    up_refs, down_refs = refs[n_blocks + 1:n_blocks + 1 + n_parts], refs[n_blocks + 1 + n_parts:n_blocks + 1 + 2 * n_parts]
    buf_ref, zero_ref, in_sem, out_sem = refs[n_blocks + 1 + 2 * n_parts:]
    step = pl.program_id(0)
    n_own, own_rows = buf_ref.shape[0], buf_ref.shape[1]
    ins = [pltpu.make_async_copy(down_ref.at[pl.ds(pl.multiple_of(idx_ref[0, own], 16), own_rows)], buf_ref.at[own], in_sem.at[own])
           for own in range(n_own)]
    outs = []
    for part, down_out in zip(parts, down_refs):
        for own in range(n_own):
            outs.append(pltpu.make_async_copy(buf_ref.at[own, pl.ds(part[0], part[1])],
                                              down_out.at[pl.ds(own * part[1], part[1])], out_sem.at[len(outs)]))
        if part[2]:
            outs.append(pltpu.make_async_copy(zero_ref.at[pl.ds(0, part[2])],
                                              down_out.at[pl.ds(n_own * part[1], part[2])], out_sem.at[len(outs)]))

    @pl.when(step == 0)
    def _():
        zero_ref[...] = jnp.zeros(zero_ref.shape, BF16)
        for copy in ins:
            copy.start()

    @pl.when(step == 1)
    def _():
        for copy in ins:
            copy.wait()
        for copy in outs:
            copy.start()

    rows = blocks[0].shape[0]
    lanes = lax.broadcasted_iota(jnp.int32, (rows, 128), 1)
    cover = [{} for _ in parts]
    pos = 0
    for number, seg in enumerate(segs):
        shift = idx_ref[1, number]
        turned = [pltpu.roll(blocks[pos + tile][...].astype(F32), (128 - shift) % 128, 1) for tile in range(seg[3] + 1)]
        pos += seg[3] + 1
        for tile in range(seg[3]):
            cover[seg[0]].setdefault(seg[2] + tile, []).append(
                (seg[1], jnp.where(lanes < 128 - shift, turned[tile], turned[tile + 1])))
    for part, tiles, up_ref in zip(parts, cover, up_refs):
        used = n_own * part[1]
        for tile in range(up_ref.shape[1] // 128):
            value = jnp.zeros((rows, 128), F32)
            for start, piece in tiles.get(tile, []):
                value = piece if start <= tile * 128 else jnp.where(lanes >= start - tile * 128, piece, value)
            if used < (tile + 1) * 128:
                value = jnp.where(lanes < used - tile * 128, value, 0.0)
            up_ref[:, tile * 128:(tile + 1) * 128] = value.astype(BF16)

    @pl.when(step == pl.num_programs(0) - 1)
    def _():
        for copy in outs:
            copy.wait()


def prepare(starts, splits, w_up, w_down):
    d_model, own_rows = w_up.shape[0], splits[-1][0] + splits[-1][1]
    n_own = starts.shape[0]
    parts = [(first, count, -(n_own * count) % FF_TILE) for first, count in splits]
    segs, shifts, bases = [], [], []
    for number, part in enumerate(parts):
        for own in range(n_own):
            dest = own * part[1]
            segs.append((number, dest, dest // 128, -(-(dest % 128 + part[1]) // 128)))
            source = starts[own] + part[0] - dest % 128
            shifts.append(source % 128)
            bases.append(source // 128)
    table = jnp.stack([jnp.pad(starts, (0, len(segs) - n_own)), jnp.stack(shifts), jnp.stack(bases)]).astype(jnp.int32)
    rows = 512
    last = w_up.shape[1] // 128 - 1
    in_specs = []
    for number, seg in enumerate(segs):
        for tile in range(seg[3] + 1):
            in_specs.append(pl.BlockSpec((rows, 128), lambda i, t, number=number, tile=tile:
                                         (i, jnp.clip(t[2, number] + tile, 0, last))))
    widths = [n_own * part[1] + part[2] for part in parts]
    outs = pl.pallas_call(
        functools.partial(prep_kernel, segs, parts),
        grid_spec=pltpu.PrefetchScalarGridSpec(
            num_scalar_prefetch=1,
            grid=(d_model // rows,),
            in_specs=in_specs + [pl.BlockSpec(memory_space=pl.ANY)],
            out_specs=[pl.BlockSpec((rows, width), lambda i, t: (i, 0)) for width in widths]
            + [pl.BlockSpec(memory_space=pl.ANY) for _ in widths],
            scratch_shapes=[pltpu.VMEM((n_own, own_rows, d_model), BF16), pltpu.VMEM((64, d_model), BF16),
                            pltpu.SemaphoreType.DMA((n_own,)), pltpu.SemaphoreType.DMA((n_own * len(parts) + len(parts),))]),
        out_shape=[jax.ShapeDtypeStruct((d_model, width), BF16) for width in widths]
        + [jax.ShapeDtypeStruct((width, d_model), BF16) for width in widths],
        compiler_params=pltpu.CompilerParams(vmem_limit_bytes=VMEM_BYTES),
        cost_estimate=pl.CostEstimate(flops=8 * d_model * sum(widths), bytes_accessed=9 * d_model * sum(widths), transcendentals=0),
    )(table, *([w_up] * len(in_specs)), w_down)
    return outs[:len(parts)], outs[len(parts):]


def ff_kernel(step_rows, copies, first_row, n_pieces, *refs):
    pieces = [(refs[2 * piece], refs[2 * piece + 1]) for piece in range(n_pieces)]
    up_ref, down_ref = refs[2 * n_pieces:2 * n_pieces + 2]
    if copies:
        act_ref, du_ref, h_out, cot_out, sem = refs[-5:]
        moves, row = [], first_row
        for h_ref, cot_ref in pieces:
            rows = pl.ds(row, h_ref.shape[0])
            moves.append(pltpu.make_async_copy(h_ref, h_out.at[rows], sem.at[len(moves)]))
            moves.append(pltpu.make_async_copy(cot_ref, cot_out.at[rows], sem.at[len(moves)]))
            row += h_ref.shape[0]

        @pl.when(pl.program_id(0) == 0)
        def _():
            for move in moves:
                move.start()
    else:
        act_ref, du_ref = refs[-2:]

    places, base = [], 0
    for h_ref, cot_ref in pieces:
        places += [(h_ref, cot_ref, first, base + first) for first in range(0, h_ref.shape[0], step_rows)]
        base += h_ref.shape[0]

    def products(h_ref, cot_ref, first, _):
        rows = slice(first, first + step_rows)
        return dot_nn(h_ref[rows, :], up_ref[...]), dot_nt(cot_ref[rows, :], down_ref[...])

    following = products(*places[0])
    for number, place in enumerate(places):
        hidden, grad_act = following
        if number + 1 < len(places):
            following = products(*places[number + 1])
        out_rows = slice(place[3], place[3] + step_rows)
        act, slope = gelu_parts(hidden)
        act_ref[out_rows, :] = act.astype(BF16)
        du_ref[out_rows, :] = (grad_act.astype(BF16).astype(F32) * slope).astype(BF16)

    if copies:
        @pl.when(pl.program_id(0) == pl.num_programs(0) - 1)
        def _():
            for move in moves:
                move.wait()


def ff_forward(index, count, pieces, up, down, copies, carry):
    tokens = sum(piece[0].shape[0] for piece in pieces)
    d_model, width = up.shape
    tile = FF_TILE
    shapes = [jax.ShapeDtypeStruct((count * tokens, width), BF16)] * 2
    specs = [pl.BlockSpec((tokens, tile), lambda n: (index, n))] * 2
    if copies:
        shapes = shapes + [jax.ShapeDtypeStruct((count * tokens, d_model), BF16)] * 2
        specs = specs + [pl.BlockSpec(memory_space=pl.ANY)] * 2
    in_specs, args = [], []
    for h_blk, cot_blk, row_blk in pieces:
        in_specs += [pl.BlockSpec(h_blk.shape, lambda n: (0, 0)),
                     pl.BlockSpec(h_blk.shape, lambda n, row_blk=row_blk: (row_blk, 0))]
        args += [h_blk, cot_blk]
    carry = list(carry)
    return pl.pallas_call(
        functools.partial(ff_kernel, FF_ROWS, copies, index * tokens, len(pieces)),
        grid=(width // tile,),
        in_specs=in_specs + [pl.BlockSpec((d_model, tile), lambda n: (0, n)), pl.BlockSpec((tile, d_model), lambda n: (n, 0))]
        + [pl.BlockSpec(memory_space=pl.ANY)] * len(carry),
        out_specs=specs,
        out_shape=shapes,
        input_output_aliases={len(args) + 2 + pos: pos for pos in range(len(carry))},
        scratch_shapes=[pltpu.SemaphoreType.DMA((2 * len(pieces),))] if copies else [],
        compiler_params=pltpu.CompilerParams(vmem_limit_bytes=VMEM_BYTES),
        cost_estimate=pl.CostEstimate(flops=4 * tokens * d_model * width, bytes_accessed=4 * d_model * (width + 2 * tokens),
                                      transcendentals=tokens * width),
    )(*args, up, down, *carry)


def grad_h_kernel(n_parts, *refs):
    total = sum(dot_nt(refs[2 * part][...], refs[2 * part + 1][...]) for part in range(n_parts))
    halves = []
    for extra in refs[2 * n_parts:-1]:
        if extra.shape == total.shape:
            total = total + extra[...]
        else:
            halves.append(extra[...])
    if halves:
        total = total + jnp.concatenate(halves, axis=0)
    refs[-1][...] = total.astype(refs[-1].dtype)


def grad_h_block(index, tokens, grad_u, up, extras, dtype):
    d_model = up[0].shape[0]
    width = sum(part.shape[1] for part in up)
    tile = 256
    in_specs, args = [], []
    for left, right in zip(grad_u, up):
        in_specs += [pl.BlockSpec((tokens, left.shape[1]), lambda n: (index, 0)), pl.BlockSpec((tile, right.shape[1]), lambda n: (n, 0))]
        args += [left, right]
    return pl.pallas_call(
        functools.partial(grad_h_kernel, len(up)),
        grid=(d_model // tile,),
        in_specs=in_specs + [pl.BlockSpec((extra.shape[0], tile), lambda n: (0, n)) for extra in extras],
        out_specs=pl.BlockSpec((tokens, tile), lambda n: (0, n)),
        out_shape=jax.ShapeDtypeStruct((tokens, d_model), dtype),
        compiler_params=pltpu.CompilerParams(vmem_limit_bytes=VMEM_BYTES),
        cost_estimate=pl.CostEstimate(flops=2 * tokens * d_model * width, bytes_accessed=2 * width * (d_model + tokens) + 4 * tokens * d_model,
                                      transcendentals=0),
    )(*args, *extras)


def head_grad_kernel(scale, n_pairs, n_tiles, *refs):
    step = pl.program_id(0)

    @pl.when(step < n_tiles)
    def _():
        total = sum(dot_nn(refs[n_pairs + pair][...], refs[pair][...]) for pair in range(n_pairs))
        refs[-1][...] = (scale * total).T

    @pl.when(step >= n_tiles)
    def _():
        refs[-1][...] = sum(ref[...] for ref in refs[2 * n_pairs:-1])


def head_grad(scale, columns, heads_t, terms):
    n_pairs = len(columns)
    rows, width, tokens = columns[0].shape[1], heads_t[0].shape[0], columns[0].shape[0]
    tile = rows
    n_tiles, n_more = width // tile, terms[0].shape[1] // tile
    last = n_tiles - 1
    return pl.pallas_call(
        functools.partial(head_grad_kernel, scale, n_pairs, n_tiles),
        grid=(n_tiles + n_more,),
        in_specs=[pl.BlockSpec((tokens, rows), lambda n: (0, 0))] * n_pairs
        + [pl.BlockSpec((tile, tokens), lambda n: (jnp.minimum(n, last), 0))] * n_pairs
        + [pl.BlockSpec((rows, tile), lambda n: (0, jnp.maximum(n - n_tiles, 0)))] * len(terms),
        out_specs=pl.BlockSpec((rows, tile), lambda n: (0, n)),
        out_shape=jax.ShapeDtypeStruct((rows, width + n_more * tile), F32),
        compiler_params=pltpu.CompilerParams(vmem_limit_bytes=VMEM_BYTES),
        cost_estimate=pl.CostEstimate(flops=2 * n_pairs * rows * width * tokens, bytes_accessed=9 * tokens * (rows + width), transcendentals=0),
    )(*columns, *heads_t, *terms)


def spread_kernel(splits, idx_ref, *refs):
    got_refs, out_ref = refs[:-1], refs[-1]
    count = got_refs[0].shape[0]
    block = splits[-1][0] + splits[-1][1]
    for dest in range(out_ref.shape[1] // block):
        row, src = dest // count, dest % count
        for (first, cols), got_ref in zip(splits, got_refs):
            out_ref[:, dest * block + first:dest * block + first + cols] = got_ref[idx_ref[0] ^ src, :, row * cols:(row + 1) * cols]


def spread_columns(my_idx, got, splits):
    count, rows = got[0].shape[:2]
    width = count * sum(part.shape[2] for part in got)
    return pl.pallas_call(
        functools.partial(spread_kernel, splits),
        in_specs=[pl.BlockSpec(memory_space=pltpu.SMEM)] + [pl.BlockSpec(memory_space=pltpu.VMEM)] * len(got),
        out_specs=pl.BlockSpec(memory_space=pltpu.VMEM),
        out_shape=jax.ShapeDtypeStruct((rows, width), F32),
        cost_estimate=pl.CostEstimate(flops=rows * width, bytes_accessed=8 * rows * width, transcendentals=0),
    )(my_idx.reshape(1), *got)


def solution(mesh):
    cp_size = mesh.shape['cp']
    dp_size = mesh.shape['dp']
    dev_count = cp_size * dp_size

    def swap(values, bits):
        return lax.ppermute(values, 'cp', [(src, src ^ bits) for src in range(cp_size)])

    def dp_reduce(grad):
        return lax.psum_scatter(grad, 'dp', scatter_dimension=0, tiled=True)

    def after(value, *earlier):
        return lax.optimization_barrier((value,) + earlier)[0]

    def per_device(x_loc, cot_loc, w_q, w_k, w_v, w_o, w_up, w_down):
        d_model = x_loc.shape[2]
        seq_len = x_loc.shape[1]
        kv_heads, head_dim = w_k.shape[1], w_k.shape[2]
        n_heads = w_q.shape[1]
        group = n_heads // kv_heads
        half = seq_len // 2
        kv_width = kv_heads * head_dim
        rows = group * head_dim
        ff_dim = w_up.shape[1]
        ff_part = ff_dim // dev_count
        my_idx = lax.axis_index('cp')
        x = x_loc[0]
        cot = cot_loc[0]
        w_q = w_q.reshape(d_model, n_heads * head_dim)
        w_o = w_o.reshape(d_model, n_heads * head_dim)
        w_kv = jnp.concatenate([w_k.reshape(d_model, kv_width), w_v.reshape(d_model, kv_width)], axis=1)
        tab = pair_table(my_idx, cp_size)

        inv_count = 1.0 / dev_count

        def own_cols(values, bits):
            width = d_model // dev_count
            return jnp.concatenate([lax.dynamic_slice_in_dim(values, (part * cp_size + (my_idx ^ bits)) * width, width, axis=1)
                                    for part in range(dp_size)], axis=1)

        kv_own = dot_nn(x, w_kv).astype(BF16)
        kv_all = lax.all_gather(kv_own, 'cp', axis=0, tiled=True)
        cot_near = swap(cot, 1)

        first_part = FF_TILE * (dp_size * ff_part // (2 * FF_TILE)) // dp_size
        splits = ((0, first_part), (first_part, ff_part - first_part))
        used = [dp_size * count for _, count in splits]
        starts = (jnp.arange(dp_size) * cp_size + my_idx) * ff_part
        w_up_own, w_down_own = prepare(starts, splits, w_up, w_down)
        cot_far = swap(after(cot, w_up_own[0]), 2)
        later = after(x, w_up_own[0])
        q_t = dot_tt(w_q, later).astype(BF16)

        kv_all = after(kv_all, q_t, w_up_own[0])
        o_f32, o_t, lse = attn_forward(tab, q_t, kv_all, kv_heads, head_dim)

        h_act = (x + dot_tt(o_t, w_o)).astype(BF16)
        h_far0 = swap(h_act[:half], 2)
        h_near = swap(h_act, 1)
        o_near = swap(o_t, 1)

        def ff_call(index, part, pieces, carry, *earlier):
            first = after(pieces[0][0], *earlier) if earlier else pieces[0][0]
            pieces = [(first,) + pieces[0][1:]] + pieces[1:]
            return ff_forward(index, cp_size, pieces, w_up_own[part], w_down_own[part], part == 0, carry)

        def remote(piece, far_piece):
            return [(far_piece, cot_far, piece), (swap(far_piece, 1), cot_last, piece)]

        own, near = [(h_act, cot, 0)], [(h_near, cot_near, 0)]
        state = ff_call(0, 0, own, ())
        h_far1 = swap(after(h_act, state[0])[half:], 2)
        cot_last = swap(after(cot_far, state[0]), 1)
        state = ff_call(1, 0, near, state)
        more = ff_call(0, 1, own, (), state[0])
        block = remote(0, after(h_far0, more[0]))
        state = ff_call(2, 0, block, state)
        act1, grad_u1 = ff_call(2, 1, block, more, state[0])

        def grad_h(index, tokens, earlier, extras, dtype):
            later = after(grad_u1, earlier)
            return grad_h_block(index, tokens, (state[1], later), w_up_own, extras, dtype)

        h_far1 = after(h_far1, act1)
        block = remote(1, h_far1)
        o_far = swap(after(o_t, h_far1), 2)
        state = ff_call(3, 0, block, state, act1)
        o_last = swap(o_far, 1)
        act0, grad_u0, h_all, cot_all = state
        part = row_major(inv_count * dot_tn(h_all, grad_u0))
        up_rows = [dp_reduce(part)]
        part = grad_h(5, half, part, [], F32)
        near0 = swap(part, 1)
        act1, grad_u1 = ff_call(3, 1, block, (act1, grad_u1), part)
        part = grad_h(4, half, act1, [near0], F32)
        far0 = swap(part, 2)
        act1, grad_u1 = ff_call(1, 1, near, (act1, grad_u1), part)
        part = grad_h(7, half, act1, [], F32)
        near1 = swap(part, 1)
        later = after(grad_u1, part)
        part = row_major(inv_count * dot_tn(h_all, later[:, :used[1]]))
        up_rows.append(dp_reduce(part))
        part = grad_h(6, half, part, [near1], F32)
        far1 = swap(part, 2)
        later = after(act0, part)
        part = row_major(inv_count * dot_tn(later, cot_all))
        down_rows = [dp_reduce(part)]
        part = grad_h(1, seq_len, part, [], F32)
        side = swap(part, 1)
        later = after(act1, part)
        part = row_major(inv_count * dot_tn(later[:, :used[1]], cot_all))
        down_rows.append(dp_reduce(part))
        far0 = after(far0, part)

        own_rows = d_model // dev_count

        def exchange(rows_of):
            blocks = [lax.dynamic_slice_in_dim(rows_of, (my_idx ^ bits) * own_rows, own_rows, axis=0) for bits in range(cp_size)]
            return jnp.stack([blocks[0]] + [row_major(swap(row_major(blocks[bits]), bits)) for bits in range(1, cp_size)])

        up_got = [exchange(up_rows[0])]
        grad_h_bf = grad_h(0, seq_len, part, [cot, side, far0, far1], BF16)

        def block_sum(left, right_t):
            def block(bits):
                return inv_count * dot_tt(own_cols(left, bits), right_t)

            return block

        def first_sends(block):
            parts = block(3), block(1)
            return (swap(parts[0], 1), swap(parts[1], 1)), parts

        def second_send(block, sent):
            part = block(2) + sent[0]
            return swap(part, 2), part

        mine = [own_cols(grad_h_bf, bits) for bits in range(cp_size)]
        later = after(grad_h_bf, mine[0])
        mine[1:] = [swap(mine[bits], bits) for bits in range(1, cp_size)]
        do_t = dot_tt(w_o, later).astype(BF16)

        def kv_block(dkv):
            blocks = dkv.reshape((cp_size, 2) + dkv.shape[1:])
            return lambda bits: lax.dynamic_index_in_dim(blocks, my_idx ^ bits, axis=0, keepdims=False)

        dq0_t, dkv0 = attn_backward(tab, q_t, do_t, o_f32, lse, kv_all, kv_heads, head_dim, 0)
        kv0_block, q0_block = kv_block(dkv0), block_sum(x, dq0_t)
        kv0_sent, parts_kv = first_sends(kv0_block)
        q0_sent, parts_q = first_sends(q0_block)
        kv0_far, part_kv = second_send(kv0_block, (after(kv0_sent[0], *parts_q), kv0_sent[1]))
        q0_far, part_q = second_send(q0_block, q0_sent)
        do_t = after(do_t, part_kv, part_q)
        dq1_t, dkv1 = attn_backward(tab, q_t, do_t, o_f32, lse, kv_all, kv_heads, head_dim, 1, 0, 2)
        q1_block = block_sum(x, dq1_t)
        q1_sent, parts_q = first_sends(q1_block)
        base_q = q0_block(0)
        q1_far, part_q = second_send(q1_block, (after(q1_sent[0], base_q), q1_sent[1]))
        do_t = after(do_t, part_q, *parts_q)
        dq2_t, dkv1 = attn_backward(tab, q_t, do_t, o_f32, lse, kv_all, kv_heads, head_dim, 1, 1, 2, (dkv1,))
        kv1_block, q2_block = kv_block(dkv1), block_sum(x, dq2_t)
        kv1_sent, parts_kv = first_sends(kv1_block)
        q2_sent, parts_q = first_sends(q2_block)
        kv1_far, part_kv = second_send(kv1_block, (after(kv1_sent[0], *parts_q), kv1_sent[1]))
        mine[0] = after(mine[0], part_kv)
        sum_oq = head_grad(inv_count, mine, (o_t, o_near, o_far, o_last), (base_q, q0_sent[1], q0_far))
        grad_oq = dp_reduce(sum_oq)
        q2_far, part_q = second_send(q2_block, (after(q2_sent[0], sum_oq), q2_sent[1]))
        kv0_far = after(kv0_far, part_q)
        kv0_own = (kv0_block(0) + kv0_sent[1] + kv0_far).astype(BF16)
        kv1_own = (kv1_block(0) + kv1_sent[1] + after(kv1_far, kv0_own)).astype(BF16)
        dkv_t = jnp.concatenate([jnp.concatenate([part[0, which], part[1, which]], axis=1)
                                 for which in range(2) for part in (kv0_own, kv1_own)], axis=0)
        w_block = block_sum(x, dkv_t)
        w_sent, _ = first_sends(w_block)
        w_far, part_w = second_send(w_block, w_sent)
        up_got.append(exchange(after(up_rows[1], part_w)))
        grad_w_up = spread_columns(my_idx, up_got, splits)
        sum_q1 = q1_block(0) + q1_sent[1] + after(q1_far, part_w)
        sum_q2 = q2_block(0) + q2_sent[1] + after(q2_far, part_w)
        sum_w = w_block(0) + w_sent[1] + w_far
        sum_qk = jnp.concatenate([sum_q1, sum_q2, sum_w], axis=1)
        grad_qk = dp_reduce(sum_qk)
        later = jnp.concatenate([after(dq0_t, sum_qk), dq1_t, dq2_t], axis=0)
        grad_x = dot_tt(later, w_q)
        grad_x = grad_h_bf + grad_x + dot_tt(after(dkv_t, sum_qk), w_kv)
        grad_w_down = jnp.concatenate(down_rows, axis=0)
        o_width = n_heads * head_dim

        grad_w_q = jnp.concatenate([grad_oq[:, o_width:], grad_qk[:, :rows]], axis=1).reshape(own_rows, n_heads, head_dim)
        grad_w_k = grad_qk[:, rows:rows + kv_width].reshape(own_rows, kv_heads, head_dim)
        grad_w_v = grad_qk[:, rows + kv_width:].reshape(own_rows, kv_heads, head_dim)
        grad_w_o = grad_oq[:, :o_width].reshape(own_rows, n_heads, head_dim)
        return grad_x.astype(BF16)[None], grad_w_q, grad_w_k, grad_w_v, grad_w_o, grad_w_up, grad_w_down

    act_spec = P('dp', 'cp', None)
    rep_three = P(None, None, None)
    rep_two = P(None, None)
    grad_three = P(('dp', 'cp'), None, None)
    grad_two = P(('dp', 'cp'), None)
    return jax.shard_map(per_device, mesh=mesh,
                         in_specs=(act_spec, act_spec, rep_three, rep_three, rep_three, rep_three, rep_two, rep_two),
                         out_specs=(act_spec, grad_three, grad_three, grad_three, grad_three, grad_two, grad_two),
                         check_vma=False)
```
